32 devices in a mesh: seq: 4 (over y, x), tm: 8 (over z, core).
Axes of the slice: x: 2, y: 2, z: 4, core: 2. Of those that a mesh axis runs over, the one named last changes fastest.
Arguments:
- inputs: bfloat16 [32, 1024, 512], P('seq', 'tm'), may hold values from -6 to 6
- lengths: int32 [32, 8], P('seq'), may hold values from 1 to 256, 1024 in all within a row
- norm_gain: bfloat16 [512], replicated, may hold values from 0.099609375 to 1.8984375
- conv_kernel: bfloat16 [3, 3, 512], replicated, may hold values from -3.5 to 3.5
- qkv_weight: bfloat16 [3, 512, 512], replicated, may hold values from -0.25 to 0.25
- out_weight: bfloat16 [512, 512], replicated, may hold values from -1 to 1
- mlp_gain: bfloat16 [512], replicated, may hold values from 0.099609375 to 1.8984375
- up_weight: bfloat16 [512, 2048], replicated, may hold values from -0.25 to 0.25
- down_weight: bfloat16 [2048, 512], replicated, may hold values from -0.125 to 0.125
- layer_scale: bfloat16 [512], replicated, may hold values from 0.5 to 2
- cotangent: bfloat16 [32, 1024, 512], P('seq', 'tm'), may hold values from -6 to 6
Outputs:
- output: bfloat16 [32, 1024, 512], P('seq', 'tm')
- d_inputs: float32 [32, 1024, 512], P('seq', 'tm')
- d_norm_gain: float32 [512], replicated
- d_conv_kernel: float32 [3, 3, 512], replicated
- d_qkv_weight: float32 [3, 512, 512], replicated
- d_out_weight: float32 [512, 512], replicated
- d_mlp_gain: float32 [512], replicated
- d_up_weight: float32 [512, 2048], replicated
- d_down_weight: float32 [2048, 512], replicated
- d_layer_scale: float32 [512], replicated
The draws below stay inside these ranges and needn't reach their ends.
Inputs may be any that keep to these rules, and one draw needn't show every extreme that they name: `lengths`: each row sums to 1024; the longest video of each sequence has exactly 256 frames.
All inputs are finite; a program needn't handle non-finite values.
Results may differ from the reference program's by a relative error of at most 0.012.
The reference program's roundings to bfloat16 on the way count: a program that leaves them out, or rounds other values in their place, can miss the bound.
Values may be sent and summed in bfloat16 or wider, within the bound.
A program may use at most 128 MiB of HBM per device.

```python
import math
import jax
import jax.numpy as jnp
import numpy as np
from jax import lax

D = 512
FF = 2048
HEADS = 4
HD = 128
HALF = 9
KS = 3
VIDS = 8
LEN = 1024
SEQS = 32
MOST = 256


def block_scale(rng, shape, split, least, largest):
    gain, own = 1.0, jax.random.fold_in(rng, 6)
    for axis_at, parts in split:
        steps = jnp.exp(jax.random.uniform(jax.random.fold_in(own, axis_at), (parts,), jnp.float32, least / len(split), largest / len(split)))
        gain = gain * jnp.repeat(steps, shape[axis_at] // parts).reshape([-1 if axis == axis_at else 1 for axis in range(len(shape))])
    return gain


def profile(number_of, total, bound, slope):
    portions = [(1 << 20) // math.isqrt(rank ** slope) + 1 for rank in range(2, number_of + 1)]
    spare, given = total - bound - (number_of - 1), [1] * (number_of - 1)
    while spare > 0:
        free = [i for i in range(number_of - 1) if given[i] < bound]
        mass, remaining = sum([portions[i] for i in free]), spare
        for i in free:
            extra = min(bound - given[i], max(1, remaining * portions[i] // mass), spare)
            given[i] = given[i] + extra
            spare = spare - extra
    return np.array([bound] + given)


def ragged(stream_key, amount, total, reach, lean):
    if amount == 2:
        one = jax.random.randint(stream_key, (), max(1, total - reach), min(reach, total - 1) + 1)
        return jnp.stack([one, total - one])
    tallies = jnp.asarray(profile(amount, total, reach, lean), jnp.int32)
    pairs = (amount - 1) // 2
    giver, receiver = tallies[1:1 + 2 * pairs:2], tallies[2:2 + 2 * pairs:2]
    room = jnp.minimum(giver - 1, reach - receiver)
    moved = jax.random.randint(jax.random.fold_in(stream_key, 1), (pairs,), 0, 1 << 20) % (room + 1)
    tallies = tallies.at[1:1 + 2 * pairs:2].set(giver - moved).at[2:2 + 2 * pairs:2].set(receiver + moved)
    return tallies[jax.random.permutation(jax.random.fold_in(stream_key, 2), amount)]


def normal_values(own_key, extent, deviation, reach, split=(), kind=jnp.bfloat16):
    drawn = deviation * jax.random.normal(own_key, extent, jnp.float32)
    if split:
        drawn = drawn * block_scale(own_key, extent, split, -0.22, 0.18)
    return jnp.clip(drawn, -reach, reach).astype(kind)


def setup_inputs(seed: int = 0) -> dict:
    keys = jax.random.split(jax.random.key(seed), 12)
    return {
        "inputs": normal_values(keys[0], (SEQS, LEN, D), 1.0, 6.0, ((0, 4), (1, 8))),
        "lengths": jax.vmap(lambda own: ragged(own, VIDS, LEN, MOST, 2))(jax.random.split(keys[1], SEQS)).reshape((SEQS, VIDS)).astype(jnp.int32),
        "norm_gain": jnp.clip(1.0 + 0.18 * jax.random.normal(keys[2], (D,), jnp.float32), 0.099609375, 1.8984375).astype(jnp.bfloat16),
        "conv_kernel": normal_values(keys[3], (3, KS, D), KS ** -0.5, 3.5),
        "qkv_weight": normal_values(keys[4], (3, D, D), D ** -0.5, 0.25),
        "out_weight": normal_values(keys[5], (D, D), (D // 16) ** -0.5, 1.0),
        "mlp_gain": jnp.clip(1.0 + 0.18 * jax.random.normal(keys[6], (D,), jnp.float32), 0.099609375, 1.8984375).astype(jnp.bfloat16),
        "up_weight": normal_values(keys[7], (D, FF), D ** -0.5, 0.25),
        "down_weight": normal_values(keys[8], (FF, D), FF ** -0.5, 0.125),
        "layer_scale": jnp.clip(jnp.exp(jax.random.uniform(keys[9], (D,), jnp.float32, math.log(0.5), math.log(2.0))), 0.5, 2.0).astype(jnp.bfloat16),
        "cotangent": normal_values(keys[10], (SEQS, LEN, D), 1.0, 6.0, ((0, 4), (1, 8))),
    }


@jax.custom_vjp
def low(v):
    return lax.optimization_barrier(v.astype(jnp.bfloat16)).astype(jnp.float32)

@jax.custom_vjp
def low_back(v):
    return v

def low_keep(v):
    return (low(v), None)

def low_pass(kept, grad):
    return (grad,)

def back_keep(v):
    return (v, None)

def back_low(kept, grad):
    return (low(grad),)
low.defvjp(low_keep, low_pass)
low_back.defvjp(back_keep, back_low)

def matmul(left, right):
    return jnp.dot(left, right, precision=lax.Precision.HIGHEST, preferred_element_type=jnp.float32)

def layer_norm(values_in, scaling):
    average = lax.optimization_barrier(jnp.mean(values_in, axis=-1, keepdims=True))
    centered = values_in - average
    spread = lax.optimization_barrier(jnp.mean(centered * centered, axis=-1, keepdims=True))
    return centered * lax.rsqrt(spread + 1e-05) * scaling

def shifted(array, offset, fill):
    pads = [(HALF, HALF)] + [(0, 0)] * (array.ndim - 1)
    padded = jnp.pad(array, pads, constant_values=fill)
    return padded[HALF + offset:HALF + offset + array.shape[0]]

def linked(segment, offset):
    return shifted(segment, offset, -1) == segment

def segments_of(lengths):
    bounds = jnp.cumsum(lengths).astype(jnp.int32)
    positions = jnp.arange(LEN, dtype=jnp.int32)
    return lax.optimization_barrier(jnp.sum((positions[:, None] >= bounds[None, :]).astype(jnp.int32), axis=1)).astype(jnp.int32)

def forward(inputs_f, norm_gain, conv_kernel, qkv_weight, out_weight, mlp_gain, up_weight, down_weight, layer_scale, segment):
    frames = inputs_f.shape[0]
    normed = low(layer_norm(inputs_f, norm_gain))
    taps = [linked(segment, offset)[:, None] for offset in (-1, 0, 1)]
    streams = []
    for stream in range(3):
        mixed = jnp.zeros_like(normed)
        for column in range(3):
            mixed = mixed + conv_kernel[stream, column] * shifted(normed, column - 1, 0.0) * taps[column]
        streams.append(low(low_back(matmul(low(mixed), qkv_weight[stream]))))
    queries, key_rows, value_rows = streams
    temper = HD ** (-0.5)
    query_heads = queries.reshape(frames, HEADS, HD)
    raw = []
    masks = []
    for offset in range(-HALF, HALF + 1):
        moved = shifted(key_rows, offset, 0.0).reshape(frames, HEADS, HD)
        raw.append(lax.optimization_barrier(jnp.sum(query_heads * moved, axis=-1)) * temper)
        masks.append(linked(segment, offset))
    scores = low_back(jnp.stack(raw, axis=-1))
    allowed = jnp.stack(masks, axis=-1)[:, None, :]
    row_max = lax.optimization_barrier(jnp.max(jnp.where(allowed, scores, -1e+30), axis=-1, keepdims=True))
    raised = jnp.where(allowed, jnp.exp(jnp.where(allowed, scores - row_max, 0.0)), 0.0)
    probs = raised / lax.optimization_barrier(jnp.sum(raised, axis=-1, keepdims=True))
    weights_low = low(probs)
    attended = jnp.zeros((frames, HEADS, HD), jnp.float32)
    for index in range(2 * HALF + 1):
        moved = shifted(value_rows, index - HALF, 0.0).reshape(frames, HEADS, HD)
        attended = attended + weights_low[:, :, index, None] * moved
    attended_low = low(low_back(attended.reshape(frames, HEADS * HD)))
    branch = low_back(matmul(attended_low, out_weight))
    residual = inputs_f + branch
    normed_two = low(layer_norm(residual, mlp_gain))
    upper = low_back(matmul(normed_two, up_weight))
    hidden = low(jax.nn.gelu(upper))
    mlp_out = low_back(matmul(hidden, down_weight))
    return residual + layer_scale * mlp_out

def reference(inputs, lengths, norm_gain, conv_kernel, qkv_weight, out_weight, mlp_gain, up_weight, down_weight, layer_scale, cotangent):
    weights_f = tuple((w.astype(jnp.float32) for w in (norm_gain, conv_kernel, qkv_weight, out_weight, mlp_gain, up_weight, down_weight, layer_scale)))

    def per_sequence(running, sliced):
        seq_in, seq_lengths, seq_cot = sliced
        segment = segments_of(seq_lengths)

        def closed(inputs_f, *weights):
            return forward(inputs_f, *weights, segment)
        layer_out, pullback = jax.vjp(closed, seq_in.astype(jnp.float32), *weights_f)
        grads = pullback(seq_cot.astype(jnp.float32))
        running = tuple((a + b for a, b in zip(running, grads[1:])))
        return (running, (layer_out.astype(jnp.bfloat16), grads[0]))
    start = tuple((jnp.zeros_like(w) for w in weights_f))
    summed, (output, d_inputs) = lax.scan(per_sequence, start, (inputs, lengths, cotangent))
    return (output, d_inputs, summed[0], summed[1], summed[2], summed[3], summed[4], summed[5], summed[6], summed[7])
```

```python
import functools

import jax
import jax.numpy as jnp
from jax import lax
from jax.experimental import pallas as pl
from jax.experimental.pallas import tpu as pltpu
from jax.sharding import PartitionSpec as P

MESH = pl.DeviceIdType.MESH


def bit_orders(seq_size, tm_size):
    seq_bits = [("seq", b) for b in range(seq_size.bit_length() - 1)]
    tm_bits = [("tm", b) for b in range(tm_size.bit_length() - 1)]
    core, rest = tm_bits[:1], tm_bits[1:]
    first = core + seq_bits + rest
    second = core + seq_bits[::-1] + rest
    third = core + rest[:1] + seq_bits + rest[1:]
    fourth = core + rest[:1] + seq_bits[::-1] + rest[1:]
    return [first, second, third, first, second, fourth]


def partner_of(axis, bit):
    me = lax.axis_index(axis)
    mine = lax.rem(me // (1 << bit), 2)
    other = me + (1 - 2 * mine) * (1 << bit)
    if axis == "seq":
        return mine, (other, lax.axis_index("tm"))
    return mine, (lax.axis_index("seq"), other)


def add_rows(dst, dst_at, left, left_at, right, right_at, rows):
    step = min(rows, 32)

    def body(i, carry):
        off = pl.multiple_of(i * step, step)
        a = left[pl.ds(left_at + off, step), :].astype(jnp.float32)
        b = right[pl.ds(right_at + off, step), :].astype(jnp.float32)
        dst[pl.ds(dst_at + off, step), :] = (a + b).astype(jnp.bfloat16)
        return carry

    lax.fori_loop(0, rows // step, body, 0)


class Reducer:
    def __init__(self, orders, rows, part, acc, recv, full, sems):
        self.orders, self.rows = orders, rows
        self.part, self.acc, self.recv, self.full = part, acc, recv, full
        self.rs_send, self.rs_recv, self.ag_send, self.ag_recv = sems

    def levels(self):
        return len(self.orders[0])

    def start_of(self, level):
        return self.rows - (self.rows >> level)

    def source(self, unit, level):
        if level == 0:
            return self.part.at[unit], 0
        return self.acc.at[unit], self.start_of(level - 1)

    def scatter_copy(self, unit, level):
        mine, peer = partner_of(*self.orders[unit % len(self.orders)][level])
        half = self.rows >> (level + 1)
        ref, base = self.source(unit, level)
        off = pl.multiple_of(base + (1 - mine) * half, 16)
        return pltpu.make_async_remote_copy(
            src_ref=ref.at[pl.ds(off, half)],
            dst_ref=self.recv.at[unit, pl.ds(self.start_of(level), half)],
            send_sem=self.rs_send.at[unit, level],
            recv_sem=self.rs_recv.at[unit, level],
            device_id=peer,
            device_id_type=MESH,
        )

    def owned(self, unit, level):
        off = 0
        order = self.orders[unit % len(self.orders)]
        for i in range(level + 1):
            mine, _ = partner_of(*order[i])
            off = off + mine * (self.rows >> (i + 1))
        return pl.multiple_of(off, 16), self.rows >> (level + 1)

    def gather_copy(self, unit, level):
        _, peer = partner_of(*self.orders[unit % len(self.orders)][level])
        off, size = self.owned(unit, level)
        return pltpu.make_async_remote_copy(
            src_ref=self.full.at[unit, pl.ds(off, size)],
            dst_ref=self.full.at[unit, pl.ds(off, size)],
            send_sem=self.ag_send.at[unit, level],
            recv_sem=self.ag_recv.at[unit, level],
            device_id=peer,
            device_id_type=MESH,
        )

    def combine(self, unit, level):
        self.scatter_copy(unit, level).wait_recv()
        mine, _ = partner_of(*self.orders[unit % len(self.orders)][level])
        half = self.rows >> (level + 1)
        ref, base = self.source(unit, level)
        off = pl.multiple_of(base + mine * half, 16)
        if level == self.levels() - 1:
            at, _ = self.owned(unit, level)
            dst = self.full.at[unit]
        else:
            at, dst = self.start_of(level), self.acc.at[unit]
        add_rows(dst, at, ref, off, self.recv.at[unit], self.start_of(level), half)

    def wait_sends(self, unit):
        for level in range(self.levels()):
            self.scatter_copy(unit, level).wait_send()
            self.gather_copy(unit, level).wait_send()


def enter(bits):
    barrier = pltpu.get_barrier_semaphore()
    for axis, bit in bits:
        _, peer = partner_of(axis, bit)
        pl.semaphore_signal(barrier, inc=1, device_id=peer, device_id_type=MESH)
    pl.semaphore_wait(barrier, len(bits))


def reduce_kernel(
    orders, units, rows, part_hbm, small_ref, full_hbm, small_out,
    part, acc, recv, full, small_recv, small_acc,
    in_sem, out_sem, rs_send, rs_recv, ag_send, ag_recv, sm_send, sm_recv,
):
    levels = len(orders[0])
    red = Reducer(orders, rows, part, acc, recv, full, (rs_send, rs_recv, ag_send, ag_recv))
    loads = [pltpu.make_async_copy(part_hbm.at[u], part.at[u], in_sem.at[u]) for u in range(units)]
    for load in loads:
        load.start()
    enter(orders[0])

    def small_copy(level):
        _, peer = partner_of(*orders[0][level])
        src = small_ref if level == 0 else small_acc.at[level - 1]
        return pltpu.make_async_remote_copy(
            src_ref=src, dst_ref=small_recv.at[level],
            send_sem=sm_send.at[level], recv_sem=sm_recv.at[level],
            device_id=peer, device_id_type=MESH,
        )

    for level in range(levels):
        for u in range(units):
            if level == 0:
                loads[u].wait()
            else:
                red.combine(u, level - 1)
            red.scatter_copy(u, level).start()
        if level > 0:
            small_copy(level - 1).wait_recv()
            prev = small_ref[...] if level == 1 else small_acc[level - 2]
            small_acc[level - 1] = prev + small_recv[level - 1]
        small_copy(level).start()
    small_copy(levels - 1).wait_recv()
    small_out[...] = small_acc[levels - 2] + small_recv[levels - 1]
    for level in range(levels - 1, -1, -1):
        for u in range(units):
            if level == levels - 1:
                red.combine(u, level)
            else:
                red.gather_copy(u, level + 1).wait_recv()
            red.gather_copy(u, level).start()
    outs = [pltpu.make_async_copy(full.at[u], full_hbm.at[u], out_sem.at[u]) for u in range(units)]
    for u in range(units):
        red.gather_copy(u, 0).wait_recv()
        outs[u].start()
    for level in range(levels):
        small_copy(level).wait_send()
    for u in range(units):
        red.wait_sends(u)
        outs[u].wait()


def reduce_all(parts, small, seq_size, tm_size):
    units, rows, cols = parts.shape
    orders = bit_orders(seq_size, tm_size)
    levels = len(orders[0])
    buf = pltpu.VMEM((units, rows, cols), jnp.bfloat16)
    dma = pltpu.SemaphoreType.DMA
    return pl.pallas_call(
        functools.partial(reduce_kernel, orders, units, rows),
        out_shape=(
            jax.ShapeDtypeStruct(parts.shape, jnp.bfloat16),
            jax.ShapeDtypeStruct(small.shape, jnp.float32),
        ),
        in_specs=[
            pl.BlockSpec(memory_space=pl.ANY),
            pl.BlockSpec(memory_space=pltpu.VMEM),
        ],
        out_specs=(
            pl.BlockSpec(memory_space=pl.ANY),
            pl.BlockSpec(memory_space=pltpu.VMEM),
        ),
        scratch_shapes=[
            buf, buf, buf, buf,
            pltpu.VMEM((levels,) + small.shape, jnp.float32),
            pltpu.VMEM((levels,) + small.shape, jnp.float32),
            dma((units,)), dma((units,)),
            dma((units, levels)), dma((units, levels)),
            dma((units, levels)), dma((units, levels)),
            dma((levels,)), dma((levels,)),
        ],
        compiler_params=pltpu.CompilerParams(
            collective_id=0, has_side_effects=True, vmem_limit_bytes=48 << 20
        ),
    )(parts, small)


HEADS = 4
HD = 128
HALF = 9


def extended(shard, sides, width):
    for axis, dim in sides:
        size, length = (lax.axis_size(axis), shard.shape[dim])
        up = [(i, (i + 1) % size) for i in range(size - 1)]
        down = [(j, i) for i, j in up]
        last = lax.slice_in_dim(shard, length - width, length, axis=dim)
        first = lax.slice_in_dim(shard, 0, width, axis=dim)
        before = lax.ppermute(last, axis, up)
        after = lax.ppermute(first, axis, down)
        shard = jnp.concatenate([before, shard, after], axis=dim)
    return shard


def from_behind(shard, axis, by):
    length = lax.axis_size(axis)
    pairs = [(i, i + by) for i in range(length) if 0 <= i + by < length]
    return lax.ppermute(shard, axis, pairs)


def layer_norm(values_in, scaling):
    average = jnp.mean(values_in, axis=-1, keepdims=True)
    centered = values_in - average
    spread = jnp.mean(centered * centered, axis=-1, keepdims=True)
    return centered * lax.rsqrt(spread + 1e-05) * scaling


def segment_rows(lengths, start_pos, row_count, seq_length):
    positions = start_pos + jnp.arange(row_count, dtype=jnp.int32)
    bounds = jnp.cumsum(lengths, axis=1)
    segment = jnp.sum((positions[None, :, None] >= bounds[:, None, :]).astype(jnp.int32), axis=2)
    inside = (positions >= 0) & (positions < seq_length)
    return jnp.where(inside[None, :], segment, -1)


def depthwise(window, kernel, segment):
    row_count = window.shape[1] - 2
    centre = segment[:, 1 : row_count + 1]
    mixed = jnp.zeros((window.shape[0], row_count, window.shape[2]), jnp.float32)
    for column in range(3):
        nearby = segment[:, column : column + row_count]
        joined = (nearby == centre) & (nearby >= 0)
        mixed = mixed + kernel[column] * window[:, column : column + row_count] * joined[..., None]
    return mixed


def project(acts, weight):
    return jnp.einsum("std,de->ste", acts, weight, preferred_element_type=jnp.float32)


def shards(
    inputs,
    lengths,
    norm_gain,
    conv_kernel,
    qkv_weight,
    out_weight,
    mlp_gain,
    up_weight,
    down_weight,
    layer_scale,
    cotangent,
):
    sequences, frames, features = inputs.shape
    reach = HALF
    seq_length = frames * lax.axis_size("tm")
    start_pos = lax.axis_index("tm") * frames
    seg_wide = segment_rows(lengths, start_pos - reach - 1, frames + 2 * reach + 2, seq_length)
    seg_own = seg_wide[:, reach : frames + reach + 2]
    gain_one = norm_gain.astype(jnp.float32)
    kernel = conv_kernel.astype(jnp.float32)
    inputs_f = inputs.astype(jnp.float32)
    normed = layer_norm(inputs_f, gain_one).astype(jnp.bfloat16)
    window = extended(normed, (("tm", 1),), 1)
    window_f = window.astype(jnp.float32)
    act_q = depthwise(window_f, kernel[0], seg_own).astype(jnp.bfloat16)
    act_k = depthwise(window_f, kernel[1], seg_own).astype(jnp.bfloat16)
    act_v = depthwise(window_f, kernel[2], seg_own).astype(jnp.bfloat16)
    queries = project(act_q, qkv_weight[0]).astype(jnp.bfloat16)
    key_value = jnp.concatenate(
        [project(act_k, qkv_weight[1]), project(act_v, qkv_weight[2])], axis=-1
    ).astype(jnp.bfloat16)
    wider = extended(key_value, (("tm", 1),), reach)
    key_rows = wider[..., :features]
    value_rows = wider[..., features:]
    span = frames + 2 * reach
    seg_keys = seg_wide[:, 1 : span + 1]
    seg_query = seg_wide[:, reach + 1 : frames + reach + 1]
    offsets = (
        jnp.arange(span, dtype=jnp.int32)[None, :] - jnp.arange(frames, dtype=jnp.int32)[:, None]
    )
    in_band = (offsets >= 0) & (offsets <= 2 * reach)
    allowed = (
        in_band[None]
        & (seg_keys[:, None, :] == seg_query[:, :, None])
        & (seg_keys[:, None, :] >= 0)
    )
    allowed = allowed[:, None]
    temper = HD ** (-0.5)
    query_heads = queries.reshape(sequences, frames, HEADS, HD)
    key_heads = key_rows.reshape(sequences, span, HEADS, HD)
    value_heads = value_rows.reshape(sequences, span, HEADS, HD)
    scores = (
        jnp.einsum("sthd,sjhd->shtj", query_heads, key_heads, preferred_element_type=jnp.float32)
        * temper
    )
    row_max = jnp.max(jnp.where(allowed, scores, -1e30), axis=-1, keepdims=True)
    raised = jnp.where(allowed, jnp.exp(jnp.where(allowed, scores - row_max, 0.0)), 0.0)
    row_sum = jnp.sum(raised, axis=-1, keepdims=True)
    probs = raised / row_sum
    log_total = row_max + jnp.log(row_sum)
    weights_low = probs.astype(jnp.bfloat16)
    attended = jnp.einsum(
        "shtj,sjhd->sthd", weights_low, value_heads, preferred_element_type=jnp.float32
    )
    act_o = attended.reshape(sequences, frames, features).astype(jnp.bfloat16)
    branch = project(act_o, out_weight)
    residual = inputs_f + branch
    gain_two = mlp_gain.astype(jnp.float32)
    normed_two = layer_norm(residual, gain_two).astype(jnp.bfloat16)
    upper = project(normed_two, up_weight)
    hidden = jax.nn.gelu(upper).astype(jnp.bfloat16)
    mlp_out = project(hidden, down_weight)
    scale_f = layer_scale.astype(jnp.float32)
    output = (residual + scale_f * mlp_out).astype(jnp.bfloat16)
    grad_out = cotangent.astype(jnp.float32)
    d_scale = jnp.sum(grad_out * mlp_out, axis=(0, 1))
    d_mlp = (grad_out * scale_f).astype(jnp.bfloat16)
    d_down = jnp.einsum("stf,std->fd", hidden, d_mlp, preferred_element_type=jnp.float32)
    d_hidden = jnp.einsum("std,fd->stf", d_mlp, down_weight, preferred_element_type=jnp.float32)
    gelu_pull = jax.vjp(jax.nn.gelu, upper)[1]
    d_upper = gelu_pull(d_hidden)[0].astype(jnp.bfloat16)
    d_up = jnp.einsum("std,stf->df", normed_two, d_upper, preferred_element_type=jnp.float32)
    d_normed_two = jnp.einsum("stf,df->std", d_upper, up_weight, preferred_element_type=jnp.float32)
    second_pull = jax.vjp(layer_norm, residual, gain_two)[1]
    d_resid_part, d_gain_two = second_pull(d_normed_two)
    d_residual = grad_out + d_resid_part
    d_branch = d_residual.astype(jnp.bfloat16)
    d_out = jnp.einsum("std,ste->de", act_o, d_branch, preferred_element_type=jnp.float32)
    d_attended = jnp.einsum("ste,de->std", d_branch, out_weight, preferred_element_type=jnp.float32)
    d_attended = d_attended.astype(jnp.bfloat16).reshape(sequences, frames, HEADS, HD)
    again = (
        jnp.einsum("sthd,sjhd->shtj", query_heads, key_heads, preferred_element_type=jnp.float32)
        * temper
    )
    probs_again = jnp.where(allowed, jnp.exp(jnp.where(allowed, again - log_total, 0.0)), 0.0)
    weights_again = probs_again.astype(jnp.bfloat16)
    d_weights = jnp.einsum(
        "sthd,sjhd->shtj", d_attended, value_heads, preferred_element_type=jnp.float32
    )
    row_dot = jnp.sum(probs_again * d_weights, axis=-1, keepdims=True)
    d_scores = (probs_again * (d_weights - row_dot)).astype(jnp.bfloat16)
    d_query = (
        jnp.einsum("shtj,sjhd->sthd", d_scores, key_heads, preferred_element_type=jnp.float32)
        * temper
    )
    d_keys = (
        jnp.einsum("shtj,sthd->sjhd", d_scores, query_heads, preferred_element_type=jnp.float32)
        * temper
    )
    d_values = jnp.einsum(
        "shtj,sthd->sjhd", weights_again, d_attended, preferred_element_type=jnp.float32
    )
    stacked = jnp.concatenate(
        [d_keys.reshape(sequences, span, features), d_values.reshape(sequences, span, features)],
        axis=-1,
    )
    from_high = from_behind(stacked[:, :reach].astype(jnp.bfloat16), "tm", -1).astype(jnp.float32)
    from_low = from_behind(stacked[:, frames + reach :].astype(jnp.bfloat16), "tm", 1).astype(
        jnp.float32
    )
    own_rows = stacked[:, reach : frames + reach]
    own_rows = own_rows.at[:, :reach].add(from_low).at[:, frames - reach :].add(from_high)
    d_query_low = d_query.reshape(sequences, frames, features).astype(jnp.bfloat16)
    d_key_low = own_rows[..., :features].astype(jnp.bfloat16)
    d_value_low = own_rows[..., features:].astype(jnp.bfloat16)
    d_qkv = jnp.stack(
        [
            jnp.einsum("std,ste->de", act_q, d_query_low, preferred_element_type=jnp.float32),
            jnp.einsum("std,ste->de", act_k, d_key_low, preferred_element_type=jnp.float32),
            jnp.einsum("std,ste->de", act_v, d_value_low, preferred_element_type=jnp.float32),
        ],
        axis=0,
    )
    d_mixed = (
        jnp.einsum("ste,de->std", d_query_low, qkv_weight[0], preferred_element_type=jnp.float32),
        jnp.einsum("ste,de->std", d_key_low, qkv_weight[1], preferred_element_type=jnp.float32),
        jnp.einsum("ste,de->std", d_value_low, qkv_weight[2], preferred_element_type=jnp.float32),
    )

    def three_convs(window_in, kernels):
        return (
            depthwise(window_in, kernels[0], seg_own),
            depthwise(window_in, kernels[1], seg_own),
            depthwise(window_in, kernels[2], seg_own),
        )

    conv_pull = jax.vjp(three_convs, window.astype(jnp.float32), kernel)[1]
    d_window, d_kernel = conv_pull(d_mixed)
    got_high = from_behind(d_window[:, :1], "tm", -1)
    got_low = from_behind(d_window[:, frames + 1 :], "tm", 1)
    d_normed = d_window[:, 1 : frames + 1].at[:, :1].add(got_low).at[:, frames - 1 :].add(got_high)
    first_pull = jax.vjp(layer_norm, inputs_f, gain_one)[1]
    d_in_part, d_gain_one = first_pull(d_normed)
    d_inputs = d_residual + d_in_part
    cols = features
    pack = lambda w: w.astype(jnp.bfloat16)
    d_up_rows = pack(d_up).reshape(cols, -1, cols).transpose(1, 0, 2).reshape(-1, cols)
    flat = jnp.concatenate(
        [pack(d_down), d_up_rows, pack(d_out), pack(d_qkv).reshape(-1, cols)], axis=0
    )
    sizes = (lax.axis_size("seq"), lax.axis_size("tm"))
    rows = max(512, 16 * sizes[0] * sizes[1])
    small = jnp.concatenate(
        [
            d_kernel.reshape(9, cols), d_gain_one[None], d_gain_two[None], d_scale[None],
            jnp.zeros((4, cols), jnp.float32),
        ],
        axis=0,
    )
    full, small = reduce_all(flat.reshape(-1, rows, cols), small, *sizes)
    full = full.reshape(-1, cols)
    hidden_size = down_weight.shape[0]
    wide = lambda w: w.astype(jnp.float32)
    sum_down = wide(full[:hidden_size])
    sum_up = wide(
        full[hidden_size : 2 * hidden_size].reshape(-1, cols, cols).transpose(1, 0, 2)
    ).reshape(cols, hidden_size)
    sum_out = wide(full[2 * hidden_size : 2 * hidden_size + cols])
    sum_qkv = wide(full[2 * hidden_size + cols :]).reshape(3, cols, cols)
    return (
        output, d_inputs, small[9], small[:9].reshape(3, 3, cols), sum_qkv, sum_out,
        small[10], sum_up, sum_down, small[11],
    )


def solution(mesh):
    placed = (
        P("seq", "tm", None),
        P("seq", None),
        P(),
        P(),
        P(),
        P(),
        P(),
        P(),
        P(),
        P(),
        P("seq", "tm", None),
    )
    return jax.shard_map(
        shards,
        mesh=mesh,
        in_specs=placed,
        out_specs=(
            P("seq", "tm", None),
            P("seq", "tm", None),
            P(),
            P(),
            P(),
            P(),
            P(),
            P(),
            P(),
            P(),
        ),
        check_vma=False,
    )
```

```python
import functools

import jax
import jax.numpy as jnp
from jax import lax
from jax.experimental import pallas as pl
from jax.experimental.pallas import tpu as pltpu
from jax.sharding import PartitionSpec as P

HEADS = 4
HD = 128
HALF = 9
HALO = 16
PAD = 8
QB = 64
KB = QB + 2 * HALO
EPS = 1e-05
MESH = pl.DeviceIdType.MESH
F32 = jnp.float32
BF16 = jnp.bfloat16


def bit_orders(seq_size, tm_size):
    seq_bits = [("seq", b) for b in range(seq_size.bit_length() - 1)]
    tm_bits = [("tm", b) for b in range(tm_size.bit_length() - 1)]
    core, rest = tm_bits[:1], tm_bits[1:]
    first = core + seq_bits + rest
    second = core + seq_bits[::-1] + rest
    third = core + rest[:1] + seq_bits + rest[1:]
    fourth = core + rest[:1] + seq_bits[::-1] + rest[1:]
    return [first, second, third, first, second, fourth, first, second, third, first, second, fourth]


def partner_of(axis, bit):
    me = lax.axis_index(axis)
    mine = lax.rem(me // (1 << bit), 2)
    other = me + (1 - 2 * mine) * (1 << bit)
    if axis == "seq":
        return mine, (other, lax.axis_index("tm"))
    return mine, (lax.axis_index("seq"), other)


def neighbour(step, size):
    return (lax.axis_index("seq"), lax.rem(lax.axis_index("tm") + step + size, size))


class Reducer:
    def __init__(self, orders, rows, part, recv, fulls, sems):
        self.orders, self.rows = orders, rows
        self.part, self.recv, self.fulls = part, recv, fulls
        self.rs_send, self.rs_recv, self.ag_send, self.ag_recv = sems
        self.levels = len(orders[0])

    def landing(self, level):
        return self.rows - (self.rows >> level)

    def owned(self, unit, level):
        off = 0
        for i in range(level + 1):
            mine, _ = partner_of(*self.orders[unit][i])
            off = off + mine * (self.rows >> (i + 1))
        return off, self.rows >> (level + 1)

    def scatter_copy(self, unit, level):
        mine, peer = partner_of(*self.orders[unit][level])
        half = self.rows >> (level + 1)
        base = self.owned(unit, level - 1)[0] if level else 0
        off = pl.multiple_of(base + (1 - mine) * half, 16)
        return pltpu.make_async_remote_copy(
            src_ref=self.part.at[unit, pl.ds(off, half)],
            dst_ref=self.recv.at[unit, pl.ds(self.landing(level), half)],
            send_sem=self.rs_send.at[unit, level],
            recv_sem=self.rs_recv.at[unit, level],
            device_id=peer,
            device_id_type=MESH,
        )

    def full(self, unit):
        held = self.fulls[0].shape[0] // self.rows
        return self.fulls[unit // held], (unit % held) * self.rows

    def gather_copy(self, unit, level):
        _, peer = partner_of(*self.orders[unit][level])
        off, size = self.owned(unit, level)
        ref, start = self.full(unit)
        region = ref.at[pl.ds(pl.multiple_of(start + off, 16), size)]
        return pltpu.make_async_remote_copy(
            src_ref=region,
            dst_ref=region,
            send_sem=self.ag_send.at[unit, level],
            recv_sem=self.ag_recv.at[unit, level],
            device_id=peer,
            device_id_type=MESH,
        )

    def combine(self, unit, level):
        self.scatter_copy(unit, level).wait_recv()
        off, half = self.owned(unit, level)
        step = min(half, 32)

        def body(i, carry):
            here = pl.ds(pl.multiple_of(off + i * step, 16), step)
            there = pl.ds(pl.multiple_of(self.landing(level) + i * step, 16), step)
            total = self.part[unit, here, :].astype(F32) + self.recv[unit, there, :].astype(F32)
            if level == self.levels - 1:
                ref, start = self.full(unit)
                ref[pl.ds(pl.multiple_of(start + off + i * step, 16), step), :] = total.astype(BF16)
            else:
                self.part[unit, here, :] = total.astype(BF16)
            return carry

        lax.fori_loop(0, half // step, body, 0)

    def tick(self, unit, i):
        if i == 0:
            self.scatter_copy(unit, 0).start()
        elif i < self.levels:
            self.combine(unit, i - 1)
            self.scatter_copy(unit, i).start()
        elif i == self.levels:
            self.combine(unit, i - 1)
            self.gather_copy(unit, self.levels - 1).start()
        elif i < 2 * self.levels:
            level = 2 * self.levels - 1 - i
            self.gather_copy(unit, level + 1).wait_recv()
            self.gather_copy(unit, level).start()
        else:
            self.gather_copy(unit, 0).wait_recv()

    def wait_sends(self, unit):
        for level in range(self.levels):
            self.scatter_copy(unit, level).wait_send()
            self.gather_copy(unit, level).wait_send()


def enter(bits, tm_size):
    barrier = pltpu.get_barrier_semaphore()
    peers = [partner_of(axis, bit)[1] for axis, bit in bits]
    peers = peers + [neighbour(1, tm_size), neighbour(-1, tm_size)]
    for peer in peers:
        pl.semaphore_signal(barrier, inc=1, device_id=peer, device_id_type=MESH)
    pl.semaphore_wait(barrier, len(peers))


def nn(a, b):
    return lax.dot_general(a, b, (((1,), (0,)), ((), ())), preferred_element_type=F32)


def nt(a, b):
    return lax.dot_general(a, b, (((1,), (1,)), ((), ())), preferred_element_type=F32)


def tn(a, b):
    return lax.dot_general(a, b, (((0,), (0,)), ((), ())), preferred_element_type=F32)


def moments(v):
    mean = jnp.mean(v, axis=-1, keepdims=True)
    centered = v - mean
    var = jnp.mean(centered * centered, axis=-1, keepdims=True)
    return centered, lax.rsqrt(var + EPS)


def fold(v):
    rows, cols = v.shape
    return jnp.sum(v.reshape(rows // 8, 8, cols), axis=0)


def gelu_pair(v):
    c = 0.7978845608028654
    square = v * v
    inner = v * (c + (c * 0.044715) * square)
    t = jnp.tanh(inner)
    half = 0.5 * (1.0 + t)
    slope = half + (0.5 * v) * (1.0 - t * t) * (c + (3.0 * 0.044715 * c) * square)
    return v * half, slope


def loop(count, body):
    def step(i, carry):
        body(i)
        return carry

    lax.fori_loop(0, count, step, 0)


def layer_kernel(cfg, *refs):
    (
        lengths, x_hbm, params, wqkv_hbm, wout_hbm, wup_hbm, wdown_hbm, cot_hbm,
        out_hbm, din_hbm, down_hbm, up_hbm, outw_hbm, qkvw_hbm, small_out,
        x, cot, wqkv, wout, wup, wdown, halo_lo, halo_hi, nf, link,
        act_q, act_k, act_v, qs, ks, vs, prob, att, res, n2, dm, hid, du, dbr, da, outs,
        dke, dve, dmx, dnb, msg_hi, msg_lo, got_lo, got_hi, dq_hi, dq_lo, dq_got_lo, dq_got_hi,
        edge, edge_mix, sums, small_cur, small_recv,
        part, recv,
        in_sem, out_sem, halo_send, halo_recv, rs_send, rs_recv, ag_send, ag_recv, sm_send, sm_recv,
    ) = refs
    orders, rows, seqs, frames, feats, ff, tm_size = cfg
    units = len(orders)
    levels = len(orders[0])
    ext = frames + 2 * HALO
    own = PAD + HALO
    seq_length = frames * tm_size
    vids = lengths.shape[1]
    temper = HD ** (-0.5)
    lanes = [pl.ds(c * 128, 128) for c in range(feats // 128)]
    blocks = frames // QB
    pairs = seqs // 2
    per_unit = rows // feats
    base = lax.axis_index("tm") * frames
    red = Reducer(orders, rows, part, recv, (hid, du), (rs_send, rs_recv, ag_send, ag_recv))

    loads = [
        pltpu.make_async_copy(src, dst, in_sem.at[i])
        for i, (src, dst) in enumerate(
            [(x_hbm, x), (wqkv_hbm, wqkv), (wout_hbm, wout), (wup_hbm, wup), (wdown_hbm, wdown), (cot_hbm, cot)]
        )
    ]
    for load in loads:
        load.start()

    def across(src, dst, i, step):
        return pltpu.make_async_remote_copy(
            src_ref=src, dst_ref=dst, send_sem=halo_send.at[i], recv_sem=halo_recv.at[i],
            device_id=neighbour(step, tm_size), device_id_type=MESH,
        )

    enter(orders[0], tm_size)
    to_next = across(x_hbm.at[:, pl.ds(frames - HALO, HALO)], halo_lo, 0, 1)
    to_prev = across(x_hbm.at[:, pl.ds(0, HALO)], halo_hi, 1, -1)
    to_next.start()
    to_prev.start()

    sums[...] = jnp.zeros_like(sums)

    def bounds_of(s):
        total, found = 0, []
        for j in range(vids):
            total = total + lengths[s, j]
            found.append(total)
        return found

    gain_one = params[pl.ds(9, 1), :]
    gain_two = params[pl.ds(10, 1), :]
    scale = params[pl.ds(11, 1), :]

    def normed_rows(rows_in):
        centered, r = moments(rows_in.astype(F32))
        return (centered * r * gain_one).astype(BF16).astype(F32)

    loads[0].wait()

    def norm_own(s):
        nf[s, pl.ds(own, frames), :] = normed_rows(x[s])
        zero = jnp.zeros((PAD, feats), F32)
        nf[s, pl.ds(0, PAD), :] = zero
        nf[s, pl.ds(PAD + ext, PAD), :] = zero
        pos = base - own + lax.broadcasted_iota(jnp.int32, (ext + 2 * PAD, 128), 0)
        cut = pos == 0
        for bound in bounds_of(s):
            cut = cut | (pos == bound)
        link[s] = jnp.where(cut, 0.0, 1.0)

    loop(seqs, norm_own)
    to_next.wait_recv()
    to_prev.wait_recv()

    def norm_halo(s):
        nf[s, pl.ds(PAD, HALO), :] = normed_rows(halo_lo[s])
        nf[s, pl.ds(own + frames, HALO), :] = normed_rows(halo_hi[s])

    loop(seqs, norm_halo)
    loads[1].wait()

    def mix_project(t):
        for i in range(2):
            s = 2 * t + i
            before_on = link[s, pl.ds(PAD, ext), :]
            after_on = link[s, pl.ds(PAD + 1, ext), :]
            for lane in lanes:
                before = nf[s, pl.ds(PAD - 1, ext), lane] * before_on
                centre = nf[s, pl.ds(PAD, ext), lane]
                after = nf[s, pl.ds(PAD + 1, ext), lane] * after_on
                for n, dst in enumerate((act_q, act_k, act_v)):
                    k0, k1, k2 = (params[pl.ds(3 * n + c, 1), lane] for c in range(3))
                    mixed = (k0 * before + k1 * centre + k2 * after).astype(BF16)
                    if n == 0:
                        dst[s, :, lane] = mixed[HALO : HALO + frames]
                    else:
                        dst[s, :, lane] = mixed
        two = pl.ds(2 * t, 2)
        for n, (src, dst) in enumerate(((act_q, qs), (act_k, ks), (act_v, vs))):
            size = src.shape[1]
            value = nn(src[two].reshape(2 * size, feats), wqkv[n])
            dst[two] = value.astype(BF16).reshape(2, size, feats)

    loop(pairs, mix_project)

    def attend(s):
        bounds = bounds_of(s)
        row = lax.broadcasted_iota(jnp.int32, (QB, KB), 0)
        col = lax.broadcasted_iota(jnp.int32, (QB, KB), 1) - HALO
        band = (col - row <= HALF) & (col - row >= -HALF)
        for b in range(blocks):
            pos_q = row + (base + b * QB)
            pos_k = col + (base + b * QB)
            seg_q = jnp.zeros((QB, KB), jnp.int32)
            seg_k = jnp.zeros((QB, KB), jnp.int32)
            for bound in bounds:
                seg_q = seg_q + (pos_q >= bound).astype(jnp.int32)
                seg_k = seg_k + (pos_k >= bound).astype(jnp.int32)
            allowed = band & (seg_q == seg_k) & (pos_k >= 0) & (pos_k < seq_length)
            for h in range(HEADS):
                head = pl.ds(h * HD, HD)
                q = qs[s, pl.ds(b * QB, QB), head]
                k = ks[s, pl.ds(b * QB, KB), head]
                v = vs[s, pl.ds(b * QB, KB), head]
                scores = jnp.where(allowed, nt(q, k) * temper, -1e30)
                top = jnp.max(scores, axis=-1, keepdims=True)
                raised = jnp.where(allowed, jnp.exp(scores - top), 0.0)
                probs = raised / jnp.sum(raised, axis=-1, keepdims=True)
                prob[s * blocks + b, h] = probs
                att[s, pl.ds(b * QB, QB), head] = nn(probs.astype(BF16), v).astype(BF16)

    loop(seqs, attend)
    for load in loads[2:]:
        load.wait()
    tall = 2 * frames
    chunk = feats
    tokens = seqs * frames
    out_copies = [
        pltpu.make_async_copy(outs.at[pl.ds(2 * t, 2)], out_hbm.at[pl.ds(2 * t, 2)], out_sem.at[t])
        for t in range(pairs)
    ]

    def feed_forward(t):
        two = pl.ds(2 * t, 2)
        flat = lambda ref: ref[two].reshape(tall, ref.shape[2])
        residual = flat(x).astype(F32) + nn(flat(att), wout[...])
        res[two] = residual.reshape(2, frames, feats)
        centered, r = moments(residual)
        n2[two] = (centered * r * gain_two).astype(BF16).reshape(2, frames, feats)
        dm[two] = (flat(cot).astype(F32) * scale).astype(BF16).reshape(2, frames, feats)

        def part_ff(j):
            cols = pl.ds(pl.multiple_of(j * chunk, chunk), chunk)
            upper = nn(flat(n2), wup[:, cols])
            d_hidden = nt(flat(dm), wdown[cols, :])
            value, slope = gelu_pair(upper)
            tile = pl.ds(pl.multiple_of(j * tokens + t * tall, tall), tall)
            hid[tile, :] = value.astype(BF16)
            du[tile, :] = (slope * d_hidden).astype(BF16)

        loop(ff // chunk, part_ff)
        mlp_out, e = 0.0, 0.0
        for j in range(ff // chunk):
            tile = pl.ds(pl.multiple_of(j * tokens + t * tall, tall), tall)
            mlp_out = mlp_out + nn(hid[tile, :], wdown[pl.ds(j * chunk, chunk), :])
            e = e + nt(du[tile, :], wup[:, pl.ds(j * chunk, chunk)])
        residual = flat(res)
        cotan = flat(cot).astype(F32)
        outs[two] = (residual + scale * mlp_out).astype(BF16).reshape(2, frames, feats)
        sums[11] += fold(cotan * mlp_out)
        centered, r = moments(residual)
        xhat = centered * r
        sums[10] += fold(e * xhat)
        eg = e * gain_two
        d_res = cotan + r * (
            eg - jnp.mean(eg, axis=-1, keepdims=True) - xhat * jnp.mean(eg * xhat, axis=-1, keepdims=True)
        )
        res[two] = d_res.reshape(2, frames, feats)
        d_branch = d_res.astype(BF16)
        dbr[two] = d_branch.reshape(2, frames, feats)
        da[two] = nt(d_branch, wout[...]).astype(BF16).reshape(2, frames, feats)

    loop(pairs, feed_forward)
    for copy in out_copies:
        copy.start()

    whole = lambda ref: ref[...].reshape(seqs * frames, ref.shape[2])

    def place(block, value):
        part[block // per_unit, pl.ds((block % per_unit) * feats, feats), :] = value.astype(BF16)

    ff_blocks = ff // feats

    def begin(block):
        if block % per_unit == per_unit - 1:
            red.tick(block // per_unit, 0)

    for j in range(ff_blocks):
        place(j, tn(hid[pl.ds(j * tokens, tokens), :], whole(dm)))
        begin(j)
    for j in range(ff_blocks):
        place(ff_blocks + j, tn(whole(n2), du[pl.ds(j * tokens, tokens), :]))
        begin(ff_blocks + j)
    place(2 * ff_blocks, tn(whole(att), whole(dbr)))
    begin(2 * ff_blocks)

    dq = dm
    dkl, dvl = n2, att

    def attend_back(s):
        for h in range(HEADS):
            head = pl.ds(h * HD, HD)
            d_k, d_v = [], []
            for b in range(blocks):
                here = pl.ds(b * QB, QB)
                keys = pl.ds(b * QB, KB)
                q, k, v = qs[s, here, head], ks[s, keys, head], vs[s, keys, head]
                d_att = da[s, here, head]
                probs = prob[s * blocks + b, h]
                d_weights = nt(d_att, v)
                dot = jnp.sum(probs * d_weights, axis=-1, keepdims=True)
                d_scores = (probs * (d_weights - dot)).astype(BF16)
                dq[s, here, head] = (nn(d_scores, k) * temper).astype(BF16)
                d_k.append(tn(d_scores, q) * temper)
                d_v.append(tn(probs.astype(BF16), d_att))
            for dst, got in ((dke, d_k), (dve, d_v)):
                tail = None
                for b in range(blocks):
                    value = got[b]
                    first = value[: KB - QB] if tail is None else value[: KB - QB] + tail
                    dst[s, pl.ds(b * QB, KB - QB), head] = first
                    dst[s, pl.ds(b * QB + KB - QB, 2 * QB - KB), head] = value[KB - QB : QB]
                    tail = value[QB:]
                dst[s, pl.ds(blocks * QB, KB - QB), head] = tail
        for i, src in enumerate((dke, dve)):
            cols = pl.ds(i * feats, feats)
            msg_hi[s, :, cols] = src[s, pl.ds(HALO + frames - 1, HALO), :].astype(BF16)
            msg_lo[s, :, cols] = src[s, pl.ds(1, HALO), :].astype(BF16)
        dq_hi[pl.ds(s, 1), :] = dq[s, pl.ds(frames - 16, 16), :].astype(F32)[15:16]
        dq_lo[pl.ds(s, 1), :] = dq[s, pl.ds(0, 16), :].astype(F32)[0:1]

    loop(seqs, attend_back)
    exchange = [
        across(msg_hi, got_lo, 2, 1), across(msg_lo, got_hi, 3, -1),
        across(dq_hi, dq_got_lo, 4, 1), across(dq_lo, dq_got_hi, 5, -1),
    ]
    for copy in exchange:
        copy.start()
    place(2 * ff_blocks + 1, tn(whole(act_q), whole(dq)))
    begin(2 * ff_blocks + 1)
    for copy in exchange:
        copy.wait_recv()
    edge[0, pl.ds(0, seqs), :] = dq_got_lo[...]
    edge[0, pl.ds(seqs, seqs), :] = dq_got_hi[...]

    def settle(s):
        for i, (src, dst) in enumerate(((dke, dkl), (dve, dvl))):
            cols = pl.ds(i * feats, feats)
            low = pl.ds(HALO - 1, HALO)
            high = pl.ds(HALO + frames - HALO + 1, HALO)
            src[s, low, :] = src[s, low, :] + got_lo[s, :, cols].astype(F32)
            src[s, high, :] = src[s, high, :] + got_hi[s, :, cols].astype(F32)
            dst[s] = src[s, pl.ds(HALO, frames), :].astype(BF16)
            edge[i + 1, pl.ds(s, 1), :] = src[s, pl.ds(HALO - 1, 1), :]
            edge[i + 1, pl.ds(seqs + s, 1), :] = src[s, pl.ds(HALO + frames, 1), :]

    loop(seqs, settle)
    inner = lambda ref: ref[:, pl.ds(HALO, frames), :].reshape(seqs * frames, feats)
    place(2 * ff_blocks + 2, tn(inner(act_k), whole(dkl)))
    begin(2 * ff_blocks + 2)
    place(2 * ff_blocks + 3, tn(inner(act_v), whole(dvl)))
    begin(2 * ff_blocks + 3)
    for n in range(3):
        edge_mix[n] = nt(edge[n].astype(BF16), wqkv[n])

    def input_grads(t):
        two = pl.ds(2 * t, 2)
        for n, src in enumerate((dq, dkl, dvl)):
            value = nt(src[two].reshape(tall, feats), wqkv[n])
            dmx[n, :, pl.ds(PAD, frames), :] = value.reshape(2, frames, feats)
        for i in range(2):
            s = 2 * t + i
            for n in range(3):
                dmx[n, i, pl.ds(PAD - 1, 1), :] = edge_mix[n, pl.ds(s, 1), :]
                dmx[n, i, pl.ds(PAD + frames, 1), :] = edge_mix[n, pl.ds(seqs + s, 1), :]
            here = link[s, pl.ds(own, frames), :]
            after = link[s, pl.ds(own + 1, frames), :]
            for lane in lanes:
                left = nf[s, pl.ds(own - 1, frames), lane] * here
                mid = nf[s, pl.ds(own, frames), lane]
                right = nf[s, pl.ds(own + 1, frames), lane] * after
                from_left, from_mid, from_right = 0.0, 0.0, 0.0
                for n in range(3):
                    k0, k1, k2 = (params[pl.ds(3 * n + c, 1), lane] for c in range(3))
                    g = dmx[n, i, pl.ds(PAD, frames), lane]
                    sums[3 * n, :, lane] += fold(g * left)
                    sums[3 * n + 1, :, lane] += fold(g * mid)
                    sums[3 * n + 2, :, lane] += fold(g * right)
                    from_mid = from_mid + k1 * g
                    from_right = from_right + k0 * dmx[n, i, pl.ds(PAD + 1, frames), lane]
                    from_left = from_left + k2 * dmx[n, i, pl.ds(PAD - 1, frames), lane]
                dnb[:, lane] = from_mid + from_right * after + from_left * here
            e = dnb[...]
            centered, r = moments(x[s].astype(F32))
            xhat = centered * r
            sums[9] += fold(e * xhat)
            eg = e * gain_one
            res[s] = res[s] + r * (
                eg - jnp.mean(eg, axis=-1, keepdims=True) - xhat * jnp.mean(eg * xhat, axis=-1, keepdims=True)
            )

    loop(pairs, input_grads)
    din_copy = pltpu.make_async_copy(res, din_hbm, out_sem.at[pairs])
    din_copy.start()
    small_cur[0] = jnp.sum(sums[...], axis=1)

    def small_copy(level):
        _, peer = partner_of(*orders[0][level])
        return pltpu.make_async_remote_copy(
            src_ref=small_cur.at[level], dst_ref=small_recv.at[level],
            send_sem=sm_send.at[level], recv_sem=sm_recv.at[level],
            device_id=peer, device_id_type=MESH,
        )

    small_copy(0).start()
    for i in range(1, 2 * levels + 1):
        for u in range(units):
            red.tick(u, i)
        if i <= levels:
            small_copy(i - 1).wait_recv()
            total = small_cur[i - 1] + small_recv[i - 1]
            if i < levels:
                small_cur[i] = total
                small_copy(i).start()
            else:
                small_out[...] = total
    weight_copies = []
    for block in range(2 * ff_blocks + 4):
        ref, start = red.full(block // per_unit)
        src = ref.at[pl.ds(start + (block % per_unit) * feats, feats)]
        if block < ff_blocks:
            dst = down_hbm.at[pl.ds(block * feats, feats)]
        elif block < 2 * ff_blocks:
            dst = up_hbm.at[:, pl.ds((block - ff_blocks) * feats, feats)]
        elif block == 2 * ff_blocks:
            dst = outw_hbm
        else:
            dst = qkvw_hbm.at[block - 2 * ff_blocks - 1]
        weight_copies.append(pltpu.make_async_copy(src, dst, out_sem.at[pairs + 1 + block]))
    for copy in weight_copies:
        copy.start()
    to_next.wait_send()
    to_prev.wait_send()
    for copy in exchange:
        copy.wait_send()
    for level in range(levels):
        small_copy(level).wait_send()
    for u in range(units):
        red.wait_sends(u)
    for copy in out_copies + [din_copy] + weight_copies:
        copy.wait()


def shards(
    inputs, lengths, norm_gain, conv_kernel, qkv_weight, out_weight, mlp_gain, up_weight,
    down_weight, layer_scale, cotangent,
):
    seqs, frames, feats = inputs.shape
    ff = up_weight.shape[1]
    seq_size, tm_size = lax.axis_size("seq"), lax.axis_size("tm")
    rows = max(feats, 16 * seq_size * tm_size)
    units = (2 * ff + 4 * feats) // rows
    orders = bit_orders(seq_size, tm_size)[:units]
    levels = len(orders[0])
    params = jnp.concatenate(
        [
            conv_kernel.reshape(9, feats), norm_gain[None], mlp_gain[None], layer_scale[None],
            jnp.zeros((4, feats), BF16),
        ],
        axis=0,
    ).astype(F32)
    ext = frames + 2 * HALO
    blocks = frames // QB
    dma = pltpu.SemaphoreType.DMA
    any_spec = pl.BlockSpec(memory_space=pl.ANY)
    vmem_spec = pl.BlockSpec(memory_space=pltpu.VMEM)
    low = lambda *shape: pltpu.VMEM(shape, BF16)
    wide = lambda *shape: pltpu.VMEM(shape, F32)
    acts = lambda: low(seqs, frames, feats)
    acts_ext = lambda: low(seqs, ext, feats)
    scratch = [
        acts(), acts(), low(3, feats, feats), low(feats, feats), low(feats, ff), low(ff, feats),
        low(seqs, HALO, feats), low(seqs, HALO, feats),
        wide(seqs, ext + 2 * PAD, feats), wide(seqs, ext + 2 * PAD, 128),
        acts(), acts_ext(), acts_ext(), acts(), acts_ext(), acts_ext(),
        wide(seqs * blocks, HEADS, QB, KB), acts(), wide(seqs, frames, feats), acts(), acts(),
        low(seqs * frames * ff // feats, feats), low(seqs * frames * ff // feats, feats), acts(), acts(), acts(),
        wide(seqs, ext, feats), wide(seqs, ext, feats), wide(3, 2, frames + 2 * PAD, feats), wide(frames, feats),
        low(seqs, HALO, 2 * feats), low(seqs, HALO, 2 * feats), low(seqs, HALO, 2 * feats), low(seqs, HALO, 2 * feats),
        wide(seqs, feats), wide(seqs, feats), wide(seqs, feats), wide(seqs, feats),
        wide(3, 2 * seqs, feats), wide(3, 2 * seqs, feats), wide(16, 8, feats),
        wide(levels, 16, feats), wide(levels, 16, feats),
        low(units, rows, feats), low(units, rows, feats),
        dma((6,)), dma((seqs // 2 + 1 + (2 * ff + 4 * feats) // feats,)), dma((6,)), dma((6,)),
        dma((units, levels)), dma((units, levels)), dma((units, levels)), dma((units, levels)),
        dma((levels,)), dma((levels,)),
    ]
    cfg = (orders, rows, seqs, frames, feats, ff, tm_size)
    out_type = jax.ShapeDtypeStruct
    output, d_inputs, down, up, out_w, qkv_w, small = pl.pallas_call(
        functools.partial(layer_kernel, cfg),
        out_shape=(
            out_type(inputs.shape, BF16), out_type(inputs.shape, F32), out_type((ff, feats), BF16),
            out_type((feats, ff), BF16), out_type((feats, feats), BF16), out_type((3, feats, feats), BF16),
            out_type((16, feats), F32),
        ),
        in_specs=[pl.BlockSpec(memory_space=pltpu.SMEM), any_spec, vmem_spec] + [any_spec] * 5,
        out_specs=(any_spec,) * 6 + (vmem_spec,),
        scratch_shapes=scratch,
        compiler_params=pltpu.CompilerParams(
            collective_id=0, has_side_effects=True, vmem_limit_bytes=67043328
        ),
    )(lengths, inputs, params, qkv_weight, out_weight, up_weight, down_weight, cotangent)
    return (
        output, d_inputs, small[9], small[:9].reshape(3, 3, feats), qkv_w.astype(F32), out_w.astype(F32),
        small[10], up.astype(F32), down.astype(F32), small[11],
    )


def solution(mesh):
    split = P("seq", "tm", None)
    return jax.shard_map(
        shards,
        mesh=mesh,
        in_specs=(split, P("seq", None)) + (P(),) * 8 + (split,),
        out_specs=(split, split) + (P(),) * 8,
        check_vma=False,
    )
```

```python
import functools

import jax
import jax.numpy as jnp
from jax import lax
from jax.experimental import pallas as pl
from jax.experimental.pallas import tpu as pltpu
from jax.sharding import PartitionSpec as P

HEADS = 4
HD = 128
HALF = 9
HALO = 16
PAD = 8
EPS = 1e-05
MESH = pl.DeviceIdType.MESH
F32 = jnp.float32
BF16 = jnp.bfloat16


def bit_orders(seq_size, tm_size):
    seq_bits = [("seq", b) for b in range(seq_size.bit_length() - 1)]
    tm_bits = [("tm", b) for b in range(tm_size.bit_length() - 1)]
    core, rest = tm_bits[:1], tm_bits[1:]
    first = core + seq_bits + rest
    second = core + seq_bits[::-1] + rest
    third = core + rest[:1] + seq_bits + rest[1:]
    fourth = core + rest[:1] + seq_bits[::-1] + rest[1:]
    return [first, second, third, first, second, fourth, first, second, third, first, second, fourth]


def partner_of(axis, bit):
    me = lax.axis_index(axis)
    mine = lax.rem(me // (1 << bit), 2)
    other = me + (1 - 2 * mine) * (1 << bit)
    if axis == "seq":
        return mine, (other, lax.axis_index("tm"))
    return mine, (lax.axis_index("seq"), other)


class Reducer:
    def __init__(self, orders, rows, part, recv, fulls, sems):
        self.orders, self.rows = orders, rows
        self.part, self.recv, self.fulls = part, recv, fulls
        self.rs_send, self.rs_recv, self.ag_send, self.ag_recv = sems
        self.levels = len(orders[0])

    def landing(self, level):
        return self.rows - (self.rows >> level)

    def owned(self, unit, level):
        off = 0
        for i in range(level + 1):
            mine, _ = partner_of(*self.orders[unit][i])
            off = off + mine * (self.rows >> (i + 1))
        return off, self.rows >> (level + 1)

    def scatter_copy(self, unit, level):
        mine, peer = partner_of(*self.orders[unit][level])
        half = self.rows >> (level + 1)
        base = self.owned(unit, level - 1)[0] if level else 0
        off = pl.multiple_of(base + (1 - mine) * half, 16)
        return pltpu.make_async_remote_copy(
            src_ref=self.part.at[unit, pl.ds(off, half)],
            dst_ref=self.recv.at[unit, pl.ds(self.landing(level), half)],
            send_sem=self.rs_send.at[unit, level],
            recv_sem=self.rs_recv.at[unit, level],
            device_id=peer,
            device_id_type=MESH,
        )

    def full(self, unit):
        held = self.fulls[0].shape[0] // self.rows
        index = unit % held
        if unit < held and self.rows == self.fulls[0].shape[1]:
            half = held // 2
            index = 2 * (unit % half) + unit // half
        return self.fulls[unit // held], index * self.rows

    def gather_copy(self, unit, level):
        _, peer = partner_of(*self.orders[unit][level])
        off, size = self.owned(unit, level)
        ref, start = self.full(unit)
        region = ref.at[pl.ds(pl.multiple_of(start + off, 16), size)]
        return pltpu.make_async_remote_copy(
            src_ref=region,
            dst_ref=region,
            send_sem=self.ag_send.at[unit, level],
            recv_sem=self.ag_recv.at[unit, level],
            device_id=peer,
            device_id_type=MESH,
        )

    def combine(self, unit, level):
        self.scatter_copy(unit, level).wait_recv()
        off, half = self.owned(unit, level)
        step = min(half, 32)

        def body(i, carry):
            here = pl.ds(pl.multiple_of(off + i * step, 16), step)
            there = pl.ds(pl.multiple_of(self.landing(level) + i * step, 16), step)
            total = self.part[unit, here, :].astype(F32) + self.recv[unit, there, :].astype(F32)
            if level == self.levels - 1:
                ref, start = self.full(unit)
                ref[pl.ds(pl.multiple_of(start + off + i * step, 16), step), :] = total.astype(BF16)
            else:
                self.part[unit, here, :] = total.astype(BF16)
            return carry

        lax.fori_loop(0, half // step, body, 0)

    def tick(self, unit, i):
        if i == 0:
            self.scatter_copy(unit, 0).start()
        elif i < self.levels:
            self.combine(unit, i - 1)
            self.scatter_copy(unit, i).start()
        elif i == self.levels:
            self.combine(unit, i - 1)
            self.gather_copy(unit, self.levels - 1).start()
        elif i < 2 * self.levels:
            level = 2 * self.levels - 1 - i
            self.gather_copy(unit, level + 1).wait_recv()
            self.gather_copy(unit, level).start()
        else:
            self.gather_copy(unit, 0).wait_recv()

    def wait_sends(self, unit):
        for level in range(self.levels):
            self.scatter_copy(unit, level).wait_send()
            self.gather_copy(unit, level).wait_send()


def beside(tm_size):
    at = lax.axis_index("tm")
    seq = lax.axis_index("seq")
    return [(at < tm_size - 1, (seq, at + 1)), (at > 0, (seq, at - 1))]


def plan_steps(orders, rows, feats, pieces, small_from):
    levels = len(orders[0])
    rate = {"core": 185e3, "link": 85e3}
    free, reached, arrival = {}, {}, {}
    small_bytes = 16 * feats * 4

    def send(unit, now, level, size):
        axis, bit = (orders[unit] if unit >= 0 else orders[0])[level]
        if (axis, bit) == ("tm", 0):
            uses, lag = [("core", size / rate["core"])], 1.0
        elif axis == "seq":
            uses, lag = [((axis, bit), 2 * size / rate["link"])], 1.8
        elif bit == 1:
            uses, lag = [((axis, 1), 2 * size / rate["link"])], 1.8
        else:
            uses = [((axis, 1), 2 * size / rate["link"]), ((axis, bit), 4 * size / rate["link"])]
            lag = 2.6
        start = max([now] + [free.get(name, 0.0) for name, _ in uses])
        for name, busy in uses:
            free[name] = start + busy
        return start + max(busy for _, busy in uses) + lag

    def bytes_of(level):
        return (rows >> (level + 1)) * feats * 2

    def step(unit, now):
        i = reached[unit]
        reached[unit] = i + 1
        if unit < 0:
            if i < levels:
                arrival[unit] = send(unit, now, i, small_bytes)
            return 0.05 if i <= levels else 0.0
        cost = 0.02 + (bytes_of(i - 1) / 2.4e6 if 0 < i <= levels else 0.0)
        if i < levels:
            arrival[unit] = send(unit, now + cost, i, bytes_of(i))
        elif i < 2 * levels:
            level = 2 * levels - 1 - i
            arrival[unit] = send(unit, now + cost, level, bytes_of(level))
        return cost

    def last(unit):
        return levels if unit < 0 else 2 * levels

    now, placed = 0.0, {}
    for slot, us, begins in pieces:
        now += us
        todo = []
        if begins is not None:
            reached[begins] = 0
            now += step(begins, now)
        while True:
            ready = [u for u in reached if reached[u] <= last(u) and arrival[u] <= now]
            if not ready:
                break
            unit = min(ready, key=lambda u: (arrival[u], u))
            todo.append((unit, reached[unit]))
            now += step(unit, now)
        placed[slot] = todo
    work_end = now
    if small_from:
        reached[-1] = 0
        now += step(-1, now)
    tail = []
    while True:
        left = [u for u in reached if reached[u] <= last(u)]
        if not left:
            break
        unit = min(left, key=lambda u: (arrival[u], u))
        now = max(now, arrival[unit])
        tail.append((unit, reached[unit]))
        now += step(unit, now)
    return placed, tail, (work_end, now)


def greet(bits, tm_size):
    barrier = pltpu.get_barrier_semaphore()
    for axis, bit in bits:
        pl.semaphore_signal(barrier, inc=1, device_id=partner_of(axis, bit)[1], device_id_type=MESH)
    for there, peer in beside(tm_size):
        @pl.when(there)
        def _():
            pl.semaphore_signal(barrier, inc=1, device_id=peer, device_id_type=MESH)


def enter(bits, tm_size):
    count = len(bits)
    for there, _ in beside(tm_size):
        count = count + there.astype(jnp.int32)
    pl.semaphore_wait(pltpu.get_barrier_semaphore(), count)


def nn(a, b):
    return lax.dot_general(a, b, (((1,), (0,)), ((), ())), preferred_element_type=F32)


def nt(a, b):
    return lax.dot_general(a, b, (((1,), (1,)), ((), ())), preferred_element_type=F32)


def tn(a, b):
    return lax.dot_general(a, b, (((0,), (0,)), ((), ())), preferred_element_type=F32)


def moments(v):
    mean = jnp.mean(v, axis=-1, keepdims=True)
    centered = v - mean
    var = jnp.mean(centered * centered, axis=-1, keepdims=True)
    return centered, lax.rsqrt(var + EPS)


def fold(v):
    rows, cols = v.shape
    return jnp.sum(v.reshape(rows // 8, 8, cols), axis=0)


def gelu_pair(v):
    c = 0.7978845608028654
    square = v * v
    inner = v * (c + (c * 0.044715) * square)
    t = jnp.tanh(inner)
    half = 0.5 * (1.0 + t)
    slope = half + (0.5 * v) * (1.0 - t * t) * (c + (3.0 * 0.044715 * c) * square)
    return v * half, slope


def loop(count, body):
    def step(i, carry):
        body(i)
        return carry

    lax.fori_loop(0, count, step, 0)


def layer_kernel(cfg, *refs):
    (
        lengths, x_hbm, norm_gain, conv_kernel, mlp_gain, layer_scale, wqkv_hbm, wout_hbm, wup_hbm, wdown_hbm, cot_hbm,
        out_hbm, din_hbm, down_hbm, up_hbm, outw_hbm, qkvw_hbm, small_out,
        params, x, cot, wqkv, wout, wup, wdown, halo_lo, halo_hi, nf, link,
        act_q, act_k, act_v, qs, ks, vs, prob, att, res, n2, dm, hid, du, dbr, da, outs,
        dke, dve, dmx, dnb, msg_hi, msg_lo, got_lo, got_hi, dq_hi, dq_lo, dq_got_lo, dq_got_hi,
        edge, edge_mix, sums, small_cur, small_recv,
        part, recv,
        in_sem, out_sem, halo_send, halo_recv, rs_send, rs_recv, ag_send, ag_recv, sm_send, sm_recv,
    ) = refs
    orders, rows, seqs, frames, feats, ff, tm_size = cfg
    units = len(orders)
    levels = len(orders[0])
    ext = frames + 2 * HALO
    own = PAD + HALO
    seq_length = frames * tm_size
    vids = lengths.shape[1]
    temper = HD ** (-0.5)
    lanes = [pl.ds(c * 128, 128) for c in range(feats // 128)]
    pairs = seqs // 2
    per_unit = rows // feats
    base = lax.axis_index("tm") * frames
    red = Reducer(orders, rows, part, recv, (hid, du), (rs_send, rs_recv, ag_send, ag_recv))

    loads = [
        pltpu.make_async_copy(src, dst, in_sem.at[i])
        for i, (src, dst) in enumerate(
            [(x_hbm, x), (wqkv_hbm, wqkv), (wout_hbm, wout), (wup_hbm, wup), (wdown_hbm, wdown), (cot_hbm, cot)]
        )
    ]
    for load in loads:
        load.start()

    class Across:
        def __init__(self, src, dst, i, side):
            (self.sends, peer), (self.gets, _) = beside(tm_size)[side], beside(tm_size)[1 - side]
            self.copy = pltpu.make_async_remote_copy(
                src_ref=src, dst_ref=dst, send_sem=halo_send.at[i], recv_sem=halo_recv.at[i],
                device_id=peer, device_id_type=MESH,
            )

        def start(self):
            pl.when(self.sends)(lambda: self.copy.start())

        def wait_recv(self):
            pl.when(self.gets)(lambda: self.copy.wait_recv())

        def wait_send(self):
            pl.when(self.sends)(lambda: self.copy.wait_send())

    greet(orders[0], tm_size)
    for n in range(3):
        params[pl.ds(3 * n, 3), :] = conv_kernel[n].astype(F32)
    for i, src in enumerate((norm_gain, mlp_gain, layer_scale)):
        params[pl.ds(9 + i, 1), :] = src[...].astype(F32).reshape(1, feats)

    def clear_missing(side, refs_in):
        there = beside(tm_size)[side][0]

        @pl.when(jnp.logical_not(there))
        def _():
            for ref in refs_in:
                ref[...] = jnp.zeros_like(ref)

    clear_missing(1, (halo_lo, got_lo, dq_got_lo))
    clear_missing(0, (halo_hi, got_hi, dq_got_hi))
    to_next = Across(x_hbm.at[:, pl.ds(frames - HALO, HALO)], halo_lo, 0, 0)
    to_prev = Across(x_hbm.at[:, pl.ds(0, HALO)], halo_hi, 1, 1)
    sums[...] = jnp.zeros_like(sums)

    def bounds_of(s):
        total, found = 0, []
        for j in range(vids):
            total = total + lengths[s, j]
            found.append(total)
        return found

    gain_one = params[pl.ds(9, 1), :]
    gain_two = params[pl.ds(10, 1), :]
    scale = params[pl.ds(11, 1), :]

    def normed_rows(rows_in):
        centered, r = moments(rows_in.astype(F32))
        return (centered * r * gain_one).astype(BF16).astype(F32)

    loads[0].wait()

    def norm_own(s):
        nf[s, pl.ds(own, frames), :] = normed_rows(x[s])
        zero = jnp.zeros((PAD, feats), F32)
        nf[s, pl.ds(0, PAD), :] = zero
        nf[s, pl.ds(PAD + ext, PAD), :] = zero
        pos = base - own + lax.broadcasted_iota(jnp.int32, (ext + 2 * PAD, 128), 0)
        cut = pos == 0
        for bound in bounds_of(s):
            cut = cut | (pos == bound)
        link[s] = jnp.where(cut, 0.0, 1.0)

    loop(seqs, norm_own)
    enter(orders[0], tm_size)
    to_next.start()
    to_prev.start()
    to_next.wait_recv()
    to_prev.wait_recv()

    def norm_halo(s):
        nf[s, pl.ds(PAD, HALO), :] = normed_rows(halo_lo[s])
        nf[s, pl.ds(own + frames, HALO), :] = normed_rows(halo_hi[s])

    loop(seqs, norm_halo)
    loads[1].wait()

    def mix_project(t):
        for i in range(2):
            s = 2 * t + i
            before_on = link[s, pl.ds(PAD, ext), :]
            after_on = link[s, pl.ds(PAD + 1, ext), :]
            for lane in lanes:
                before = nf[s, pl.ds(PAD - 1, ext), lane] * before_on
                centre = nf[s, pl.ds(PAD, ext), lane]
                after = nf[s, pl.ds(PAD + 1, ext), lane] * after_on
                for n, dst in enumerate((act_q, act_k, act_v)):
                    k0, k1, k2 = (params[pl.ds(3 * n + c, 1), lane] for c in range(3))
                    mixed = (k0 * before + k1 * centre + k2 * after).astype(BF16)
                    if n == 0:
                        dst[s, :, lane] = mixed[HALO : HALO + frames]
                    else:
                        dst[s, :, lane] = mixed
        two = pl.ds(2 * t, 2)
        for n, (src, dst) in enumerate(((act_q, qs), (act_k, ks), (act_v, vs))):
            size = src.shape[1]
            value = nn(src[two].reshape(2 * size, feats), wqkv[n])
            dst[two] = value.astype(BF16).reshape(2, size, feats)

    loop(pairs, mix_project)

    def attend(s):
        key = lax.broadcasted_iota(jnp.int32, (ext, frames), 0) - HALO
        query = lax.broadcasted_iota(jnp.int32, (ext, frames), 1)
        band = (key - query <= HALF) & (key - query >= -HALF)
        pos_k = key + base
        pos_q = lax.broadcasted_iota(jnp.int32, (8, frames), 1) + base
        seg_k = jnp.zeros((ext, frames), jnp.int32)
        seg_q = jnp.zeros((8, frames), jnp.int32)
        for bound in bounds_of(s):
            seg_k = seg_k + (pos_k >= bound).astype(jnp.int32)
            seg_q = seg_q + (pos_q >= bound).astype(jnp.int32)
        allowed = band & (seg_k == seg_q[0:1]) & (pos_k >= 0) & (pos_k < seq_length)
        bias = jnp.where(allowed, 0.0, -1e30)
        for h in range(HEADS):
            head = pl.ds(h * HD, HD)
            scores = nt(ks[s, :, head], qs[s, :, head]) * temper + bias
            top = jnp.max(scores, axis=0, keepdims=True)
            raised = jnp.exp(scores - top)
            probs = raised * (1.0 / jnp.sum(raised, axis=0, keepdims=True))
            prob[s, h] = probs
            att[s, :, head] = tn(probs.astype(BF16), vs[s, :, head]).astype(BF16)

    loop(seqs, attend)
    for load in loads[2:]:
        load.wait()
    tall = 2 * frames
    chunk = feats
    tokens = seqs * frames
    out_copies = [
        pltpu.make_async_copy(outs.at[pl.ds(2 * t, 2)], out_hbm.at[pl.ds(2 * t, 2)], out_sem.at[t])
        for t in range(pairs)
    ]

    def flat(ref, t):
        return ref[pl.ds(2 * t, 2)].reshape(tall, ref.shape[2])

    def back(value):
        return value.reshape(2, frames, feats)

    def residual_norm(t):
        two = pl.ds(2 * t, 2)
        residual = flat(x, t).astype(F32) + nn(flat(att, t), wout[...])
        res[two] = back(residual)
        centered, r = moments(residual)
        n2[two] = back((centered * r * gain_two).astype(BF16))
        dm[two] = back((flat(cot, t).astype(F32) * scale).astype(BF16))

    loop(pairs, residual_norm)
    whole = lambda ref: ref[...].reshape(seqs * frames, ref.shape[2])
    early = pl.ds(0, frames)

    def place(block, value):
        part[block // per_unit, pl.ds((block % per_unit) * feats, feats), :] = value.astype(BF16)

    ff_blocks = ff // feats
    weight_copies = []

    def block_copy(block):
        ref, start = red.full(block // per_unit)
        src = ref.at[pl.ds(start + (block % per_unit) * feats, feats)]
        if block < ff_blocks:
            dst = down_hbm.at[pl.ds(block * feats, feats)]
        elif block < 2 * ff_blocks:
            dst = up_hbm.at[:, pl.ds((block - ff_blocks) * feats, feats)]
        elif block == 2 * ff_blocks:
            dst = outw_hbm
        else:
            dst = qkvw_hbm.at[block - 2 * ff_blocks - 1]
        return pltpu.make_async_copy(src, dst, out_sem.at[pairs + 1 + block])

    def unit_begun(block):
        return block // per_unit if block % per_unit == per_unit - 1 else None

    pieces = []
    for j in range(ff_blocks):
        pieces += [(("f", j, t), 0.95, None) for t in range(pairs)]
        pieces += [(("d", j), 0.73, unit_begun(j)), (("u", j), 0.73, unit_begun(ff_blocks + j))]
    pieces += [(("x", t), 0.8, None) for t in range(pairs)]
    pieces += [("o", 0.73, unit_begun(2 * ff_blocks))]
    pieces += [(("b", s), 1.0, None) for s in range(seqs)]
    pieces += [
        ("q", 0.73, unit_begun(2 * ff_blocks + 1)), ("w", 2.5, None),
        ("k", 0.73, unit_begun(2 * ff_blocks + 2)), ("v", 0.73, unit_begun(2 * ff_blocks + 3)),
    ]
    pieces += [(("i", s), 0.8, None) for s in range(seqs)]
    placed, tail, _ = plan_steps(orders, rows, feats, pieces, True)

    def advance(u, i):
        red.tick(u, i)
        if i == 2 * levels:
            for block in range(u * per_unit, (u + 1) * per_unit):
                weight_copies.append(block_copy(block))
                weight_copies[-1].start()

    def slot(name, index=None, count=0):
        if index is None:
            for u, i in placed[name]:
                advance(u, i)
            return
        for k in range(count):
            if placed[name + (k,)]:
                pl.when(index == k)(lambda k=k: [advance(u, i) for u, i in placed[name + (k,)]] and None)

    def begin(block):
        u = unit_begun(block)
        if u is not None:
            advance(u, 0)

    mlp_sum, e_sum = dke, dve

    def add_back(ref, t, first, value):
        two = pl.ds(2 * t, 2)
        ref[two, early, :] = back(value) if first else ref[two, early, :] + back(value)

    for j in range(ff_blocks):
        cols = pl.ds(j * chunk, chunk)

        def hidden_chunk(t, j=j, cols=cols):
            upper = nn(flat(n2, t), wup[:, cols])
            d_hidden = nt(flat(dm, t), wdown[cols, :])
            value, slope = gelu_pair(upper)
            value, slope = value.astype(BF16), (slope * d_hidden).astype(BF16)
            tile = pl.ds(pl.multiple_of(j * tokens + t * tall, tall), tall)
            hid[tile, :] = value
            du[tile, :] = slope
            add_back(mlp_sum, t, j == 0, nn(value, wdown[cols, :]))
            add_back(e_sum, t, j == 0, nt(slope, wup[:, cols]))
            slot(("f", j), t, pairs)

        loop(pairs, hidden_chunk)
        rows_j = pl.ds(j * tokens, tokens)
        place(j, tn(hid[rows_j, :], whole(dm)))
        begin(j)
        slot(("d", j))
        place(ff_blocks + j, tn(whole(n2), du[rows_j, :]))
        begin(ff_blocks + j)
        slot(("u", j))

    def feed_back(t):
        two = pl.ds(2 * t, 2)
        mlp_out = mlp_sum[two, early, :].reshape(tall, feats)
        e = e_sum[two, early, :].reshape(tall, feats)
        residual = flat(res, t)
        cotan = flat(cot, t).astype(F32)
        outs[two] = back((residual + scale * mlp_out).astype(BF16))
        sums[11] += fold(cotan * mlp_out)
        centered, r = moments(residual)
        xhat = centered * r
        sums[10] += fold(e * xhat)
        eg = e * gain_two
        d_res = cotan + r * (
            eg - jnp.mean(eg, axis=-1, keepdims=True) - xhat * jnp.mean(eg * xhat, axis=-1, keepdims=True)
        )
        res[two] = back(d_res)
        d_branch = d_res.astype(BF16)
        dbr[two] = back(d_branch)
        da[two] = back(nt(d_branch, wout[...]).astype(BF16))
        slot(("x",), t, pairs)

    loop(pairs, feed_back)
    for copy in out_copies:
        copy.start()

    place(2 * ff_blocks, tn(whole(att), whole(dbr)))
    begin(2 * ff_blocks)
    slot("o")

    dq = dm
    dkl, dvl = n2, att

    def attend_back(s):
        for h in range(HEADS):
            head = pl.ds(h * HD, HD)
            q, d_att, probs = qs[s, :, head], da[s, :, head], prob[s, h]
            d_weights = nt(vs[s, :, head], d_att)
            dot = jnp.sum(probs * d_weights, axis=0, keepdims=True)
            d_scores = (probs * (d_weights - dot)).astype(BF16)
            dq[s, :, head] = (tn(d_scores, ks[s, :, head]) * temper).astype(BF16)
            dke[s, :, head] = nn(d_scores, q) * temper
            dve[s, :, head] = nn(probs.astype(BF16), d_att)
        for i, src in enumerate((dke, dve)):
            cols = pl.ds(i * feats, feats)
            msg_hi[s, :, cols] = src[s, pl.ds(HALO + frames - 1, HALO), :].astype(BF16)
            msg_lo[s, :, cols] = src[s, pl.ds(1, HALO), :].astype(BF16)
        dq_hi[pl.ds(s, 1), :] = dq[s, pl.ds(frames - 16, 16), :].astype(F32)[15:16]
        dq_lo[pl.ds(s, 1), :] = dq[s, pl.ds(0, 16), :].astype(F32)[0:1]
        slot(("b",), s, seqs)

    loop(seqs, attend_back)
    exchange = [
        Across(msg_hi, got_lo, 2, 0), Across(msg_lo, got_hi, 3, 1),
        Across(dq_hi, dq_got_lo, 4, 0), Across(dq_lo, dq_got_hi, 5, 1),
    ]
    for copy in exchange:
        copy.start()
    place(2 * ff_blocks + 1, tn(whole(act_q), whole(dq)))
    begin(2 * ff_blocks + 1)
    slot("q")
    for copy in exchange:
        copy.wait_recv()
    edge[0, pl.ds(0, seqs), :] = dq_got_lo[...]
    edge[0, pl.ds(seqs, seqs), :] = dq_got_hi[...]

    def settle(s):
        for i, (src, dst) in enumerate(((dke, dkl), (dve, dvl))):
            cols = pl.ds(i * feats, feats)
            low = pl.ds(HALO - 1, HALO)
            high = pl.ds(HALO + frames - HALO + 1, HALO)
            src[s, low, :] = src[s, low, :] + got_lo[s, :, cols].astype(F32)
            src[s, high, :] = src[s, high, :] + got_hi[s, :, cols].astype(F32)
            dst[s] = src[s, pl.ds(HALO, frames), :].astype(BF16)
            edge[i + 1, pl.ds(s, 1), :] = src[s, pl.ds(HALO - 1, 1), :]
            edge[i + 1, pl.ds(seqs + s, 1), :] = src[s, pl.ds(HALO + frames, 1), :]

    loop(seqs, settle)
    slot("w")
    inner = lambda ref: ref[:, pl.ds(HALO, frames), :].reshape(seqs * frames, feats)
    place(2 * ff_blocks + 2, tn(inner(act_k), whole(dkl)))
    begin(2 * ff_blocks + 2)
    slot("k")
    place(2 * ff_blocks + 3, tn(inner(act_v), whole(dvl)))
    begin(2 * ff_blocks + 3)
    slot("v")
    for n in range(3):
        edge_mix[n] = nt(edge[n].astype(BF16), wqkv[n])

    def input_grads(t):
        two = pl.ds(2 * t, 2)
        for n, src in enumerate((dq, dkl, dvl)):
            value = nt(src[two].reshape(tall, feats), wqkv[n])
            dmx[n, :, pl.ds(PAD, frames), :] = value.reshape(2, frames, feats)
        for i in range(2):
            s = 2 * t + i
            for n in range(3):
                dmx[n, i, pl.ds(PAD - 1, 1), :] = edge_mix[n, pl.ds(s, 1), :]
                dmx[n, i, pl.ds(PAD + frames, 1), :] = edge_mix[n, pl.ds(seqs + s, 1), :]
            here = link[s, pl.ds(own, frames), :]
            after = link[s, pl.ds(own + 1, frames), :]
            for lane in lanes:
                left = nf[s, pl.ds(own - 1, frames), lane] * here
                mid = nf[s, pl.ds(own, frames), lane]
                right = nf[s, pl.ds(own + 1, frames), lane] * after
                from_left, from_mid, from_right = 0.0, 0.0, 0.0
                for n in range(3):
                    k0, k1, k2 = (params[pl.ds(3 * n + c, 1), lane] for c in range(3))
                    g = dmx[n, i, pl.ds(PAD, frames), lane]
                    sums[3 * n, :, lane] += fold(g * left)
                    sums[3 * n + 1, :, lane] += fold(g * mid)
                    sums[3 * n + 2, :, lane] += fold(g * right)
                    from_mid = from_mid + k1 * g
                    from_right = from_right + k0 * dmx[n, i, pl.ds(PAD + 1, frames), lane]
                    from_left = from_left + k2 * dmx[n, i, pl.ds(PAD - 1, frames), lane]
                dnb[:, lane] = from_mid + from_right * after + from_left * here
            e = dnb[...]
            centered, r = moments(x[s].astype(F32))
            xhat = centered * r
            sums[9] += fold(e * xhat)
            eg = e * gain_one
            res[s] = res[s] + r * (
                eg - jnp.mean(eg, axis=-1, keepdims=True) - xhat * jnp.mean(eg * xhat, axis=-1, keepdims=True)
            )
            for k in range(i, seqs, 2):
                if placed[("i", k)]:
                    pl.when(s == k)(lambda k=k: [advance(u, step) for u, step in placed[("i", k)]] and None)

    loop(pairs, input_grads)
    din_copy = pltpu.make_async_copy(res, din_hbm, out_sem.at[pairs])
    din_copy.start()
    small_cur[0] = jnp.sum(sums[...], axis=1)

    def small_copy(level):
        _, peer = partner_of(*orders[0][level])
        return pltpu.make_async_remote_copy(
            src_ref=small_cur.at[level], dst_ref=small_recv.at[level],
            send_sem=sm_send.at[level], recv_sem=sm_recv.at[level],
            device_id=peer, device_id_type=MESH,
        )

    small_copy(0).start()
    for u, small_at in tail:
        if u >= 0:
            advance(u, small_at)
            continue
        small_copy(small_at - 1).wait_recv()
        total = small_cur[small_at - 1] + small_recv[small_at - 1]
        if small_at < levels:
            small_cur[small_at] = total
            small_copy(small_at).start()
        else:
            small_out[...] = total
    to_next.wait_send()
    to_prev.wait_send()
    for copy in exchange:
        copy.wait_send()
    for level in range(levels):
        small_copy(level).wait_send()
    for u in range(units):
        red.wait_sends(u)
    for copy in out_copies + [din_copy] + weight_copies:
        copy.wait()


def widen_kernel(
    down, up, out_w, qkv_w, small, d_gain_one, d_kernel, d_qkv, d_out, d_gain_two, d_up, d_down, d_scale,
    narrow, broad, in_sem, out_sem,
):
    count, feats, _ = narrow.shape
    ff_blocks = (count - 4) // 2
    moves = []
    for j in range(ff_blocks):
        here = pl.ds(j * feats, feats)
        moves.append((down.at[here], d_down.at[here]))
    for j in range(ff_blocks):
        here = pl.ds(j * feats, feats)
        moves.append((up.at[:, here], d_up.at[:, here]))
    moves.append((out_w, d_out))
    for n in range(3):
        moves.append((qkv_w.at[n], d_qkv.at[n]))
    loads = [pltpu.make_async_copy(m[0], narrow.at[i], in_sem.at[i]) for i, m in enumerate(moves)]
    stores = [pltpu.make_async_copy(broad.at[i], m[1], out_sem.at[i]) for i, m in enumerate(moves)]
    for load in loads:
        load.start()
    for n in range(3):
        d_kernel[n] = small[pl.ds(3 * n, 3), :]
    for i, dst in enumerate((d_gain_one, d_gain_two, d_scale)):
        dst[...] = small[pl.ds(9 + i, 1), :].reshape(feats)
    for i in range(count):
        loads[i].wait()

        def widen(r):
            here = pl.ds(pl.multiple_of(r * 32, 32), 32)
            broad[i, here, :] = narrow[i, here, :].astype(F32)

        loop(feats // 32, widen)
        stores[i].start()
    for store in stores:
        store.wait()


def shards(
    inputs, lengths, norm_gain, conv_kernel, qkv_weight, out_weight, mlp_gain, up_weight,
    down_weight, layer_scale, cotangent,
):
    seqs, frames, feats = inputs.shape
    ff = up_weight.shape[1]
    seq_size, tm_size = lax.axis_size("seq"), lax.axis_size("tm")
    rows = max(feats, 16 * seq_size * tm_size)
    units = (2 * ff + 4 * feats) // rows
    orders = bit_orders(seq_size, tm_size)[:units]
    levels = len(orders[0])
    ext = frames + 2 * HALO
    dma = pltpu.SemaphoreType.DMA
    any_spec = pl.BlockSpec(memory_space=pl.ANY)
    vmem_spec = pl.BlockSpec(memory_space=pltpu.VMEM)
    low = lambda *shape: pltpu.VMEM(shape, BF16)
    wide = lambda *shape: pltpu.VMEM(shape, F32)
    acts = lambda: low(seqs, frames, feats)
    acts_ext = lambda: low(seqs, ext, feats)
    scratch = [
        wide(16, feats), acts(), acts(), low(3, feats, feats), low(feats, feats), low(feats, ff), low(ff, feats),
        low(seqs, HALO, feats), low(seqs, HALO, feats),
        wide(seqs, ext + 2 * PAD, feats), wide(seqs, ext + 2 * PAD, 128),
        acts(), acts_ext(), acts_ext(), acts(), acts_ext(), acts_ext(),
        wide(seqs, HEADS, ext, frames), acts(), wide(seqs, frames, feats), acts(), acts(),
        low(seqs * frames * ff // feats, feats), low(seqs * frames * ff // feats, feats), acts(), acts(), acts(),
        wide(seqs, ext, feats), wide(seqs, ext, feats), wide(3, 2, frames + 2 * PAD, feats), wide(frames, feats),
        low(seqs, HALO, 2 * feats), low(seqs, HALO, 2 * feats), low(seqs, HALO, 2 * feats), low(seqs, HALO, 2 * feats),
        wide(seqs, feats), wide(seqs, feats), wide(seqs, feats), wide(seqs, feats),
        wide(3, 2 * seqs, feats), wide(3, 2 * seqs, feats), wide(16, 8, feats),
        wide(levels, 16, feats), wide(levels, 16, feats),
        low(units, rows, feats), low(units, rows, feats),
        dma((6,)), dma((seqs // 2 + 1 + (2 * ff + 4 * feats) // feats,)), dma((6,)), dma((6,)),
        dma((units, levels)), dma((units, levels)), dma((units, levels)), dma((units, levels)),
        dma((levels,)), dma((levels,)),
    ]
    cfg = (orders, rows, seqs, frames, feats, ff, tm_size)
    out_type = jax.ShapeDtypeStruct
    output, d_inputs, down, up, out_w, qkv_w, small = pl.pallas_call(
        functools.partial(layer_kernel, cfg),
        out_shape=(
            out_type(inputs.shape, BF16), out_type(inputs.shape, F32), out_type((ff, feats), BF16),
            out_type((feats, ff), BF16), out_type((feats, feats), BF16), out_type((3, feats, feats), BF16),
            out_type((16, feats), F32),
        ),
        in_specs=[pl.BlockSpec(memory_space=pltpu.SMEM), any_spec] + [vmem_spec] * 4 + [any_spec] * 5,
        out_specs=(any_spec,) * 6 + (vmem_spec,),
        scratch_shapes=scratch,
        compiler_params=pltpu.CompilerParams(
            collective_id=0, has_side_effects=True, vmem_limit_bytes=67043328
        ),
    )(lengths, inputs, norm_gain, conv_kernel, mlp_gain, layer_scale, qkv_weight, out_weight, up_weight, down_weight, cotangent)
    count = (2 * ff + 4 * feats) // feats
    d_gain_one, d_kernel, d_qkv, d_out, d_gain_two, d_up, d_down, d_scale = pl.pallas_call(
        widen_kernel,
        out_shape=(
            out_type((feats,), F32), out_type((3, 3, feats), F32), out_type((3, feats, feats), F32),
            out_type((feats, feats), F32), out_type((feats,), F32), out_type((feats, ff), F32),
            out_type((ff, feats), F32), out_type((feats,), F32),
        ),
        in_specs=[pl.BlockSpec(memory_space=pltpu.HBM)] * 4 + [vmem_spec],
        out_specs=(vmem_spec, vmem_spec, any_spec, any_spec, vmem_spec, any_spec, any_spec, vmem_spec),
        scratch_shapes=[
            low(count, feats, feats), wide(count, feats, feats), dma((count,)), dma((count,)),
        ],
        compiler_params=pltpu.CompilerParams(vmem_limit_bytes=67043328),
    )(down, up, out_w, qkv_w, small)
    return (output, d_inputs, d_gain_one, d_kernel, d_qkv, d_out, d_gain_two, d_up, d_down, d_scale)


def solution(mesh):
    split = P("seq", "tm", None)
    return jax.shard_map(
        shards,
        mesh=mesh,
        in_specs=(split, P("seq", None)) + (P(),) * 8 + (split,),
        out_specs=(split, split) + (P(),) * 8,
        check_vma=False,
    )
```

```python
import functools

import jax
import jax.numpy as jnp
from jax import lax
from jax.experimental import pallas as pl
from jax.experimental.pallas import tpu as pltpu
from jax.sharding import PartitionSpec as P

HEADS = 4
HD = 128
HALF = 9
HALO = 16
PAD = 8
EPS = 1e-05
MESH = pl.DeviceIdType.MESH
F32 = jnp.float32
BF16 = jnp.bfloat16


CHOICE = (4, 0, 1, 1, 1, 7, 0, 1, 1, 0, 1, 5)


def step_orders(seq_size, tm_size):
    seq_bits = [("seq", b) for b in range(seq_size.bit_length() - 1)]
    tm_bits = [("tm", b) for b in range(tm_size.bit_length() - 1)]
    one = lambda bits: [(bit,) for bit in bits]
    two = lambda bits: [tuple(bits[i : i + 2]) for i in range(0, len(bits), 2)]
    core, rest = one(tm_bits[:1]), tm_bits[1:]
    swapped = seq_bits[::-1]
    kinds = [
        core + one(seq_bits) + two(rest),
        core + one(swapped) + two(rest),
        core + one(rest[:1]) + one(seq_bits) + one(rest[1:]),
        core + one(rest[:1]) + one(swapped) + one(rest[1:]),
        core + two(seq_bits) + two(rest),
        core + two(rest) + two(seq_bits),
        core + one(seq_bits) + one(rest),
        core + one(swapped) + one(rest),
    ]
    return kinds, [kinds[c] for c in CHOICE]


def bit_of(axis, bit):
    return lax.rem(lax.axis_index(axis) // (1 << bit), 2)


def peer_of(bits, flips):
    at = {"seq": lax.axis_index("seq"), "tm": lax.axis_index("tm")}
    for i, (axis, bit) in enumerate(bits):
        if flips >> i & 1:
            at[axis] = at[axis] + (1 - 2 * bit_of(axis, bit)) * (1 << bit)
    return at["seq"], at["tm"]


def digit_of(bits, flips=0):
    total = 0
    for i, (axis, bit) in enumerate(bits):
        mine = bit_of(axis, bit)
        total = total + (1 - mine if flips >> i & 1 else mine) * (1 << i)
    return total


class Reducer:
    def __init__(self, orders, rows, part, recv, fulls, sems):
        self.orders, self.rows = orders, rows
        self.part, self.recv, self.fulls = part, recv, fulls
        self.rs_send, self.rs_recv, self.ag_send, self.ag_recv = sems

    def levels(self, unit):
        return len(self.orders[unit])

    def size(self, unit, level):
        return self.rows >> sum(len(bits) for bits in self.orders[unit][:level])

    def owned(self, unit, level):
        off = 0
        for i in range(level):
            off = off + digit_of(self.orders[unit][i]) * self.size(unit, i + 1)
        return off

    def peers(self, unit, level):
        return range(1, 1 << len(self.orders[unit][level]))

    def slot(self, unit, level, flips):
        return sum((1 << len(bits)) - 1 for bits in self.orders[unit][:level]) + flips - 1

    def landing(self, unit, level, flips):
        return self.rows - self.size(unit, level) + (flips - 1) * self.size(unit, level + 1)

    def scatter_copies(self, unit, level):
        bits, found = self.orders[unit][level], []
        size = self.size(unit, level + 1)
        for flips in self.peers(unit, level):
            off = pl.multiple_of(self.owned(unit, level) + digit_of(bits, flips) * size, 16)
            at = self.slot(unit, level, flips)
            found.append(pltpu.make_async_remote_copy(
                src_ref=self.part.at[unit, pl.ds(off, size)],
                dst_ref=self.recv.at[unit, pl.ds(self.landing(unit, level, flips), size)],
                send_sem=self.rs_send.at[unit, at],
                recv_sem=self.rs_recv.at[unit, at],
                device_id=peer_of(bits, flips),
                device_id_type=MESH,
            ))
        return found

    def full(self, unit):
        held = self.fulls[0].shape[0] // self.rows
        index = unit % held
        if unit < held and self.rows == self.fulls[0].shape[1]:
            half = held // 2
            index = 2 * (unit % half) + unit // half
        return self.fulls[unit // held], index * self.rows

    def gather_copies(self, unit, level):
        bits, found = self.orders[unit][level], []
        ref, start = self.full(unit)
        off = pl.multiple_of(start + self.owned(unit, level + 1), 16)
        region = ref.at[pl.ds(off, self.size(unit, level + 1))]
        for flips in self.peers(unit, level):
            at = self.slot(unit, level, flips)
            found.append(pltpu.make_async_remote_copy(
                src_ref=region,
                dst_ref=region,
                send_sem=self.ag_send.at[unit, at],
                recv_sem=self.ag_recv.at[unit, at],
                device_id=peer_of(bits, flips),
                device_id_type=MESH,
            ))
        return found

    def combine(self, unit, level):
        for copy in self.scatter_copies(unit, level):
            copy.wait_recv()
        off, size = self.owned(unit, level + 1), self.size(unit, level + 1)
        step = min(size, 32)

        def body(i, carry):
            here = pl.ds(pl.multiple_of(off + i * step, 16), step)
            total = self.part[unit, here, :].astype(F32)
            for flips in self.peers(unit, level):
                there = pl.ds(pl.multiple_of(self.landing(unit, level, flips) + i * step, 16), step)
                total = total + self.recv[unit, there, :].astype(F32)
            if level == self.levels(unit) - 1:
                ref, start = self.full(unit)
                ref[pl.ds(pl.multiple_of(start + off + i * step, 16), step), :] = total.astype(BF16)
            else:
                self.part[unit, here, :] = total.astype(BF16)
            return carry

        lax.fori_loop(0, size // step, body, 0)

    def tick(self, unit, i):
        levels = self.levels(unit)
        if 0 < i <= levels:
            self.combine(unit, i - 1)
        elif i > levels:
            for copy in self.gather_copies(unit, 2 * levels - i):
                copy.wait_recv()
        if i < levels:
            out = self.scatter_copies(unit, i)
        elif i < 2 * levels:
            out = self.gather_copies(unit, 2 * levels - 1 - i)
        else:
            out = []
        for copy in out:
            copy.start()

    def wait_sends(self, unit):
        for level in range(self.levels(unit)):
            for copy in self.scatter_copies(unit, level) + self.gather_copies(unit, level):
                copy.wait_send()


def plan_steps(orders, small_steps, rows, feats, pieces):
    core_rate, link_rate = 600e3, 115e3
    free, reached, arrival = {}, {}, {}
    levels = {u: len(order) for u, order in enumerate(orders)}
    levels[-1] = len(small_steps)

    def size_of(unit, level):
        return (rows >> sum(len(bits) for bits in orders[unit][: level + 1])) * feats * 2

    def send(unit, now, level):
        bits = (orders[unit] if unit >= 0 else small_steps)[level]
        size = size_of(unit, level) if unit >= 0 else 16 * feats * 4
        wire = 2 * size / link_rate
        near, far = ("tm", 1), ("tm", 2)
        if bits[0] == ("tm", 0):
            uses, lag = [("core", size / core_rate)], 1.1
        elif len(bits) == 2:
            if bits[0][0] == "seq":
                uses, lag = [(bit, 2 * wire) for bit in bits], 3.3
            else:
                uses, lag = [(near, 3 * wire), (far, 4 * wire)], 4.0
        elif bits[0][0] == "seq" or bits[0] == near:
            uses, lag = [(bits[0], wire)], 2.6
        else:
            uses, lag = [(near, wire), (far, 2 * wire)], 3.3
        start = max([now] + [free.get(name, 0.0) for name, _ in uses])
        for name, busy in uses:
            free[name] = start + busy
        return start + max(busy for _, busy in uses) + lag

    def step(unit, now):
        i = reached[unit]
        reached[unit] = i + 1
        cost = 0.05
        if unit >= 0:
            cost = 0.02 + (size_of(unit, i - 1) / 2.4e6 if 0 < i <= levels[unit] else 0.0)
        if i < levels[unit]:
            arrival[unit] = send(unit, now + cost, i)
        elif i < last(unit):
            arrival[unit] = send(unit, now + cost, 2 * levels[unit] - 1 - i)
        return cost

    def last(unit):
        return levels[unit] if unit < 0 else 2 * levels[unit]

    now, placed = 0.0, {}
    for slot, us, begins in pieces:
        now += us
        todo = []
        if begins is not None:
            reached[begins] = 0
            now += step(begins, now)
        while True:
            ready = [u for u in reached if reached[u] <= last(u) and arrival[u] <= now]
            if not ready:
                break
            unit = min(ready, key=lambda u: (arrival[u], u))
            todo.append((unit, reached[unit]))
            now += step(unit, now)
        placed[slot] = todo
    work_end = now
    reached[-1] = 0
    now += step(-1, now)
    tail = []
    while True:
        left = [u for u in reached if reached[u] <= last(u)]
        if not left:
            break
        unit = min(left, key=lambda u: (arrival[u], u))
        now = max(now, arrival[unit])
        tail.append((unit, reached[unit]))
        now += step(unit, now)
    return placed, tail, (work_end, now)


def make_pieces(seqs, ff_blocks, per_unit):
    pairs = seqs // 2
    begun = lambda block: block // per_unit if block % per_unit == per_unit - 1 else None
    pieces = []
    for j in range(ff_blocks):
        pieces += [(("f", j, t), 0.95, None) for t in range(pairs)]
        pieces += [(("d", j), 0.73, begun(j)), (("u", j), 0.73, begun(ff_blocks + j))]
    pieces += [(("x", t), 0.75, None) for t in range(pairs)]
    pieces += [(("b", s), 1.1, None) for s in range(seqs)]
    pieces += [
        ("q", 0.73, begun(2 * ff_blocks + 1)), ("o", 0.73, begun(2 * ff_blocks)), ("w", 1.5, None),
        ("k", 0.73, begun(2 * ff_blocks + 2)), ("v", 0.73, begun(2 * ff_blocks + 3)),
    ]
    pieces += [(("i", s), 0.95, None) for s in range(seqs)]
    return pieces


def beside(tm_size):
    at = lax.axis_index("tm")
    seq = lax.axis_index("seq")
    return [(at < tm_size - 1, (seq, at + 1)), (at > 0, (seq, at - 1))]


def greet(bits, tm_size):
    barrier = pltpu.get_barrier_semaphore()
    for step, flips in bits:
        pl.semaphore_signal(barrier, inc=1, device_id=peer_of(step, flips), device_id_type=MESH)
    for there, peer in beside(tm_size):
        @pl.when(there)
        def _():
            pl.semaphore_signal(barrier, inc=1, device_id=peer, device_id_type=MESH)


def enter(bits, tm_size):
    count = len(bits)
    for there, _ in beside(tm_size):
        count = count + there.astype(jnp.int32)
    pl.semaphore_wait(pltpu.get_barrier_semaphore(), count)


def nn(a, b):
    return lax.dot_general(a, b, (((1,), (0,)), ((), ())), preferred_element_type=F32)


def nt(a, b):
    return lax.dot_general(a, b, (((1,), (1,)), ((), ())), preferred_element_type=F32)


def tn(a, b):
    return lax.dot_general(a, b, (((0,), (0,)), ((), ())), preferred_element_type=F32)


def moments(v):
    mean = jnp.mean(v, axis=-1, keepdims=True)
    centered = v - mean
    var = jnp.mean(centered * centered, axis=-1, keepdims=True)
    return centered, lax.rsqrt(var + EPS)


def fold(v):
    rows, cols = v.shape
    return jnp.sum(v.reshape(rows // 8, 8, cols), axis=0)


def gelu_pair(v):
    c = 0.7978845608028654
    square = v * v
    inner = v * (c + (c * 0.044715) * square)
    t = jnp.tanh(inner)
    half = 0.5 * (1.0 + t)
    slope = half + (0.5 * v) * (1.0 - t * t) * (c + (3.0 * 0.044715 * c) * square)
    return v * half, slope


def loop(count, body):
    def step(i, carry):
        body(i)
        return carry

    lax.fori_loop(0, count, step, 0)


def layer_kernel(cfg, *refs):
    (
        lengths, x_hbm, norm_gain, conv_kernel, mlp_gain, layer_scale, wqkv_hbm, wout_hbm, wup_hbm, wdown_hbm, cot_hbm,
        out_hbm, din_hbm, down_hbm, up_hbm, outw_hbm, qkvw_hbm, small_out,
        params, x, cot, wqkv, wout, wup, wdown, halo_lo, halo_hi, nf, link,
        act_q, act_k, act_v, qs, ks, vs, prob, att, res, n2, dm, hid, du, dbr, da, outs,
        dke, dve, dmx, msg_hi, msg_lo, got_lo, got_hi, dq_hi, dq_lo, dq_got_lo, dq_got_hi,
        edge, edge_mix, sums, small_cur, small_recv,
        part, recv,
        in_sem, out_sem, halo_send, halo_recv, rs_send, rs_recv, ag_send, ag_recv, sm_send, sm_recv,
    ) = refs
    orders, small_steps, rows, seqs, frames, feats, ff, tm_size = cfg
    units = len(orders)
    levels = len(small_steps)
    greeted = sorted({(bits, flips) for order in orders + [small_steps] for bits in order for flips in range(1, 1 << len(bits))})
    known = {}
    for bits, flips in greeted:
        known.setdefault(tuple(bit for i, bit in enumerate(bits) if flips >> i & 1), (bits, flips))
    greeted = list(known.values())
    ext = frames + 2 * HALO
    own = PAD + HALO
    seq_length = frames * tm_size
    vids = lengths.shape[1]
    temper = HD ** (-0.5)
    lanes = [pl.ds(c * 128, 128) for c in range(feats // 128)]
    pairs = seqs // 2
    per_unit = rows // feats
    base = lax.axis_index("tm") * frames
    red = Reducer(orders, rows, part, recv, (hid, du), (rs_send, rs_recv, ag_send, ag_recv))

    loads = [
        pltpu.make_async_copy(src, dst, in_sem.at[i])
        for i, (src, dst) in enumerate(
            [(x_hbm, x), (wqkv_hbm, wqkv), (wout_hbm, wout), (wup_hbm, wup), (wdown_hbm, wdown), (cot_hbm, cot)]
        )
    ]
    for load in loads:
        load.start()

    class Across:
        def __init__(self, src, dst, i, side):
            (self.sends, peer), (self.gets, _) = beside(tm_size)[side], beside(tm_size)[1 - side]
            self.copy = pltpu.make_async_remote_copy(
                src_ref=src, dst_ref=dst, send_sem=halo_send.at[i], recv_sem=halo_recv.at[i],
                device_id=peer, device_id_type=MESH,
            )

        def start(self):
            pl.when(self.sends)(lambda: self.copy.start())

        def wait_recv(self):
            pl.when(self.gets)(lambda: self.copy.wait_recv())

        def wait_send(self):
            pl.when(self.sends)(lambda: self.copy.wait_send())

    greet(greeted, tm_size)
    for n in range(3):
        params[pl.ds(3 * n, 3), :] = conv_kernel[n].astype(F32)
    for i, src in enumerate((norm_gain, mlp_gain, layer_scale)):
        params[pl.ds(9 + i, 1), :] = src[...].astype(F32).reshape(1, feats)

    def clear_missing(side, refs_in):
        there = beside(tm_size)[side][0]

        @pl.when(jnp.logical_not(there))
        def _():
            for ref in refs_in:
                ref[...] = jnp.zeros_like(ref)

    clear_missing(1, (halo_lo, got_lo, dq_got_lo))
    clear_missing(0, (halo_hi, got_hi, dq_got_hi))
    to_next = Across(x.at[:, pl.ds(frames - HALO, HALO)], halo_lo, 0, 0)
    to_prev = Across(x.at[:, pl.ds(0, HALO)], halo_hi, 1, 1)
    sums[...] = jnp.zeros_like(sums)

    def bounds_of(s):
        total, found = 0, []
        for j in range(vids):
            total = total + lengths[s, j]
            found.append(total)
        return found

    gain_one = params[pl.ds(9, 1), :]
    gain_two = params[pl.ds(10, 1), :]
    scale = params[pl.ds(11, 1), :]

    def normed_rows(rows_in):
        centered, r = moments(rows_in.astype(F32))
        return (centered * r * gain_one).astype(BF16).astype(F32)

    loads[0].wait()

    def norm_own(s):
        nf[s, pl.ds(own, frames), :] = normed_rows(x[s])
        zero = jnp.zeros((PAD, feats), F32)
        nf[s, pl.ds(0, PAD), :] = zero
        nf[s, pl.ds(PAD + ext, PAD), :] = zero
        pos = base - own + lax.broadcasted_iota(jnp.int32, (ext + 2 * PAD, 128), 0)
        cut = pos == 0
        for bound in bounds_of(s):
            cut = cut | (pos == bound)
        link[s] = jnp.where(cut, 0.0, 1.0)

    loop(seqs, norm_own)
    enter(greeted, tm_size)
    to_next.start()
    to_prev.start()
    loads[1].wait()
    streams = ((act_q, qs, 0), (act_k, ks, HALO), (act_v, vs, HALO))

    def mixed_rows(s, start, count, lane):
        before = nf[s, pl.ds(PAD + start - 1, count), lane] * link[s, pl.ds(PAD + start, count), :]
        centre = nf[s, pl.ds(PAD + start, count), lane]
        after = nf[s, pl.ds(PAD + start + 1, count), lane] * link[s, pl.ds(PAD + start + 1, count), :]
        found = []
        for n in range(3):
            k0, k1, k2 = (params[pl.ds(3 * n + c, 1), lane] for c in range(3))
            found.append((k0 * before + k1 * centre + k2 * after).astype(BF16))
        return found

    def mix_project(t):
        two = pl.ds(2 * t, 2)
        rows_of = lambda i: [mixed_rows(2 * t + i, HALO, frames, lane) for lane in lanes]
        found = [rows_of(0), rows_of(1)]
        acts = [
            jnp.concatenate([jnp.concatenate([m[n] for m in half], axis=1) for half in found], axis=0)
            for n in range(3)
        ]
        values = [nn(act, wqkv[n]).astype(BF16) for n, act in enumerate(acts)]
        for (kept, dst, skip), act, value in zip(streams, acts, values):
            kept[two] = act.reshape(2, frames, feats)
            dst[two, pl.ds(skip, frames), :] = value.reshape(2, frames, feats)

    loop(pairs, mix_project)
    to_next.wait_recv()
    to_prev.wait_recv()
    ends = 2 * HALO

    def norm_halo(i):
        four = pl.ds(pl.multiple_of(4 * i, 4), 4)
        for src, at in ((halo_lo, PAD), (halo_hi, own + frames)):
            value = normed_rows(src[four].reshape(4 * HALO, feats))
            nf[four, pl.ds(at, HALO), :] = value.reshape(4, HALO, feats)

    loop(seqs // 4, norm_halo)

    def mix_ends(s):
        sides = ((0, 0, HALO, 0), (ends, frames, 0, frames - HALO))
        found = [[mixed_rows(s, start, ends, lane) for lane in lanes] for _, start, _, _ in sides]
        for (at, _, keep, row), half in zip(sides, found):
            for n in range(3):
                mixed = jnp.concatenate([m[n] for m in half], axis=1)
                tile = pl.ds(pl.multiple_of((n * seqs + s) * 2 * ends + at, ends), ends)
                hid[tile, :] = mixed
                streams[n][0][s, pl.ds(row, HALO), :] = mixed[keep : keep + HALO]

    loop(seqs, mix_ends)
    for n, (_, dst, skip) in enumerate(streams):
        count = seqs * 2 * ends
        value = nn(hid[pl.ds(n * count, count), :], wqkv[n]).astype(BF16).reshape(seqs, 2 * ends, feats)
        piece = lambda first, last: lax.slice_in_dim(value, first, last, axis=1)
        if skip:
            dst[:, pl.ds(0, ends), :] = piece(0, ends)
            dst[:, pl.ds(frames, ends), :] = piece(ends, 2 * ends)
        else:
            dst[:, pl.ds(0, HALO), :] = piece(HALO, ends)
            dst[:, pl.ds(frames - HALO, HALO), :] = piece(ends, ends + HALO)

    def attend(s):
        key = lax.broadcasted_iota(jnp.int32, (ext, frames), 0) - HALO
        query = lax.broadcasted_iota(jnp.int32, (ext, frames), 1)
        band = (key - query <= HALF) & (key - query >= -HALF)
        pos_k = key + base
        pos_q = lax.broadcasted_iota(jnp.int32, (8, frames), 1) + base
        seg_k = jnp.zeros((ext, frames), jnp.int32)
        seg_q = jnp.zeros((8, frames), jnp.int32)
        for bound in bounds_of(s):
            seg_k = seg_k + (pos_k >= bound).astype(jnp.int32)
            seg_q = seg_q + (pos_q >= bound).astype(jnp.int32)
        allowed = band & (seg_k == seg_q[0:1]) & (pos_k >= 0) & (pos_k < seq_length)
        bias = jnp.where(allowed, 0.0, -1e30)
        heads = [pl.ds(h * HD, HD) for h in range(HEADS)]
        scores = [nt(ks[s, :, head], qs[s, :, head]) * temper + bias for head in heads]
        raised = [jnp.exp(value - jnp.max(value, axis=0, keepdims=True)) for value in scores]
        probs = [value * (1.0 / jnp.sum(value, axis=0, keepdims=True)) for value in raised]
        for h, head in enumerate(heads):
            prob[s, h] = probs[h]
        found = [tn(probs[h].astype(BF16), vs[s, :, head]) for h, head in enumerate(heads)]
        for h, head in enumerate(heads):
            att[s, :, head] = found[h].astype(BF16)

    loop(seqs, attend)
    for load in loads[2:]:
        load.wait()
    tall = 2 * frames
    chunk = feats
    tokens = seqs * frames
    out_copies = [
        pltpu.make_async_copy(outs.at[pl.ds(2 * t, 2)], out_hbm.at[pl.ds(2 * t, 2)], out_sem.at[t])
        for t in range(pairs)
    ]

    def flat(ref, t):
        return ref[pl.ds(2 * t, 2)].reshape(tall, ref.shape[2])

    def back(value):
        return value.reshape(2, frames, feats)

    def residual_norm(t):
        two = pl.ds(2 * t, 2)
        residual = flat(x, t).astype(F32) + nn(flat(att, t), wout[...])
        d_mlp = (flat(cot, t).astype(F32) * scale).astype(BF16)
        centered, r = moments(residual)
        normed_two = (centered * r * gain_two).astype(BF16)
        res[two] = back(residual)
        n2[two] = back(normed_two)
        dm[two] = back(d_mlp)

    loop(pairs, residual_norm)
    whole = lambda ref: ref[...].reshape(seqs * frames, ref.shape[2])
    early = pl.ds(0, frames)

    def place(block, value):
        part[block // per_unit, pl.ds((block % per_unit) * feats, feats), :] = value.astype(BF16)

    ff_blocks = ff // feats

    def block_copy(block):
        ref, start = red.full(block // per_unit)
        src = ref.at[pl.ds(start + (block % per_unit) * feats, feats)]
        if block < ff_blocks:
            dst = down_hbm.at[pl.ds(block * feats, feats)]
        elif block < 2 * ff_blocks:
            dst = up_hbm.at[:, pl.ds((block - ff_blocks) * feats, feats)]
        elif block == 2 * ff_blocks:
            dst = outw_hbm
        else:
            dst = qkvw_hbm.at[block - 2 * ff_blocks - 1]
        return pltpu.make_async_copy(src, dst, out_sem.at[pairs + 1 + block])

    def unit_begun(block):
        return block // per_unit if block % per_unit == per_unit - 1 else None

    placed, tail, _ = plan_steps(orders, small_steps, rows, feats, make_pieces(seqs, ff_blocks, per_unit))

    def advance(u, i):
        red.tick(u, i)
        if i == 2 * red.levels(u):
            for block in range(u * per_unit, (u + 1) * per_unit):
                block_copy(block).start()

    def slot(name, index=None, count=0):
        if index is None:
            for u, i in placed[name]:
                advance(u, i)
            return
        for k in range(count):
            if placed[name + (k,)]:
                pl.when(index == k)(lambda k=k: [advance(u, i) for u, i in placed[name + (k,)]] and None)

    def begin(block):
        u = unit_begun(block)
        if u is not None:
            advance(u, 0)

    mlp_sum, e_sum = dke, dve

    for j in range(ff_blocks):
        cols = pl.ds(j * chunk, chunk)

        def hidden_chunk(t, j=j, cols=cols):
            upper = nn(flat(n2, t), wup[:, cols])
            d_hidden = nt(flat(dm, t), wdown[cols, :])
            value, slope = gelu_pair(upper)
            value, slope = value.astype(BF16), (slope * d_hidden).astype(BF16)
            tile = pl.ds(pl.multiple_of(j * tokens + t * tall, tall), tall)
            mlp_part, e_part = nn(value, wdown[cols, :]), nt(slope, wup[:, cols])
            two = pl.ds(2 * t, 2)
            if j:
                mlp_part = mlp_part + mlp_sum[two, early, :].reshape(tall, feats)
                e_part = e_part + e_sum[two, early, :].reshape(tall, feats)
            hid[tile, :] = value
            du[tile, :] = slope
            mlp_sum[two, early, :] = back(mlp_part)
            e_sum[two, early, :] = back(e_part)
            slot(("f", j), t, pairs)

        loop(pairs, hidden_chunk)
        rows_j = pl.ds(j * tokens, tokens)
        place(j, tn(hid[rows_j, :], whole(dm)))
        begin(j)
        slot(("d", j))
        place(ff_blocks + j, tn(whole(n2), du[rows_j, :]))
        begin(ff_blocks + j)
        slot(("u", j))

    def feed_back(t):
        two = pl.ds(2 * t, 2)
        mlp_out = mlp_sum[two, early, :].reshape(tall, feats)
        e = e_sum[two, early, :].reshape(tall, feats)
        residual = flat(res, t)
        cotan = flat(cot, t).astype(F32)
        output = (residual + scale * mlp_out).astype(BF16)
        centered, r = moments(residual)
        xhat = centered * r
        eg = e * gain_two
        d_res = cotan + r * (
            eg - jnp.mean(eg, axis=-1, keepdims=True) - xhat * jnp.mean(eg * xhat, axis=-1, keepdims=True)
        )
        d_branch = d_res.astype(BF16)
        d_att = nt(d_branch, wout[...]).astype(BF16)
        scale_sum = sums[11] + fold(cotan * mlp_out)
        gain_sum = sums[10] + fold(e * xhat)
        outs[two] = back(output)
        res[two] = back(d_res)
        dbr[two] = back(d_branch)
        da[two] = back(d_att)
        sums[11] = scale_sum
        sums[10] = gain_sum
        slot(("x",), t, pairs)

    loop(pairs, feed_back)
    for copy in out_copies:
        copy.start()


    dq = dm
    dkl, dvl = n2, att

    exchange = []
    for t in range(pairs):
        two = pl.ds(2 * t, 2)
        exchange += [
            Across(msg_hi.at[two], got_lo.at[two], 4 + 2 * t, 0),
            Across(msg_lo.at[two], got_hi.at[two], 5 + 2 * t, 1),
        ]
    exchange += [Across(dq_hi, dq_got_lo, 2, 0), Across(dq_lo, dq_got_hi, 3, 1)]

    def attend_back(s):
        heads = [pl.ds(h * HD, HD) for h in range(HEADS)]
        d_atts = [da[s, :, head] for head in heads]
        probs = [prob[s, h] for h in range(HEADS)]
        d_weights = [nt(vs[s, :, head], d_att) for head, d_att in zip(heads, d_atts)]
        d_scores = [
            (p * (d_w - jnp.sum(p * d_w, axis=0, keepdims=True))).astype(BF16) for p, d_w in zip(probs, d_weights)
        ]
        found = [
            (tn(d_s, ks[s, :, head]), nn(d_s, qs[s, :, head]), nn(p.astype(BF16), d_att))
            for head, d_s, p, d_att in zip(heads, d_scores, probs, d_atts)
        ]
        for head, (d_q, d_k, d_v) in zip(heads, found):
            dq[s, :, head] = (d_q * temper).astype(BF16)
            dke[s, :, head] = d_k * temper
            dve[s, :, head] = d_v
        for i, src in enumerate((dke, dve)):
            cols = pl.ds(i * feats, feats)
            msg_hi[s, :, cols] = src[s, pl.ds(HALO + frames - 1, HALO), :].astype(BF16)
            msg_lo[s, :, cols] = src[s, pl.ds(1, HALO), :].astype(BF16)
        dq_hi[pl.ds(s, 1), :] = dq[s, pl.ds(frames - 16, 16), :].astype(F32)[15:16]
        dq_lo[pl.ds(s, 1), :] = dq[s, pl.ds(0, 16), :].astype(F32)[0:1]
        for t in range(pairs):
            pl.when(s == 2 * t + 1)(lambda t=t: [copy.start() for copy in exchange[2 * t : 2 * t + 2]] and None)
        slot(("b",), s, seqs)

    loop(seqs, attend_back)
    for copy in exchange[2 * pairs :]:
        copy.start()
    place(2 * ff_blocks + 1, tn(whole(act_q), whole(dq)))
    begin(2 * ff_blocks + 1)
    slot("q")
    place(2 * ff_blocks, tn(whole(att), whole(dbr)))
    begin(2 * ff_blocks)
    slot("o")
    for copy in exchange:
        copy.wait_recv()
    edge[0, pl.ds(0, seqs), :] = dq_got_lo[...]
    edge[0, pl.ds(seqs, seqs), :] = dq_got_hi[...]

    def settle(s):
        for i, (src, dst) in enumerate(((dke, dkl), (dve, dvl))):
            cols = pl.ds(i * feats, feats)
            low = pl.ds(HALO - 1, HALO)
            high = pl.ds(HALO + frames - HALO + 1, HALO)
            src[s, low, :] = src[s, low, :] + got_lo[s, :, cols].astype(F32)
            src[s, high, :] = src[s, high, :] + got_hi[s, :, cols].astype(F32)
            dst[s] = src[s, pl.ds(HALO, frames), :].astype(BF16)
            edge[i + 1, pl.ds(s, 1), :] = src[s, pl.ds(HALO - 1, 1), :]
            edge[i + 1, pl.ds(seqs + s, 1), :] = src[s, pl.ds(HALO + frames, 1), :]

    loop(seqs, settle)
    slot("w")
    place(2 * ff_blocks + 2, tn(whole(act_k), whole(dkl)))
    begin(2 * ff_blocks + 2)
    slot("k")
    place(2 * ff_blocks + 3, tn(whole(act_v), whole(dvl)))
    begin(2 * ff_blocks + 3)
    slot("v")
    for n in range(3):
        edge_mix[n] = nt(edge[n].astype(BF16), wqkv[n])

    def input_grads(t):
        two = pl.ds(2 * t, 2)
        for n, src in enumerate((dq, dkl, dvl)):
            value = nt(src[two].reshape(tall, feats), wqkv[n])
            dmx[n, :, pl.ds(PAD, frames), :] = value.reshape(2, frames, feats)
        for i in range(2):
            s = 2 * t + i
            for n in range(3):
                dmx[n, i, pl.ds(PAD - 1, 1), :] = edge_mix[n, pl.ds(s, 1), :]
                dmx[n, i, pl.ds(PAD + frames, 1), :] = edge_mix[n, pl.ds(seqs + s, 1), :]
            here = link[s, pl.ds(own, frames), :]
            after = link[s, pl.ds(own + 1, frames), :]
            e_parts, taps = [], []
            for lane in lanes:
                left = nf[s, pl.ds(own - 1, frames), lane] * here
                mid = nf[s, pl.ds(own, frames), lane]
                right = nf[s, pl.ds(own + 1, frames), lane] * after
                from_left, from_mid, from_right = 0.0, 0.0, 0.0
                for n in range(3):
                    k0, k1, k2 = (params[pl.ds(3 * n + c, 1), lane] for c in range(3))
                    g = dmx[n, i, pl.ds(PAD, frames), lane]
                    taps.append([fold(g * left), fold(g * mid), fold(g * right)])
                    from_mid = from_mid + k1 * g
                    from_right = from_right + k0 * dmx[n, i, pl.ds(PAD + 1, frames), lane]
                    from_left = from_left + k2 * dmx[n, i, pl.ds(PAD - 1, frames), lane]
                e_parts.append(from_mid + from_right * after + from_left * here)
            e = jnp.concatenate(e_parts, axis=1)
            centered, r = moments(x[s].astype(F32))
            xhat = centered * r
            eg = e * gain_one
            d_in = res[s] + r * (
                eg - jnp.mean(eg, axis=-1, keepdims=True) - xhat * jnp.mean(eg * xhat, axis=-1, keepdims=True)
            )
            for n in range(3):
                for c in range(3):
                    tap = jnp.concatenate([taps[3 * l + n][c] for l in range(len(lanes))], axis=1)
                    sums[3 * n + c] = sums[3 * n + c] + tap
            sums[9] = sums[9] + fold(e * xhat)
            res[s] = d_in
            for k in range(i, seqs, 2):
                if placed[("i", k)]:
                    pl.when(s == k)(lambda k=k: [advance(u, step) for u, step in placed[("i", k)]] and None)

    loop(pairs, input_grads)
    din_copy = pltpu.make_async_copy(res, din_hbm, out_sem.at[pairs])
    din_copy.start()
    small_cur[0] = jnp.sum(sums[...], axis=1)

    def small_copy(level):
        peer = peer_of(small_steps[level], 1)
        return pltpu.make_async_remote_copy(
            src_ref=small_cur.at[level], dst_ref=small_recv.at[level],
            send_sem=sm_send.at[level], recv_sem=sm_recv.at[level],
            device_id=peer, device_id_type=MESH,
        )

    small_copy(0).start()
    for u, small_at in tail:
        if u >= 0:
            advance(u, small_at)
            continue
        small_copy(small_at - 1).wait_recv()
        total = small_cur[small_at - 1] + small_recv[small_at - 1]
        if small_at < levels:
            small_cur[small_at] = total
            small_copy(small_at).start()
        else:
            small_out[...] = total
    to_next.wait_send()
    to_prev.wait_send()
    for copy in exchange:
        copy.wait_send()
    for level in range(levels):
        small_copy(level).wait_send()
    for u in range(units):
        red.wait_sends(u)
    for copy in out_copies + [din_copy] + [block_copy(b) for b in range(2 * ff_blocks + 4)]:
        copy.wait()


def widen_kernel(
    output_in, d_in, down, up, out_w, qkv_w, small, output, d_inputs, d_gain_one, d_kernel, d_qkv, d_out, d_gain_two, d_up, d_down, d_scale,
    low_held, wide_held, narrow, broad, in_sem, out_sem,
):
    count, feats, _ = narrow.shape
    ff_blocks = (count - 4) // 2
    moves = []
    for j in range(ff_blocks):
        here = pl.ds(j * feats, feats)
        moves.append((down.at[here], d_down.at[here]))
    for j in range(ff_blocks):
        here = pl.ds(j * feats, feats)
        moves.append((up.at[:, here], d_up.at[:, here]))
    moves.append((out_w, d_out))
    for n in range(3):
        moves.append((qkv_w.at[n], d_qkv.at[n]))
    loads = [pltpu.make_async_copy(m[0], narrow.at[i], in_sem.at[i]) for i, m in enumerate(moves)]
    stores = [pltpu.make_async_copy(broad.at[i], m[1], out_sem.at[i]) for i, m in enumerate(moves)]
    passes = []
    for i, (src, held, dst) in enumerate(((output_in, low_held, output), (d_in, wide_held, d_inputs))):
        passes.append((
            pltpu.make_async_copy(src, held, in_sem.at[count + i]),
            pltpu.make_async_copy(held, dst, out_sem.at[count + i]),
        ))
    for load in loads + [get for get, _ in passes]:
        load.start()
    for n in range(3):
        d_kernel[n] = small[pl.ds(3 * n, 3), :]
    for i, dst in enumerate((d_gain_one, d_gain_two, d_scale)):
        dst[...] = small[pl.ds(9 + i, 1), :].reshape(feats)
    for i in range(count):
        loads[i].wait()

        def widen(r):
            here = pl.ds(pl.multiple_of(r * 32, 32), 32)
            broad[i, here, :] = narrow[i, here, :].astype(F32)

        loop(feats // 32, widen)
        stores[i].start()
    for get, put in passes:
        get.wait()
        put.start()
    for store in stores + [put for _, put in passes]:
        store.wait()


def shards(
    inputs, lengths, norm_gain, conv_kernel, qkv_weight, out_weight, mlp_gain, up_weight,
    down_weight, layer_scale, cotangent,
):
    seqs, frames, feats = inputs.shape
    ff = up_weight.shape[1]
    seq_size, tm_size = lax.axis_size("seq"), lax.axis_size("tm")
    rows = max(feats, 16 * seq_size * tm_size)
    units = (2 * ff + 4 * feats) // rows
    kinds, orders = step_orders(seq_size, tm_size)
    orders, small_steps = orders[:units], kinds[-2]
    levels = len(small_steps)
    copies = max(sum((1 << len(bits)) - 1 for bits in order) for order in orders)
    ext = frames + 2 * HALO
    dma = pltpu.SemaphoreType.DMA
    any_spec = pl.BlockSpec(memory_space=pl.ANY)
    vmem_spec = pl.BlockSpec(memory_space=pltpu.VMEM)
    low = lambda *shape: pltpu.VMEM(shape, BF16)
    wide = lambda *shape: pltpu.VMEM(shape, F32)
    acts = lambda: low(seqs, frames, feats)
    acts_ext = lambda: low(seqs, ext, feats)
    scratch = [
        wide(16, feats), acts(), acts(), low(3, feats, feats), low(feats, feats), low(feats, ff), low(ff, feats),
        low(seqs, HALO, feats), low(seqs, HALO, feats),
        wide(seqs, ext + 2 * PAD, feats), wide(seqs, ext + 2 * PAD, 128),
        acts(), acts(), acts(), acts(), acts_ext(), acts_ext(),
        wide(seqs, HEADS, ext, frames), acts(), wide(seqs, frames, feats), acts(), acts(),
        low(seqs * frames * ff // feats, feats), low(seqs * frames * ff // feats, feats), acts(), acts(), acts(),
        wide(seqs, ext, feats), wide(seqs, ext, feats), wide(3, 2, frames + 2 * PAD, feats),
        low(seqs, HALO, 2 * feats), low(seqs, HALO, 2 * feats), low(seqs, HALO, 2 * feats), low(seqs, HALO, 2 * feats),
        wide(seqs, feats), wide(seqs, feats), wide(seqs, feats), wide(seqs, feats),
        wide(3, 2 * seqs, feats), wide(3, 2 * seqs, feats), wide(16, 8, feats),
        wide(levels, 16, feats), wide(levels, 16, feats),
        low(units, rows, feats), low(units, rows, feats),
        dma((6,)), dma((seqs // 2 + 1 + (2 * ff + 4 * feats) // feats,)), dma((4 + seqs,)), dma((4 + seqs,)),
        dma((units, copies)), dma((units, copies)), dma((units, copies)), dma((units, copies)),
        dma((levels,)), dma((levels,)),
    ]
    cfg = (orders, small_steps, rows, seqs, frames, feats, ff, tm_size)
    out_type = jax.ShapeDtypeStruct
    output, d_inputs, down, up, out_w, qkv_w, small = pl.pallas_call(
        functools.partial(layer_kernel, cfg),
        out_shape=(
            out_type(inputs.shape, BF16), out_type(inputs.shape, F32), out_type((ff, feats), BF16),
            out_type((feats, ff), BF16), out_type((feats, feats), BF16), out_type((3, feats, feats), BF16),
            out_type((16, feats), F32),
        ),
        in_specs=[pl.BlockSpec(memory_space=pltpu.SMEM), any_spec] + [vmem_spec] * 4 + [any_spec] * 5,
        out_specs=(any_spec,) * 6 + (vmem_spec,),
        scratch_shapes=scratch,
        compiler_params=pltpu.CompilerParams(
            collective_id=0, has_side_effects=True, vmem_limit_bytes=67043328
        ),
    )(lengths, inputs, norm_gain, conv_kernel, mlp_gain, layer_scale, qkv_weight, out_weight, up_weight, down_weight, cotangent)
    count = (2 * ff + 4 * feats) // feats
    hbm_spec = pl.BlockSpec(memory_space=pltpu.HBM)
    return pl.pallas_call(
        widen_kernel,
        out_shape=(
            out_type(inputs.shape, BF16), out_type(inputs.shape, F32),
            out_type((feats,), F32), out_type((3, 3, feats), F32), out_type((3, feats, feats), F32),
            out_type((feats, feats), F32), out_type((feats,), F32), out_type((feats, ff), F32),
            out_type((ff, feats), F32), out_type((feats,), F32),
        ),
        in_specs=[hbm_spec] * 6 + [vmem_spec],
        out_specs=(hbm_spec,) * 2 + (vmem_spec, vmem_spec, hbm_spec, hbm_spec, vmem_spec, hbm_spec, hbm_spec, vmem_spec),
        scratch_shapes=[
            acts(), wide(seqs, frames, feats), low(count, feats, feats), wide(count, feats, feats),
            dma((count + 2,)), dma((count + 2,)),
        ],
        compiler_params=pltpu.CompilerParams(vmem_limit_bytes=67043328),
    )(output, d_inputs, down, up, out_w, qkv_w, small)


def solution(mesh):
    split = P("seq", "tm", None)
    return jax.shard_map(
        shards,
        mesh=mesh,
        in_specs=(split, P("seq", None)) + (P(),) * 8 + (split,),
        out_specs=(split, split) + (P(),) * 8,
        check_vma=False,
    )
```

```python
import functools

import jax
import jax.numpy as jnp
from jax import lax
from jax.experimental import pallas as pl
from jax.experimental.pallas import tpu as pltpu
from jax.sharding import PartitionSpec as P

HEADS = 4
HD = 128
HALF = 9
HALO = 16
PAD = 8
EPS = 1e-05
MESH = pl.DeviceIdType.MESH
F32 = jnp.float32
BF16 = jnp.bfloat16


CHOICE = (4, 4, 10, 7, 4, 10, 10, 6, 4, 5, 4, 4)


def step_orders(seq_size, tm_size):
    seq_bits = [("seq", b) for b in range(seq_size.bit_length() - 1)]
    tm_bits = [("tm", b) for b in range(tm_size.bit_length() - 1)]
    one = lambda bits: [(bit,) for bit in bits]
    two = lambda bits: [tuple(bits[i : i + 2]) for i in range(0, len(bits), 2)]
    core, rest = one(tm_bits[:1]), tm_bits[1:]
    swapped = seq_bits[::-1]
    kinds = [
        core + one(seq_bits) + two(rest),
        core + one(swapped) + two(rest),
        core + one(rest[:1]) + one(seq_bits) + one(rest[1:]),
        core + one(rest[:1]) + one(swapped) + one(rest[1:]),
        core + two(seq_bits) + two(rest),
        core + two(rest) + two(seq_bits),
        core + one(seq_bits) + one(rest),
        core + one(swapped) + one(rest),
        core + two(rest) + one(seq_bits),
        core + two(rest) + one(swapped),
        core + two(seq_bits) + one(rest),
        core + one(seq_bits[:1]) + two(rest) + one(seq_bits[1:]),
        core + one(swapped[:1]) + two(rest) + one(swapped[1:]),
        core + one(seq_bits[:1]) + one(rest[:1]) + one(seq_bits[1:]) + one(rest[1:]),
        core + one(swapped[:1]) + one(rest[:1]) + one(swapped[1:]) + one(rest[1:]),
    ]
    return kinds, [kinds[c] for c in CHOICE]


def bit_of(axis, bit):
    return lax.rem(lax.axis_index(axis) // (1 << bit), 2)


def peer_of(bits, flips):
    at = {"seq": lax.axis_index("seq"), "tm": lax.axis_index("tm")}
    for i, (axis, bit) in enumerate(bits):
        if flips >> i & 1:
            at[axis] = at[axis] + (1 - 2 * bit_of(axis, bit)) * (1 << bit)
    return at["seq"], at["tm"]


def digit_of(bits, flips=0):
    total = 0
    for i, (axis, bit) in enumerate(bits):
        mine = bit_of(axis, bit)
        total = total + (1 - mine if flips >> i & 1 else mine) * (1 << i)
    return total


def gathered_at(unit, rows, held_rows, feats):
    held = held_rows // rows
    index = unit % held
    if unit < held and rows == feats:
        half = held // 2
        index = 2 * (unit % half) + unit // half
    return unit // held, index * rows


class Reducer:
    def __init__(self, orders, rows, part, recv, fulls, sems):
        self.orders, self.rows = orders, rows
        self.part, self.recv, self.fulls = part, recv, fulls
        self.rs_send, self.rs_recv, self.ag_send, self.ag_recv = sems

    def levels(self, unit):
        return len(self.orders[unit])

    def size(self, unit, level):
        return self.rows >> sum(len(bits) for bits in self.orders[unit][:level])

    def owned(self, unit, level):
        off = 0
        for i in range(level):
            off = off + digit_of(self.orders[unit][i]) * self.size(unit, i + 1)
        return off

    def peers(self, unit, level):
        return range(1, 1 << len(self.orders[unit][level]))

    def slot(self, unit, level, flips):
        return sum((1 << len(bits)) - 1 for bits in self.orders[unit][:level]) + flips - 1

    def landing(self, unit, level, flips):
        return self.rows - self.size(unit, level) + (flips - 1) * self.size(unit, level + 1)

    def scatter_copies(self, unit, level):
        bits, found = self.orders[unit][level], []
        size = self.size(unit, level + 1)
        for flips in self.peers(unit, level):
            off = pl.multiple_of(self.owned(unit, level) + digit_of(bits, flips) * size, 16)
            at = self.slot(unit, level, flips)
            found.append(pltpu.make_async_remote_copy(
                src_ref=self.part.at[unit, pl.ds(off, size)],
                dst_ref=self.recv.at[unit, pl.ds(self.landing(unit, level, flips), size)],
                send_sem=self.rs_send.at[unit, at],
                recv_sem=self.rs_recv.at[unit, at],
                device_id=peer_of(bits, flips),
                device_id_type=MESH,
            ))
        return found

    def full(self, unit):
        which, start = gathered_at(unit, self.rows, *self.fulls[0].shape)
        return self.fulls[which], start

    def gather_copies(self, unit, level):
        bits, found = self.orders[unit][level], []
        ref, start = self.full(unit)
        off = pl.multiple_of(start + self.owned(unit, level + 1), 16)
        region = ref.at[pl.ds(off, self.size(unit, level + 1))]
        for flips in self.peers(unit, level):
            at = self.slot(unit, level, flips)
            found.append(pltpu.make_async_remote_copy(
                src_ref=region,
                dst_ref=region,
                send_sem=self.ag_send.at[unit, at],
                recv_sem=self.ag_recv.at[unit, at],
                device_id=peer_of(bits, flips),
                device_id_type=MESH,
            ))
        return found

    def combine(self, unit, level):
        for copy in self.scatter_copies(unit, level):
            copy.wait_recv()
        off, size = self.owned(unit, level + 1), self.size(unit, level + 1)
        step = min(size, 32)

        def body(i, carry):
            here = pl.ds(pl.multiple_of(off + i * step, 16), step)
            total = self.part[unit, here, :].astype(F32)
            for flips in self.peers(unit, level):
                there = pl.ds(pl.multiple_of(self.landing(unit, level, flips) + i * step, 16), step)
                total = total + self.recv[unit, there, :].astype(F32)
            if level == self.levels(unit) - 1:
                ref, start = self.full(unit)
                ref[pl.ds(pl.multiple_of(start + off + i * step, 16), step), :] = total.astype(BF16)
            else:
                self.part[unit, here, :] = total.astype(BF16)
            return carry

        lax.fori_loop(0, size // step, body, 0)

    def tick(self, unit, i):
        levels = self.levels(unit)
        if 0 < i <= levels:
            self.combine(unit, i - 1)
        elif i > levels:
            for copy in self.gather_copies(unit, 2 * levels - i):
                copy.wait_recv()
        if i < levels:
            out = self.scatter_copies(unit, i)
        elif i < 2 * levels:
            out = self.gather_copies(unit, 2 * levels - 1 - i)
        else:
            out = []
        for copy in out:
            copy.start()

    def wait_sends(self, unit):
        for level in range(self.levels(unit)):
            for copy in self.scatter_copies(unit, level) + self.gather_copies(unit, level):
                copy.wait_send()


def plan_steps(orders, small_steps, rows, feats, pieces):
    core_rate, link_rate = 600e3, 104e3
    free, reached, arrival = {}, {}, {}
    levels = {u: len(order) for u, order in enumerate(orders)}
    levels[-1] = len(small_steps)

    def size_of(unit, level):
        return (rows >> sum(len(bits) for bits in orders[unit][: level + 1])) * feats * 2

    def send(unit, now, level):
        bits = (orders[unit] if unit >= 0 else small_steps)[level]
        size = size_of(unit, level) if unit >= 0 else 16 * feats * 4
        wire = 2 * size / link_rate
        near, far = ("tm", 1), ("tm", 2)
        if bits[0] == ("tm", 0):
            uses, lag = [("core", size / core_rate)], 1.1
        elif len(bits) == 2:
            if bits[0][0] == "seq":
                uses, lag = [(bit, 2 * wire) for bit in bits], 3.3
            else:
                uses, lag = [(near, 3 * wire), (far, 4 * wire)], 4.0
        elif bits[0][0] == "seq" or bits[0] == near:
            uses, lag = [(bits[0], wire)], 2.6
        else:
            uses, lag = [(near, wire), (far, 2 * wire)], 3.3
        start = max([now] + [free.get(name, 0.0) for name, _ in uses])
        for name, busy in uses:
            free[name] = start + busy
        return start + max(busy for _, busy in uses) + lag

    def step(unit, now):
        i = reached[unit]
        reached[unit] = i + 1
        cost = 0.05
        if unit >= 0:
            cost = 0.02 + (size_of(unit, i - 1) / 2.4e6 if 0 < i <= levels[unit] else 0.0)
        if i < levels[unit]:
            arrival[unit] = send(unit, now + cost, i)
        elif i < last(unit):
            arrival[unit] = send(unit, now + cost, 2 * levels[unit] - 1 - i)
        return cost

    def last(unit):
        return levels[unit] if unit < 0 else 2 * levels[unit]

    now, crossed, placed = 0.0, 0.0, {}
    for slot, us, begins in pieces:
        now = (max(now, crossed) if slot == "w" else now) + us
        if slot[0] == "b" and slot[1] % 2:
            free[("tm", 1)] = max(now, free.get(("tm", 1), 0.0)) + 0.65
            free[("tm", 2)] = max(now, free.get(("tm", 2), 0.0)) + 0.65
            crossed = max(free[("tm", 1)], free[("tm", 2)]) + 2.6
        todo = []
        if begins is not None:
            reached[begins] = 0
            now += step(begins, now)
        while True:
            ready = [u for u in reached if reached[u] <= last(u) and arrival[u] <= now]
            if not ready:
                break
            unit = min(ready, key=lambda u: (arrival[u], u))
            todo.append((unit, reached[unit]))
            now += step(unit, now)
        placed[slot] = todo
    work_end = now
    reached[-1] = 0
    now += step(-1, now)
    tail = []
    while True:
        left = [u for u in reached if reached[u] <= last(u)]
        if not left:
            break
        unit = min(left, key=lambda u: (arrival[u], u))
        now = max(now, arrival[unit])
        tail.append((unit, reached[unit]))
        now += step(unit, now)
    return placed, tail, (work_end, now)


def make_pieces(seqs, ff_blocks, per_unit):
    pairs = seqs // 2
    begun = lambda block: block // per_unit if block % per_unit == per_unit - 1 else None
    pieces = []
    for j in range(ff_blocks):
        pieces += [(("f", j, t), 0.93, None) for t in range(pairs)]
        pieces += [(("d", j), 0.73, begun(j)), (("u", j), 0.73, begun(ff_blocks + j))]
    pieces += [(("x", t), 0.63, None) for t in range(pairs)]
    pieces += [(("b", s), 0.68, None) for s in range(seqs)]
    pieces += [
        ("q", 0.73, begun(2 * ff_blocks + 1)), ("o", 0.73, begun(2 * ff_blocks)), ("w", 0.8, None),
        ("k", 0.73, begun(2 * ff_blocks + 2)), ("v", 0.73, begun(2 * ff_blocks + 3)),
    ]
    pieces += [(("i", s), 0.92, None) for s in range(seqs)]
    return pieces


def beside(tm_size):
    at = lax.axis_index("tm")
    seq = lax.axis_index("seq")
    return [(at < tm_size - 1, (seq, at + 1)), (at > 0, (seq, at - 1))]


def greet(bits, tm_size):
    barrier = pltpu.get_barrier_semaphore()
    for step, flips in bits:
        pl.semaphore_signal(barrier, inc=1, device_id=peer_of(step, flips), device_id_type=MESH)
    for there, peer in beside(tm_size):
        @pl.when(there)
        def _():
            pl.semaphore_signal(barrier, inc=1, device_id=peer, device_id_type=MESH)


def enter(bits, tm_size):
    count = len(bits)
    for there, _ in beside(tm_size):
        count = count + there.astype(jnp.int32)
    pl.semaphore_wait(pltpu.get_barrier_semaphore(), count)


def nn(a, b):
    return lax.dot_general(a, b, (((1,), (0,)), ((), ())), preferred_element_type=F32)


def nt(a, b):
    return lax.dot_general(a, b, (((1,), (1,)), ((), ())), preferred_element_type=F32)


def tn(a, b):
    return lax.dot_general(a, b, (((0,), (0,)), ((), ())), preferred_element_type=F32)


def moments(v):
    mean = jnp.mean(v, axis=-1, keepdims=True)
    centered = v - mean
    var = jnp.mean(centered * centered, axis=-1, keepdims=True)
    return centered, lax.rsqrt(var + EPS)


def fold(v):
    rows, cols = v.shape
    return jnp.sum(v.reshape(rows // 8, 8, cols), axis=0)


def gelu_pair(v):
    c = 0.7978845608028654
    square = v * v
    inner = v * (c + (c * 0.044715) * square)
    t = jnp.tanh(inner)
    half = 0.5 * (1.0 + t)
    slope = half + (0.5 * v) * (1.0 - t * t) * (c + (3.0 * 0.044715 * c) * square)
    return v * half, slope


def loop(count, body):
    def step(i, carry):
        body(i)
        return carry

    lax.fori_loop(0, count, step, 0)


def layer_kernel(cfg, *refs):
    (
        lengths, x_hbm, norm_gain, conv_kernel, mlp_gain, layer_scale, wqkv_hbm, wout_hbm, wup_hbm, wdown_hbm, cot_hbm,
        outs, res, hid, du, small_out,
        params, x, cot, wqkv, wout, wup, wdown, halo_lo, halo_hi, nf, link,
        act_q, act_k, act_v, qs, ks, vs, prob, att, n2, dm, dbr, da,
        dke, dve, dmx, msg_hi, msg_lo, got_lo, got_hi, dq_hi, dq_lo, dq_got_lo, dq_got_hi,
        edge, edge_mix, sums, small_cur, small_recv,
        part, recv,
        in_sem, halo_send, halo_recv, rs_send, rs_recv, ag_send, ag_recv, sm_send, sm_recv,
    ) = refs
    orders, small_steps, rows, seqs, frames, feats, ff, tm_size = cfg
    units = len(orders)
    levels = len(small_steps)
    greeted = sorted({(bits, flips) for order in orders + [small_steps] for bits in order for flips in range(1, 1 << len(bits))})
    known = {}
    for bits, flips in greeted:
        known.setdefault(tuple(bit for i, bit in enumerate(bits) if flips >> i & 1), (bits, flips))
    greeted = list(known.values())
    ext = frames + 2 * HALO
    own = PAD + HALO
    seq_length = frames * tm_size
    vids = lengths.shape[1]
    temper = HD ** (-0.5)
    lanes = [pl.ds(c * 128, 128) for c in range(feats // 128)]
    pairs = seqs // 2
    per_unit = rows // feats
    base = lax.axis_index("tm") * frames
    red = Reducer(orders, rows, part, recv, (hid, du), (rs_send, rs_recv, ag_send, ag_recv))

    loads = [
        pltpu.make_async_copy(src, dst, in_sem.at[i])
        for i, (src, dst) in enumerate(
            [(x_hbm, x), (wqkv_hbm, wqkv), (wout_hbm, wout), (wup_hbm, wup), (wdown_hbm, wdown), (cot_hbm, cot)]
        )
    ]
    for load in loads:
        load.start()

    class Across:
        def __init__(self, src, dst, i, side):
            (self.sends, peer), (self.gets, _) = beside(tm_size)[side], beside(tm_size)[1 - side]
            self.copy = pltpu.make_async_remote_copy(
                src_ref=src, dst_ref=dst, send_sem=halo_send.at[i], recv_sem=halo_recv.at[i],
                device_id=peer, device_id_type=MESH,
            )

        def start(self):
            pl.when(self.sends)(lambda: self.copy.start())

        def wait_recv(self):
            pl.when(self.gets)(lambda: self.copy.wait_recv())

        def wait_send(self):
            pl.when(self.sends)(lambda: self.copy.wait_send())

    greet(greeted, tm_size)
    for n in range(3):
        params[pl.ds(3 * n, 3), :] = conv_kernel[n].astype(F32)
    for i, src in enumerate((norm_gain, mlp_gain, layer_scale)):
        params[pl.ds(9 + i, 1), :] = src[...].astype(F32).reshape(1, feats)

    def clear_missing(side, refs_in):
        there = beside(tm_size)[side][0]

        @pl.when(jnp.logical_not(there))
        def _():
            for ref in refs_in:
                ref[...] = jnp.zeros_like(ref)

    clear_missing(1, (halo_lo, got_lo, dq_got_lo))
    clear_missing(0, (halo_hi, got_hi, dq_got_hi))
    to_next = Across(x.at[:, pl.ds(frames - HALO, HALO)], halo_lo, 0, 0)
    to_prev = Across(x.at[:, pl.ds(0, HALO)], halo_hi, 1, 1)
    sums[...] = jnp.zeros_like(sums)

    def bounds_of(s):
        total, found = 0, []
        for j in range(vids):
            total = total + lengths[s, j]
            found.append(total)
        return found

    gain_one = params[pl.ds(9, 1), :]
    gain_two = params[pl.ds(10, 1), :]
    scale = params[pl.ds(11, 1), :]

    def normed_rows(rows_in):
        centered, r = moments(rows_in.astype(F32))
        return (centered * r * gain_one).astype(BF16).astype(F32)

    loads[0].wait()

    def norm_own(s):
        nf[s, pl.ds(own, frames), :] = normed_rows(x[s])
        zero = jnp.zeros((PAD, feats), F32)
        nf[s, pl.ds(0, PAD), :] = zero
        nf[s, pl.ds(PAD + ext, PAD), :] = zero
        pos = base - own + lax.broadcasted_iota(jnp.int32, (ext + 2 * PAD, 128), 0)
        cut = pos == 0
        for bound in bounds_of(s):
            cut = cut | (pos == bound)
        link[s] = jnp.where(cut, 0.0, 1.0)

    loop(seqs, norm_own)
    enter(greeted, tm_size)
    to_next.start()
    to_prev.start()
    loads[1].wait()
    streams = ((act_q, qs, 0), (act_k, ks, HALO), (act_v, vs, HALO))

    def mixed_rows(s, start, count, lane):
        before = nf[s, pl.ds(PAD + start - 1, count), lane] * link[s, pl.ds(PAD + start, count), :]
        centre = nf[s, pl.ds(PAD + start, count), lane]
        after = nf[s, pl.ds(PAD + start + 1, count), lane] * link[s, pl.ds(PAD + start + 1, count), :]
        found = []
        for n in range(3):
            k0, k1, k2 = (params[pl.ds(3 * n + c, 1), lane] for c in range(3))
            found.append((k0 * before + k1 * centre + k2 * after).astype(BF16))
        return found

    def mix_project(t):
        two = pl.ds(2 * t, 2)
        rows_of = lambda i: [mixed_rows(2 * t + i, HALO, frames, lane) for lane in lanes]
        found = [rows_of(0), rows_of(1)]
        acts = [
            jnp.concatenate([jnp.concatenate([m[n] for m in half], axis=1) for half in found], axis=0)
            for n in range(3)
        ]
        values = [nn(act, wqkv[n]).astype(BF16) for n, act in enumerate(acts)]
        for (kept, dst, skip), act, value in zip(streams, acts, values):
            kept[two] = act.reshape(2, frames, feats)
            dst[two, pl.ds(skip, frames), :] = value.reshape(2, frames, feats)

    loop(pairs, mix_project)
    to_next.wait_recv()
    to_prev.wait_recv()
    ends = 2 * HALO

    def norm_halo(i):
        four = pl.ds(pl.multiple_of(4 * i, 4), 4)
        for src, at in ((halo_lo, PAD), (halo_hi, own + frames)):
            value = normed_rows(src[four].reshape(4 * HALO, feats))
            nf[four, pl.ds(at, HALO), :] = value.reshape(4, HALO, feats)

    loop(seqs // 4, norm_halo)

    def mix_ends(s):
        sides = ((0, 0, HALO, 0), (ends, frames, 0, frames - HALO))
        found = [[mixed_rows(s, start, ends, lane) for lane in lanes] for _, start, _, _ in sides]
        for (at, _, keep, row), half in zip(sides, found):
            for n in range(3):
                mixed = jnp.concatenate([m[n] for m in half], axis=1)
                tile = pl.ds(pl.multiple_of((n * seqs + s) * 2 * ends + at, ends), ends)
                hid[tile, :] = mixed
                streams[n][0][s, pl.ds(row, HALO), :] = mixed[keep : keep + HALO]

    loop(seqs, mix_ends)
    for n, (_, dst, skip) in enumerate(streams):
        count = seqs * 2 * ends
        value = nn(hid[pl.ds(n * count, count), :], wqkv[n]).astype(BF16).reshape(seqs, 2 * ends, feats)
        piece = lambda first, last: lax.slice_in_dim(value, first, last, axis=1)
        if skip:
            dst[:, pl.ds(0, ends), :] = piece(0, ends)
            dst[:, pl.ds(frames, ends), :] = piece(ends, 2 * ends)
        else:
            dst[:, pl.ds(0, HALO), :] = piece(HALO, ends)
            dst[:, pl.ds(frames - HALO, HALO), :] = piece(ends, ends + HALO)

    def attend(s):
        key = lax.broadcasted_iota(jnp.int32, (ext, frames), 0) - HALO
        query = lax.broadcasted_iota(jnp.int32, (ext, frames), 1)
        band = (key - query <= HALF) & (key - query >= -HALF)
        pos_k = key + base
        pos_q = lax.broadcasted_iota(jnp.int32, (8, frames), 1) + base
        seg_k = jnp.zeros((ext, frames), jnp.int32)
        seg_q = jnp.zeros((8, frames), jnp.int32)
        for bound in bounds_of(s):
            seg_k = seg_k + (pos_k >= bound).astype(jnp.int32)
            seg_q = seg_q + (pos_q >= bound).astype(jnp.int32)
        allowed = band & (seg_k == seg_q[0:1]) & (pos_k >= 0) & (pos_k < seq_length)
        bias = jnp.where(allowed, 0.0, -1e30)
        heads = [pl.ds(h * HD, HD) for h in range(HEADS)]
        scores = [nt(ks[s, :, head], qs[s, :, head]) * temper + bias for head in heads]
        raised = [jnp.exp(value - jnp.max(value, axis=0, keepdims=True)) for value in scores]
        probs = [value * (1.0 / jnp.sum(value, axis=0, keepdims=True)) for value in raised]
        for h, head in enumerate(heads):
            prob[s, h] = probs[h]
        found = [tn(probs[h].astype(BF16), vs[s, :, head]) for h, head in enumerate(heads)]
        for h, head in enumerate(heads):
            att[s, :, head] = found[h].astype(BF16)

    loop(seqs, attend)
    for load in loads[2:]:
        load.wait()
    tall = 2 * frames
    chunk = feats
    tokens = seqs * frames
    def flat(ref, t):
        return ref[pl.ds(2 * t, 2)].reshape(tall, ref.shape[2])

    def back(value):
        return value.reshape(2, frames, feats)

    def residual_norm(t):
        two = pl.ds(2 * t, 2)
        residual = flat(x, t).astype(F32) + nn(flat(att, t), wout[...])
        d_mlp = (flat(cot, t).astype(F32) * scale).astype(BF16)
        centered, r = moments(residual)
        normed_two = (centered * r * gain_two).astype(BF16)
        res[two] = back(residual)
        n2[two] = back(normed_two)
        dm[two] = back(d_mlp)

    loop(pairs, residual_norm)
    whole = lambda ref: ref[...].reshape(seqs * frames, ref.shape[2])
    early = pl.ds(0, frames)

    def place(block, value):
        part[block // per_unit, pl.ds((block % per_unit) * feats, feats), :] = value.astype(BF16)

    ff_blocks = ff // feats

    def unit_begun(block):
        return block // per_unit if block % per_unit == per_unit - 1 else None

    placed, tail, _ = plan_steps(orders, small_steps, rows, feats, make_pieces(seqs, ff_blocks, per_unit))

    def advance(u, i):
        red.tick(u, i)

    def slot(name, index=None, count=0):
        if index is None:
            for u, i in placed[name]:
                advance(u, i)
            return
        for k in range(count):
            if placed[name + (k,)]:
                pl.when(index == k)(lambda k=k: [advance(u, i) for u, i in placed[name + (k,)]] and None)

    def begin(block):
        u = unit_begun(block)
        if u is not None:
            advance(u, 0)

    mlp_sum, e_sum = dke, dve

    for j in range(ff_blocks):
        cols = pl.ds(j * chunk, chunk)

        def hidden_chunk(t, j=j, cols=cols):
            upper = nn(flat(n2, t), wup[:, cols])
            d_hidden = nt(flat(dm, t), wdown[cols, :])
            value, slope = gelu_pair(upper)
            value, slope = value.astype(BF16), (slope * d_hidden).astype(BF16)
            tile = pl.ds(pl.multiple_of(j * tokens + t * tall, tall), tall)
            mlp_part, e_part = nn(value, wdown[cols, :]), nt(slope, wup[:, cols])
            two = pl.ds(2 * t, 2)
            if j:
                mlp_part = mlp_part + mlp_sum[two, early, :].reshape(tall, feats)
                e_part = e_part + e_sum[two, early, :].reshape(tall, feats)
            hid[tile, :] = value
            du[tile, :] = slope
            mlp_sum[two, early, :] = back(mlp_part)
            e_sum[two, early, :] = back(e_part)
            slot(("f", j), t, pairs)

        loop(pairs, hidden_chunk)
        rows_j = pl.ds(j * tokens, tokens)
        place(j, tn(hid[rows_j, :], whole(dm)))
        begin(j)
        slot(("d", j))
        place(ff_blocks + j, tn(whole(n2), du[rows_j, :]))
        begin(ff_blocks + j)
        slot(("u", j))

    def feed_back(t):
        two = pl.ds(2 * t, 2)
        mlp_out = mlp_sum[two, early, :].reshape(tall, feats)
        e = e_sum[two, early, :].reshape(tall, feats)
        residual = flat(res, t)
        cotan = flat(cot, t).astype(F32)
        output = (residual + scale * mlp_out).astype(BF16)
        centered, r = moments(residual)
        xhat = centered * r
        eg = e * gain_two
        d_res = cotan + r * (
            eg - jnp.mean(eg, axis=-1, keepdims=True) - xhat * jnp.mean(eg * xhat, axis=-1, keepdims=True)
        )
        d_branch = d_res.astype(BF16)
        d_att = nt(d_branch, wout[...]).astype(BF16)
        scale_sum = sums[11] + fold(cotan * mlp_out)
        gain_sum = sums[10] + fold(e * xhat)
        outs[two] = back(output)
        res[two] = back(d_res)
        dbr[two] = back(d_branch)
        da[two] = back(d_att)
        sums[11] = scale_sum
        sums[10] = gain_sum
        slot(("x",), t, pairs)

    loop(pairs, feed_back)


    dq = dm
    dkl, dvl = n2, att

    exchange = []
    for t in range(pairs):
        two = pl.ds(2 * t, 2)
        exchange += [
            Across(msg_hi.at[two], got_lo.at[two], 4 + 2 * t, 0),
            Across(msg_lo.at[two], got_hi.at[two], 5 + 2 * t, 1),
        ]
    exchange += [Across(dq_hi, dq_got_lo, 2, 0), Across(dq_lo, dq_got_hi, 3, 1)]

    def attend_back(s):
        heads = [pl.ds(h * HD, HD) for h in range(HEADS)]
        d_atts = [da[s, :, head] for head in heads]
        probs = [prob[s, h] for h in range(HEADS)]
        d_weights = [nt(vs[s, :, head], d_att) for head, d_att in zip(heads, d_atts)]
        d_scores = [
            (p * (d_w - jnp.sum(p * d_w, axis=0, keepdims=True))).astype(BF16) for p, d_w in zip(probs, d_weights)
        ]
        found = [
            (tn(d_s, ks[s, :, head]), nn(d_s, qs[s, :, head]), nn(p.astype(BF16), d_att))
            for head, d_s, p, d_att in zip(heads, d_scores, probs, d_atts)
        ]
        for head, (d_q, d_k, d_v) in zip(heads, found):
            dq[s, :, head] = (d_q * temper).astype(BF16)
            dke[s, :, head] = d_k * temper
            dve[s, :, head] = d_v
        for i, src in enumerate((dke, dve)):
            cols = pl.ds(i * feats, feats)
            msg_hi[s, :, cols] = src[s, pl.ds(HALO + frames - 1, HALO), :].astype(BF16)
            msg_lo[s, :, cols] = src[s, pl.ds(1, HALO), :].astype(BF16)
        dq_hi[pl.ds(s, 1), :] = dq[s, pl.ds(frames - 16, 16), :].astype(F32)[15:16]
        dq_lo[pl.ds(s, 1), :] = dq[s, pl.ds(0, 16), :].astype(F32)[0:1]
        for t in range(pairs):
            pl.when(s == 2 * t + 1)(lambda t=t: [copy.start() for copy in exchange[2 * t : 2 * t + 2]] and None)
        slot(("b",), s, seqs)

    loop(seqs, attend_back)
    for copy in exchange[2 * pairs :]:
        copy.start()
    place(2 * ff_blocks + 1, tn(whole(act_q), whole(dq)))
    begin(2 * ff_blocks + 1)
    slot("q")
    place(2 * ff_blocks, tn(whole(att), whole(dbr)))
    begin(2 * ff_blocks)
    slot("o")
    for copy in exchange:
        copy.wait_recv()
    edge[0, pl.ds(0, seqs), :] = dq_got_lo[...]
    edge[0, pl.ds(seqs, seqs), :] = dq_got_hi[...]

    def settle(s):
        for i, (src, dst) in enumerate(((dke, dkl), (dve, dvl))):
            cols = pl.ds(i * feats, feats)
            low = pl.ds(HALO - 1, HALO)
            high = pl.ds(HALO + frames - HALO + 1, HALO)
            src[s, low, :] = src[s, low, :] + got_lo[s, :, cols].astype(F32)
            src[s, high, :] = src[s, high, :] + got_hi[s, :, cols].astype(F32)
            dst[s] = src[s, pl.ds(HALO, frames), :].astype(BF16)
            edge[i + 1, pl.ds(s, 1), :] = src[s, pl.ds(HALO - 1, 1), :]
            edge[i + 1, pl.ds(seqs + s, 1), :] = src[s, pl.ds(HALO + frames, 1), :]

    loop(seqs, settle)
    slot("w")
    place(2 * ff_blocks + 2, tn(whole(act_k), whole(dkl)))
    begin(2 * ff_blocks + 2)
    slot("k")
    place(2 * ff_blocks + 3, tn(whole(act_v), whole(dvl)))
    begin(2 * ff_blocks + 3)
    slot("v")
    for n in range(3):
        edge_mix[n] = nt(edge[n].astype(BF16), wqkv[n])

    def input_grads(t):
        two = pl.ds(2 * t, 2)
        for n, src in enumerate((dq, dkl, dvl)):
            value = nt(src[two].reshape(tall, feats), wqkv[n])
            dmx[n, :, pl.ds(PAD, frames), :] = value.reshape(2, frames, feats)
        for i in range(2):
            s = 2 * t + i
            for n in range(3):
                dmx[n, i, pl.ds(PAD - 1, 1), :] = edge_mix[n, pl.ds(s, 1), :]
                dmx[n, i, pl.ds(PAD + frames, 1), :] = edge_mix[n, pl.ds(seqs + s, 1), :]
            here = link[s, pl.ds(own, frames), :]
            after = link[s, pl.ds(own + 1, frames), :]
            e_parts, taps = [], []
            for lane in lanes:
                left = nf[s, pl.ds(own - 1, frames), lane] * here
                mid = nf[s, pl.ds(own, frames), lane]
                right = nf[s, pl.ds(own + 1, frames), lane] * after
                from_left, from_mid, from_right = 0.0, 0.0, 0.0
                for n in range(3):
                    k0, k1, k2 = (params[pl.ds(3 * n + c, 1), lane] for c in range(3))
                    g = dmx[n, i, pl.ds(PAD, frames), lane]
                    taps.append([fold(g * left), fold(g * mid), fold(g * right)])
                    from_mid = from_mid + k1 * g
                    from_right = from_right + k0 * dmx[n, i, pl.ds(PAD + 1, frames), lane]
                    from_left = from_left + k2 * dmx[n, i, pl.ds(PAD - 1, frames), lane]
                e_parts.append(from_mid + from_right * after + from_left * here)
            e = jnp.concatenate(e_parts, axis=1)
            centered, r = moments(x[s].astype(F32))
            xhat = centered * r
            eg = e * gain_one
            d_in = res[s] + r * (
                eg - jnp.mean(eg, axis=-1, keepdims=True) - xhat * jnp.mean(eg * xhat, axis=-1, keepdims=True)
            )
            for n in range(3):
                for c in range(3):
                    tap = jnp.concatenate([taps[3 * l + n][c] for l in range(len(lanes))], axis=1)
                    sums[3 * n + c] = sums[3 * n + c] + tap
            sums[9] = sums[9] + fold(e * xhat)
            res[s] = d_in
            for k in range(i, seqs, 2):
                if placed[("i", k)]:
                    pl.when(s == k)(lambda k=k: [advance(u, step) for u, step in placed[("i", k)]] and None)

    loop(pairs, input_grads)
    small_cur[0] = jnp.sum(sums[...], axis=1)

    def small_copy(level):
        peer = peer_of(small_steps[level], 1)
        return pltpu.make_async_remote_copy(
            src_ref=small_cur.at[level], dst_ref=small_recv.at[level],
            send_sem=sm_send.at[level], recv_sem=sm_recv.at[level],
            device_id=peer, device_id_type=MESH,
        )

    small_copy(0).start()
    for u, small_at in tail:
        if u >= 0:
            advance(u, small_at)
            continue
        small_copy(small_at - 1).wait_recv()
        total = small_cur[small_at - 1] + small_recv[small_at - 1]
        if small_at < levels:
            small_cur[small_at] = total
            small_copy(small_at).start()
        else:
            small_out[...] = total
    to_next.wait_send()
    to_prev.wait_send()
    for copy in exchange:
        copy.wait_send()
    for level in range(levels):
        small_copy(level).wait_send()
    for u in range(units):
        red.wait_sends(u)


def widen_kernel(
    places, outs, res, hid, du, small,
    output, d_inputs, d_gain_one, d_kernel, d_qkv, d_out, d_gain_two, d_up, d_down, d_scale, broad, sem,
):
    count, feats, _ = broad.shape
    ff_blocks = (count - 4) // 2
    passes = [pltpu.make_async_copy(src, dst, sem.at[count + i]) for i, (src, dst) in enumerate(((outs, output), (res, d_inputs)))]
    for put in passes:
        put.start()
    targets = [d_down.at[pl.ds(j * feats, feats)] for j in range(ff_blocks)]
    targets += [d_up.at[:, pl.ds(j * feats, feats)] for j in range(ff_blocks)]
    targets += [d_out] + [d_qkv.at[n] for n in range(3)]
    stores = []
    for i, (which, start) in enumerate(places):
        src = (hid, du)[which]

        def widen(r, src=src, start=start, i=i):
            here = pl.ds(pl.multiple_of(r * 64, 64), 64)
            broad[i, here, :] = src[pl.ds(pl.multiple_of(start + r * 64, 64), 64), :].astype(F32)

        loop(feats // 64, widen)
        stores.append(pltpu.make_async_copy(broad.at[i], targets[i], sem.at[i]))
        stores[-1].start()
    for n in range(3):
        d_kernel[n] = small[pl.ds(3 * n, 3), :]
    for i, dst in enumerate((d_gain_one, d_gain_two, d_scale)):
        dst[...] = small[pl.ds(9 + i, 1), :].reshape(feats)
    for store in passes + stores:
        store.wait()


def shards(
    inputs, lengths, norm_gain, conv_kernel, qkv_weight, out_weight, mlp_gain, up_weight,
    down_weight, layer_scale, cotangent,
):
    seqs, frames, feats = inputs.shape
    ff = up_weight.shape[1]
    seq_size, tm_size = lax.axis_size("seq"), lax.axis_size("tm")
    rows = max(feats, 16 * seq_size * tm_size)
    units = (2 * ff + 4 * feats) // rows
    kinds, orders = step_orders(seq_size, tm_size)
    orders, small_steps = orders[:units], kinds[6]
    levels = len(small_steps)
    copies = max(sum((1 << len(bits)) - 1 for bits in order) for order in orders)
    ext = frames + 2 * HALO
    dma = pltpu.SemaphoreType.DMA
    any_spec = pl.BlockSpec(memory_space=pl.ANY)
    vmem_spec = pl.BlockSpec(memory_space=pltpu.VMEM)
    low = lambda *shape: pltpu.VMEM(shape, BF16)
    wide = lambda *shape: pltpu.VMEM(shape, F32)
    acts = lambda: low(seqs, frames, feats)
    acts_ext = lambda: low(seqs, ext, feats)
    scratch = [
        wide(16, feats), acts(), acts(), low(3, feats, feats), low(feats, feats), low(feats, ff), low(ff, feats),
        low(seqs, HALO, feats), low(seqs, HALO, feats),
        wide(seqs, ext + 2 * PAD, feats), wide(seqs, ext + 2 * PAD, 128),
        acts(), acts(), acts(), acts(), acts_ext(), acts_ext(),
        wide(seqs, HEADS, ext, frames), acts(), acts(), acts(),
        acts(), acts(),
        wide(seqs, ext, feats), wide(seqs, ext, feats), wide(3, 2, frames + 2 * PAD, feats),
        low(seqs, HALO, 2 * feats), low(seqs, HALO, 2 * feats), low(seqs, HALO, 2 * feats), low(seqs, HALO, 2 * feats),
        wide(seqs, feats), wide(seqs, feats), wide(seqs, feats), wide(seqs, feats),
        wide(3, 2 * seqs, feats), wide(3, 2 * seqs, feats), wide(16, 8, feats),
        wide(levels, 16, feats), wide(levels, 16, feats),
        low(units, rows, feats), low(units, rows, feats),
        dma((6,)), dma((4 + seqs,)), dma((4 + seqs,)),
        dma((units, copies)), dma((units, copies)), dma((units, copies)), dma((units, copies)),
        dma((levels,)), dma((levels,)),
    ]
    cfg = (orders, small_steps, rows, seqs, frames, feats, ff, tm_size)
    out_type = jax.ShapeDtypeStruct
    stay = lambda v: pltpu.with_memory_space_constraint(v, pltpu.HBM)
    held = out_type((seqs * frames * ff // feats, feats), BF16)
    outs, res, hid, du, small = pl.pallas_call(
        functools.partial(layer_kernel, cfg),
        out_shape=(
            pltpu.VMEM(inputs.shape, BF16), pltpu.VMEM(inputs.shape, F32), pltpu.VMEM(held.shape, BF16),
            pltpu.VMEM(held.shape, BF16), pltpu.VMEM((16, feats), F32),
        ),
        in_specs=[pl.BlockSpec(memory_space=pltpu.SMEM), any_spec] + [vmem_spec] * 4 + [any_spec] * 5,
        out_specs=(vmem_spec,) * 5,
        scratch_shapes=scratch,
        compiler_params=pltpu.CompilerParams(
            collective_id=0, has_side_effects=True, vmem_limit_bytes=50 << 20
        ),
    )(
        lengths, stay(inputs), norm_gain, conv_kernel, mlp_gain, layer_scale, stay(qkv_weight), stay(out_weight),
        stay(up_weight), stay(down_weight), stay(cotangent),
    )
    count = (2 * ff + 4 * feats) // feats
    per_unit = rows // feats
    places = []
    for block in range(count):
        which, start = gathered_at(block // per_unit, rows, *held.shape)
        places.append((which, start + block % per_unit * feats))
    hbm_spec = pl.BlockSpec(memory_space=pltpu.HBM)
    return pl.pallas_call(
        functools.partial(widen_kernel, places),
        out_shape=(
            out_type(inputs.shape, BF16), out_type(inputs.shape, F32),
            out_type((feats,), F32), out_type((3, 3, feats), F32), out_type((3, feats, feats), F32),
            out_type((feats, feats), F32), out_type((feats,), F32), out_type((feats, ff), F32),
            out_type((ff, feats), F32), out_type((feats,), F32),
        ),
        in_specs=[vmem_spec] * 5,
        out_specs=(hbm_spec,) * 2 + (vmem_spec, vmem_spec, hbm_spec, hbm_spec, vmem_spec, hbm_spec, hbm_spec, vmem_spec),
        scratch_shapes=[wide(count, feats, feats), dma((count + 2,))],
        compiler_params=pltpu.CompilerParams(vmem_limit_bytes=16 << 20),
    )(outs, res, hid, du, small)


def solution(mesh):
    split = P("seq", "tm", None)
    return jax.shard_map(
        shards,
        mesh=mesh,
        in_specs=(split, P("seq", None)) + (P(),) * 8 + (split,),
        out_specs=(split, split) + (P(),) * 8,
        check_vma=False,
    )
```

```python
import functools

import jax
import jax.numpy as jnp
from jax import lax
from jax.experimental import pallas as pl
from jax.experimental.pallas import tpu as pltpu
from jax.sharding import PartitionSpec as P

HEADS = 4
HD = 128
HALF = 9
HALO = 16
PAD = 8
EPS = 1e-05
MESH = pl.DeviceIdType.MESH
F32 = jnp.float32
BF16 = jnp.bfloat16


LEAD = (5, 0, 2, 2, 0, 0, 5, 0, -3, 2, 10, 10)
CHOICE = (4, 3, 6, 1, 0, 1, 2, 4, 0, 1, 0, 1)


def step_orders(seq_size, tm_size):
    seq_bits = [("seq", b) for b in range(seq_size.bit_length() - 1)]
    tm_bits = [("tm", b) for b in range(tm_size.bit_length() - 1)]
    one = lambda bits: [(bit,) for bit in bits]
    two = lambda bits: [tuple(bits[i : i + 2]) for i in range(0, len(bits), 2)]
    core, rest = one(tm_bits[:1]), tm_bits[1:]
    swapped = seq_bits[::-1]
    kinds = [
        core + one(seq_bits) + two(rest),
        core + one(swapped) + two(rest),
        core + one(rest[:1]) + one(seq_bits) + one(rest[1:]),
        core + one(rest[:1]) + one(swapped) + one(rest[1:]),
        core + two(seq_bits) + two(rest),
        core + two(rest) + two(seq_bits),
        core + one(seq_bits) + one(rest),
        core + one(swapped) + one(rest),
        core + two(rest) + one(seq_bits),
        core + two(rest) + one(swapped),
        core + two(seq_bits) + one(rest),
        core + one(seq_bits[:1]) + two(rest) + one(seq_bits[1:]),
        core + one(swapped[:1]) + two(rest) + one(swapped[1:]),
        core + one(seq_bits[:1]) + one(rest[:1]) + one(seq_bits[1:]) + one(rest[1:]),
        core + one(swapped[:1]) + one(rest[:1]) + one(swapped[1:]) + one(rest[1:]),
    ]
    return kinds, [kinds[c] for c in CHOICE]


def bit_of(axis, bit):
    return lax.rem(lax.axis_index(axis) // (1 << bit), 2)


def peer_of(bits, flips):
    at = {"seq": lax.axis_index("seq"), "tm": lax.axis_index("tm")}
    for i, (axis, bit) in enumerate(bits):
        if flips >> i & 1:
            at[axis] = at[axis] + (1 - 2 * bit_of(axis, bit)) * (1 << bit)
    return at["seq"], at["tm"]


def digit_of(bits, flips=0):
    total = 0
    for i, (axis, bit) in enumerate(bits):
        mine = bit_of(axis, bit)
        total = total + (1 - mine if flips >> i & 1 else mine) * (1 << i)
    return total


def gathered_at(unit, rows, held_rows, feats):
    held = held_rows // rows
    index = unit % held
    if unit < held and rows == feats:
        half = held // 2
        index = 2 * (unit % half) + unit // half
    return unit // held, index * rows


class Reducer:
    def __init__(self, orders, rows, part, recv, fulls, sems):
        self.orders, self.rows = orders, rows
        self.part, self.recv, self.fulls = part, recv, fulls
        self.rs_send, self.rs_recv, self.ag_send, self.ag_recv = sems

    def levels(self, unit):
        return len(self.orders[unit])

    def size(self, unit, level):
        return self.rows >> sum(len(bits) for bits in self.orders[unit][:level])

    def owned(self, unit, level):
        off = 0
        for i in range(level):
            off = off + digit_of(self.orders[unit][i]) * self.size(unit, i + 1)
        return off

    def peers(self, unit, level):
        return range(1, 1 << len(self.orders[unit][level]))

    def slot(self, unit, level, flips):
        return sum((1 << len(bits)) - 1 for bits in self.orders[unit][:level]) + flips - 1

    def landing(self, unit, level, flips):
        return self.rows - self.size(unit, level) + (flips - 1) * self.size(unit, level + 1)

    def scatter_copies(self, unit, level):
        bits, found = self.orders[unit][level], []
        size = self.size(unit, level + 1)
        for flips in self.peers(unit, level):
            off = pl.multiple_of(self.owned(unit, level) + digit_of(bits, flips) * size, 16)
            at = self.slot(unit, level, flips)
            found.append(pltpu.make_async_remote_copy(
                src_ref=self.part.at[unit, pl.ds(off, size)],
                dst_ref=self.recv.at[unit, pl.ds(self.landing(unit, level, flips), size)],
                send_sem=self.rs_send.at[unit, at],
                recv_sem=self.rs_recv.at[unit, at],
                device_id=peer_of(bits, flips),
                device_id_type=MESH,
            ))
        return found

    def full(self, unit):
        which, start = gathered_at(unit, self.rows, *self.fulls[0].shape)
        return self.fulls[which], start

    def gather_copies(self, unit, level):
        bits, found = self.orders[unit][level], []
        ref, start = self.full(unit)
        off = pl.multiple_of(start + self.owned(unit, level + 1), 16)
        region = ref.at[pl.ds(off, self.size(unit, level + 1))]
        for flips in self.peers(unit, level):
            at = self.slot(unit, level, flips)
            found.append(pltpu.make_async_remote_copy(
                src_ref=region,
                dst_ref=region,
                send_sem=self.ag_send.at[unit, at],
                recv_sem=self.ag_recv.at[unit, at],
                device_id=peer_of(bits, flips),
                device_id_type=MESH,
            ))
        return found

    def combine(self, unit, level):
        for copy in self.scatter_copies(unit, level):
            copy.wait_recv()
        off, size = self.owned(unit, level + 1), self.size(unit, level + 1)
        step = min(size, 32)

        def body(i, carry):
            here = pl.ds(pl.multiple_of(off + i * step, 16), step)
            total = self.part[unit, here, :].astype(F32)
            for flips in self.peers(unit, level):
                there = pl.ds(pl.multiple_of(self.landing(unit, level, flips) + i * step, 16), step)
                total = total + self.recv[unit, there, :].astype(F32)
            if level == self.levels(unit) - 1:
                ref, start = self.full(unit)
                ref[pl.ds(pl.multiple_of(start + off + i * step, 16), step), :] = total.astype(BF16)
            else:
                self.part[unit, here, :] = total.astype(BF16)
            return carry

        lax.fori_loop(0, size // step, body, 0)

    def tick(self, unit, i):
        levels = self.levels(unit)
        if 0 < i <= levels:
            self.combine(unit, i - 1)
        elif i > levels:
            for copy in self.gather_copies(unit, 2 * levels - i):
                copy.wait_recv()
        if i < levels:
            out = self.scatter_copies(unit, i)
        elif i < 2 * levels:
            out = self.gather_copies(unit, 2 * levels - 1 - i)
        else:
            out = []
        for copy in out:
            copy.start()

    def wait_sends(self, unit):
        for level in range(self.levels(unit)):
            for copy in self.scatter_copies(unit, level) + self.gather_copies(unit, level):
                copy.wait_send()


def plan_steps(orders, small_steps, rows, feats, pieces, lead):
    core_rate, link_rate = 600e3, 104e3
    free, reached, arrival = {}, {}, {}
    levels = {u: len(order) for u, order in enumerate(orders)}
    levels[-1] = len(small_steps)

    def size_of(unit, level):
        return (rows >> sum(len(bits) for bits in orders[unit][: level + 1])) * feats * 2

    def send(unit, now, level):
        bits = (orders[unit] if unit >= 0 else small_steps)[level]
        size = size_of(unit, level) if unit >= 0 else 16 * feats * 4
        wire = 2 * size / link_rate
        near, far = ("tm", 1), ("tm", 2)
        if bits[0] == ("tm", 0):
            uses, lag = [("core", size / core_rate)], 1.1
        elif len(bits) == 2:
            if bits[0][0] == "seq":
                uses, lag = [(bit, 2 * wire) for bit in bits], 3.3
            else:
                uses, lag = [(near, 3 * wire), (far, 4 * wire)], 4.0
        elif bits[0][0] == "seq" or bits[0] == near:
            uses, lag = [(bits[0], wire)], 2.6
        else:
            uses, lag = [(near, wire), (far, 2 * wire)], 3.3
        start = max([now] + [free.get(name, 0.0) for name, _ in uses])
        for name, busy in uses:
            free[name] = start + busy
        return start + max(busy for _, busy in uses) + lag

    def step(unit, now):
        i = reached[unit]
        reached[unit] = i + 1
        cost = 0.05
        if unit >= 0:
            cost = 0.02 + (size_of(unit, i - 1) / 2.4e6 if 0 < i <= levels[unit] else 0.0)
        if i < levels[unit]:
            arrival[unit] = send(unit, now + cost, i)
        elif i < last(unit):
            arrival[unit] = send(unit, now + cost, 2 * levels[unit] - 1 - i)
        return cost

    def last(unit):
        return levels[unit] if unit < 0 else 2 * levels[unit]

    now, crossed, placed = 0.0, 0.0, {}
    for slot, us, begins in pieces:
        now = (max(now, crossed) if slot == "w" else now) + us
        if slot[0] == "b" and slot[1] % 2:
            free[("tm", 1)] = max(now, free.get(("tm", 1), 0.0)) + 0.65
            free[("tm", 2)] = max(now, free.get(("tm", 2), 0.0)) + 0.65
            crossed = max(free[("tm", 1)], free[("tm", 2)]) + 2.6
        todo = []
        if begins is not None:
            reached[begins] = 0
            now += step(begins, now)
        while True:
            ready = [u for u in reached if reached[u] <= last(u) and arrival[u] <= now]
            if not ready:
                break
            unit = min(ready, key=lambda u: (arrival[u] - lead[u], u))
            todo.append((unit, reached[unit]))
            now += step(unit, now)
        placed[slot] = todo
    work_end = now
    reached[-1] = 0
    now += step(-1, now)
    tail = []
    while True:
        left = [u for u in reached if reached[u] <= last(u)]
        if not left:
            break
        unit = min(left, key=lambda u: (arrival[u], u))
        now = max(now, arrival[unit])
        tail.append((unit, reached[unit]))
        now += step(unit, now)
    return placed, tail, (work_end, now)


def make_pieces(seqs, ff_blocks, per_unit):
    pairs = seqs // 2
    begun = lambda block: block // per_unit if block % per_unit == per_unit - 1 else None
    pieces = []
    for j in range(ff_blocks):
        pieces += [(("f", j, t), 1.53, None) for t in range(seqs // 4)]
        pieces += [(("d", j), 0.73, begun(j)), (("u", j), 0.73, begun(ff_blocks + j))]
    pieces += [(("x", t), 0.63, None) for t in range(pairs)]
    pieces += [(("b", s), 0.64, None) for s in range(seqs)]
    pieces += [
        ("q", 0.73, begun(2 * ff_blocks + 1)), ("o", 0.73, begun(2 * ff_blocks)), ("w", 0.5, None),
        ("k", 0.73, begun(2 * ff_blocks + 2)), ("v", 0.73, begun(2 * ff_blocks + 3)),
    ]
    pieces += [(("i", s), 0.91, None) for s in range(seqs)]
    return pieces


def beside(tm_size):
    at = lax.axis_index("tm")
    seq = lax.axis_index("seq")
    return [(at < tm_size - 1, (seq, at + 1)), (at > 0, (seq, at - 1))]


def greet(bits, tm_size):
    barrier = pltpu.get_barrier_semaphore()
    for step, flips in bits:
        pl.semaphore_signal(barrier, inc=1, device_id=peer_of(step, flips), device_id_type=MESH)
    for there, peer in beside(tm_size):
        @pl.when(there)
        def _():
            pl.semaphore_signal(barrier, inc=1, device_id=peer, device_id_type=MESH)


def enter(bits, tm_size):
    count = len(bits)
    for there, _ in beside(tm_size):
        count = count + there.astype(jnp.int32)
    pl.semaphore_wait(pltpu.get_barrier_semaphore(), count)


def nn(a, b):
    return lax.dot_general(a, b, (((1,), (0,)), ((), ())), preferred_element_type=F32)


def nt(a, b):
    return lax.dot_general(a, b, (((1,), (1,)), ((), ())), preferred_element_type=F32)


def tn(a, b):
    return lax.dot_general(a, b, (((0,), (0,)), ((), ())), preferred_element_type=F32)


def moments(v):
    mean = jnp.mean(v, axis=-1, keepdims=True)
    centered = v - mean
    var = jnp.mean(centered * centered, axis=-1, keepdims=True)
    return centered, lax.rsqrt(var + EPS)


def fold(v):
    rows, cols = v.shape
    return jnp.sum(v.reshape(rows // 8, 8, cols), axis=0)


def gelu_pair(v):
    c = 0.7978845608028654
    square = v * v
    inner = v * (c + (c * 0.044715) * square)
    t = jnp.tanh(inner)
    half = 0.5 * (1.0 + t)
    slope = half + (0.5 * v) * (1.0 - t * t) * (c + (3.0 * 0.044715 * c) * square)
    return v * half, slope


def loop(count, body):
    def step(i, carry):
        body(i)
        return carry

    lax.fori_loop(0, count, step, 0)


def layer_kernel(cfg, *refs):
    (
        lengths, x_hbm, norm_gain, conv_kernel, mlp_gain, layer_scale, wqkv_hbm, wout_hbm, wup_hbm, wdown_hbm, cot_hbm,
        outs, res, hid, du, small_out,
        params, x, cot, wqkv, wout, wup, wdown, halo_lo, halo_hi, nf, link,
        act_q, act_k, act_v, qs, ks, vs, prob, att, n2, dm, dbr, da,
        dke, dve, dmx, msg_hi, msg_lo, got_lo, got_hi, dq_hi, dq_lo, dq_got_lo, dq_got_hi,
        edge, edge_mix, sums, small_cur, small_recv,
        part, recv,
        in_sem, halo_send, halo_recv, rs_send, rs_recv, ag_send, ag_recv, sm_send, sm_recv,
    ) = refs
    orders, small_steps, rows, seqs, frames, feats, ff, tm_size = cfg
    units = len(orders)
    levels = len(small_steps)
    greeted = sorted({(bits, flips) for order in orders + [small_steps] for bits in order for flips in range(1, 1 << len(bits))})
    known = {}
    for bits, flips in greeted:
        known.setdefault(tuple(bit for i, bit in enumerate(bits) if flips >> i & 1), (bits, flips))
    greeted = list(known.values())
    ext = frames + 2 * HALO
    own = PAD + HALO
    seq_length = frames * tm_size
    vids = lengths.shape[1]
    temper = HD ** (-0.5)
    lanes = [pl.ds(c * 128, 128) for c in range(feats // 128)]
    pairs = seqs // 2
    per_unit = rows // feats
    base = lax.axis_index("tm") * frames
    red = Reducer(orders, rows, part, recv, (hid, du), (rs_send, rs_recv, ag_send, ag_recv))

    loads = [
        pltpu.make_async_copy(src, dst, in_sem.at[i])
        for i, (src, dst) in enumerate(
            [(x_hbm, x), (wqkv_hbm, wqkv), (wout_hbm, wout), (wup_hbm, wup), (wdown_hbm, wdown), (cot_hbm, cot)]
        )
    ]
    loads[0].start()

    class Across:
        def __init__(self, src, dst, i, side):
            (self.sends, peer), (self.gets, _) = beside(tm_size)[side], beside(tm_size)[1 - side]
            self.copy = pltpu.make_async_remote_copy(
                src_ref=src, dst_ref=dst, send_sem=halo_send.at[i], recv_sem=halo_recv.at[i],
                device_id=peer, device_id_type=MESH,
            )

        def start(self):
            pl.when(self.sends)(lambda: self.copy.start())

        def wait_recv(self):
            pl.when(self.gets)(lambda: self.copy.wait_recv())

        def wait_send(self):
            pl.when(self.sends)(lambda: self.copy.wait_send())

    greet(greeted, tm_size)
    for n in range(3):
        params[pl.ds(3 * n, 3), :] = conv_kernel[n].astype(F32)
    for i, src in enumerate((norm_gain, mlp_gain, layer_scale)):
        params[pl.ds(9 + i, 1), :] = src[...].astype(F32).reshape(1, feats)

    def clear_missing(side, refs_in):
        there = beside(tm_size)[side][0]

        @pl.when(jnp.logical_not(there))
        def _():
            for ref in refs_in:
                ref[...] = jnp.zeros_like(ref)

    clear_missing(1, (halo_lo, got_lo, dq_got_lo))
    clear_missing(0, (halo_hi, got_hi, dq_got_hi))
    to_next = Across(x.at[:, pl.ds(frames - HALO, HALO)], halo_lo, 0, 0)
    to_prev = Across(x.at[:, pl.ds(0, HALO)], halo_hi, 1, 1)
    sums[...] = jnp.zeros_like(sums)

    def bounds_of(s):
        total, found = 0, []
        for j in range(vids):
            total = total + lengths[s, j]
            found.append(total)
        return found

    gain_one = params[pl.ds(9, 1), :]
    gain_two = params[pl.ds(10, 1), :]
    scale = params[pl.ds(11, 1), :]

    def normed_rows(rows_in):
        centered, r = moments(rows_in.astype(F32))
        return (centered * r * gain_one).astype(BF16).astype(F32)

    loads[0].wait()
    for load in loads[1:]:
        load.start()

    def norm_own(t):
        two = pl.ds(2 * t, 2)
        value = normed_rows(x[two].reshape(2 * frames, feats))
        pos = base - own + lax.broadcasted_iota(jnp.int32, (ext + 2 * PAD, 128), 0)
        links = []
        for i in range(2):
            cut = pos == 0
            for bound in bounds_of(2 * t + i):
                cut = cut | (pos == bound)
            links.append(jnp.where(cut, 0.0, 1.0))
        zero = jnp.zeros((2, PAD, feats), F32)
        nf[two, pl.ds(own, frames), :] = value.reshape(2, frames, feats)
        nf[two, pl.ds(0, PAD), :] = zero
        nf[two, pl.ds(PAD + ext, PAD), :] = zero
        for i in range(2):
            link[2 * t + i] = links[i]

    loop(pairs, norm_own)
    enter(greeted, tm_size)
    to_next.start()
    to_prev.start()
    loads[1].wait()
    streams = ((act_q, qs, 0), (act_k, ks, HALO), (act_v, vs, HALO))

    def mixed_rows(s, start, count, lane):
        before = nf[s, pl.ds(PAD + start - 1, count), lane] * link[s, pl.ds(PAD + start, count), :]
        centre = nf[s, pl.ds(PAD + start, count), lane]
        after = nf[s, pl.ds(PAD + start + 1, count), lane] * link[s, pl.ds(PAD + start + 1, count), :]
        found = []
        for n in range(3):
            k0, k1, k2 = (params[pl.ds(3 * n + c, 1), lane] for c in range(3))
            found.append((k0 * before + k1 * centre + k2 * after).astype(BF16))
        return found

    def mix_project(t):
        two = pl.ds(2 * t, 2)
        rows_of = lambda i: [mixed_rows(2 * t + i, HALO, frames, lane) for lane in lanes]
        found = [rows_of(0), rows_of(1)]
        acts = [
            jnp.concatenate([jnp.concatenate([m[n] for m in half], axis=1) for half in found], axis=0)
            for n in range(3)
        ]
        values = [nn(act, wqkv[n]).astype(BF16) for n, act in enumerate(acts)]
        for (kept, dst, skip), act, value in zip(streams, acts, values):
            kept[two] = act.reshape(2, frames, feats)
            dst[two, pl.ds(skip, frames), :] = value.reshape(2, frames, feats)

    loop(pairs, mix_project)
    to_next.wait_recv()
    to_prev.wait_recv()
    ends = 2 * HALO

    def norm_halo(i):
        four = pl.ds(pl.multiple_of(4 * i, 4), 4)
        for src, at in ((halo_lo, PAD), (halo_hi, own + frames)):
            value = normed_rows(src[four].reshape(4 * HALO, feats))
            nf[four, pl.ds(at, HALO), :] = value.reshape(4, HALO, feats)

    loop(seqs // 4, norm_halo)

    def mix_ends(s):
        sides = ((0, 0, HALO, 0), (ends, frames, 0, frames - HALO))
        found = [[mixed_rows(s, start, ends, lane) for lane in lanes] for _, start, _, _ in sides]
        for (at, _, keep, row), half in zip(sides, found):
            for n in range(3):
                mixed = jnp.concatenate([m[n] for m in half], axis=1)
                tile = pl.ds(pl.multiple_of((n * seqs + s) * 2 * ends + at, ends), ends)
                hid[tile, :] = mixed
                streams[n][0][s, pl.ds(row, HALO), :] = mixed[keep : keep + HALO]

    loop(seqs, mix_ends)
    for n, (_, dst, skip) in enumerate(streams):
        count = seqs * 2 * ends
        value = nn(hid[pl.ds(n * count, count), :], wqkv[n]).astype(BF16).reshape(seqs, 2 * ends, feats)
        piece = lambda first, last: lax.slice_in_dim(value, first, last, axis=1)
        if skip:
            dst[:, pl.ds(0, ends), :] = piece(0, ends)
            dst[:, pl.ds(frames, ends), :] = piece(ends, 2 * ends)
        else:
            dst[:, pl.ds(0, HALO), :] = piece(HALO, ends)
            dst[:, pl.ds(frames - HALO, HALO), :] = piece(ends, ends + HALO)

    def attend(s):
        key = lax.broadcasted_iota(jnp.int32, (ext, frames), 0) - HALO
        query = lax.broadcasted_iota(jnp.int32, (ext, frames), 1)
        band = (key - query <= HALF) & (key - query >= -HALF)
        pos_k = key + base
        pos_q = lax.broadcasted_iota(jnp.int32, (8, frames), 1) + base
        seg_k = jnp.zeros((ext, frames), jnp.int32)
        seg_q = jnp.zeros((8, frames), jnp.int32)
        for bound in bounds_of(s):
            seg_k = seg_k + (pos_k >= bound).astype(jnp.int32)
            seg_q = seg_q + (pos_q >= bound).astype(jnp.int32)
        allowed = band & (seg_k == seg_q[0:1]) & (pos_k >= 0) & (pos_k < seq_length)
        bias = jnp.where(allowed, 0.0, -1e30)
        heads = [pl.ds(h * HD, HD) for h in range(HEADS)]
        scores = [nt(ks[s, :, head], qs[s, :, head]) * temper + bias for head in heads]
        raised = [jnp.exp(value - jnp.max(value, axis=0, keepdims=True)) for value in scores]
        probs = [value * (1.0 / jnp.sum(value, axis=0, keepdims=True)) for value in raised]
        for h, head in enumerate(heads):
            prob[s, h] = probs[h]
        found = [tn(probs[h].astype(BF16), vs[s, :, head]) for h, head in enumerate(heads)]
        for h, head in enumerate(heads):
            att[s, :, head] = found[h].astype(BF16)

    loop(seqs, attend)
    for load in loads[2:]:
        load.wait()
    tall = 2 * frames
    chunk = feats
    tokens = seqs * frames
    def flat(ref, t):
        return ref[pl.ds(2 * t, 2)].reshape(tall, ref.shape[2])

    def back(value):
        return value.reshape(2, frames, feats)

    def residual_norm(t):
        two = pl.ds(2 * t, 2)
        residual = flat(x, t).astype(F32) + nn(flat(att, t), wout[...])
        d_mlp = (flat(cot, t).astype(F32) * scale).astype(BF16)
        centered, r = moments(residual)
        normed_two = (centered * r * gain_two).astype(BF16)
        res[two] = back(residual)
        n2[two] = back(normed_two)
        dm[two] = back(d_mlp)

    loop(pairs, residual_norm)
    whole = lambda ref: ref[...].reshape(seqs * frames, ref.shape[2])
    early = pl.ds(0, frames)

    def place(block, value):
        part[block // per_unit, pl.ds((block % per_unit) * feats, feats), :] = value.astype(BF16)

    ff_blocks = ff // feats

    def unit_begun(block):
        return block // per_unit if block % per_unit == per_unit - 1 else None

    placed, tail, _ = plan_steps(orders, small_steps, rows, feats, make_pieces(seqs, ff_blocks, per_unit), LEAD)

    def advance(u, i):
        red.tick(u, i)

    def slot(name, index=None, count=0):
        if index is None:
            for u, i in placed[name]:
                advance(u, i)
            return
        for k in range(count):
            if placed[name + (k,)]:
                pl.when(index == k)(lambda k=k: [advance(u, i) for u, i in placed[name + (k,)]] and None)

    def begin(block):
        u = unit_begun(block)
        if u is not None:
            advance(u, 0)

    mlp_sum, e_sum = dke, dve

    for j in range(ff_blocks):
        cols = pl.ds(j * chunk, chunk)

        def hidden_chunk(t, j=j, cols=cols):
            four = pl.ds(4 * t, 4)
            high = 4 * frames
            upper = nn(n2[four].reshape(high, feats), wup[:, cols])
            d_hidden = nt(dm[four].reshape(high, feats), wdown[cols, :])
            value, slope = gelu_pair(upper)
            value, slope = value.astype(BF16), (slope * d_hidden).astype(BF16)
            tile = pl.ds(pl.multiple_of(j * tokens + t * high, high), high)
            mlp_part, e_part = nn(value, wdown[cols, :]), nt(slope, wup[:, cols])
            if j:
                mlp_part = mlp_part + mlp_sum[four, early, :].reshape(high, feats)
                e_part = e_part + e_sum[four, early, :].reshape(high, feats)
            hid[tile, :] = value
            du[tile, :] = slope
            mlp_sum[four, early, :] = mlp_part.reshape(4, frames, feats)
            e_sum[four, early, :] = e_part.reshape(4, frames, feats)
            slot(("f", j), t, seqs // 4)

        loop(seqs // 4, hidden_chunk)
        rows_j = pl.ds(j * tokens, tokens)
        place(j, tn(hid[rows_j, :], whole(dm)))
        begin(j)
        slot(("d", j))
        place(ff_blocks + j, tn(whole(n2), du[rows_j, :]))
        begin(ff_blocks + j)
        slot(("u", j))

    def feed_back(t):
        two = pl.ds(2 * t, 2)
        mlp_out = mlp_sum[two, early, :].reshape(tall, feats)
        e = e_sum[two, early, :].reshape(tall, feats)
        residual = flat(res, t)
        cotan = flat(cot, t).astype(F32)
        output = (residual + scale * mlp_out).astype(BF16)
        centered, r = moments(residual)
        xhat = centered * r
        eg = e * gain_two
        d_res = cotan + r * (
            eg - jnp.mean(eg, axis=-1, keepdims=True) - xhat * jnp.mean(eg * xhat, axis=-1, keepdims=True)
        )
        d_branch = d_res.astype(BF16)
        d_att = nt(d_branch, wout[...]).astype(BF16)
        scale_sum = sums[11] + fold(cotan * mlp_out)
        gain_sum = sums[10] + fold(e * xhat)
        outs[two] = back(output)
        res[two] = back(d_res)
        dbr[two] = back(d_branch)
        da[two] = back(d_att)
        sums[11] = scale_sum
        sums[10] = gain_sum
        slot(("x",), t, pairs)

    loop(pairs, feed_back)


    dq = dm
    dkl, dvl = n2, att

    exchange = []
    for t in range(pairs):
        two = pl.ds(2 * t, 2)
        exchange += [
            Across(msg_hi.at[two], got_lo.at[two], 4 + 2 * t, 0),
            Across(msg_lo.at[two], got_hi.at[two], 5 + 2 * t, 1),
        ]
    exchange += [Across(dq_hi, dq_got_lo, 2, 0), Across(dq_lo, dq_got_hi, 3, 1)]

    def attend_back(s):
        heads = [pl.ds(h * HD, HD) for h in range(HEADS)]
        d_atts = [da[s, :, head] for head in heads]
        probs = [prob[s, h] for h in range(HEADS)]
        d_weights = [nt(vs[s, :, head], d_att) for head, d_att in zip(heads, d_atts)]
        d_scores = [
            (p * (d_w - jnp.sum(p * d_w, axis=0, keepdims=True))).astype(BF16) for p, d_w in zip(probs, d_weights)
        ]
        found = [
            (tn(d_s, ks[s, :, head]), nn(d_s, qs[s, :, head]), nn(p.astype(BF16), d_att))
            for head, d_s, p, d_att in zip(heads, d_scores, probs, d_atts)
        ]
        for head, (d_q, d_k, d_v) in zip(heads, found):
            dq[s, :, head] = (d_q * temper).astype(BF16)
            dke[s, :, head] = d_k * temper
            dve[s, :, head] = d_v
        for i, src in enumerate((dke, dve)):
            cols = pl.ds(i * feats, feats)
            msg_hi[s, :, cols] = src[s, pl.ds(HALO + frames - 1, HALO), :].astype(BF16)
            msg_lo[s, :, cols] = src[s, pl.ds(1, HALO), :].astype(BF16)
        dq_hi[pl.ds(s, 1), :] = dq[s, pl.ds(frames - 16, 16), :].astype(F32)[15:16]
        dq_lo[pl.ds(s, 1), :] = dq[s, pl.ds(0, 16), :].astype(F32)[0:1]
        for t in range(pairs):
            pl.when(s == 2 * t + 1)(lambda t=t: [copy.start() for copy in exchange[2 * t : 2 * t + 2]] and None)
        slot(("b",), s, seqs)

    loop(seqs, attend_back)
    for copy in exchange[2 * pairs :]:
        copy.start()
    place(2 * ff_blocks + 1, tn(whole(act_q), whole(dq)))
    begin(2 * ff_blocks + 1)
    slot("q")
    place(2 * ff_blocks, tn(whole(att), whole(dbr)))
    begin(2 * ff_blocks)
    slot("o")
    for copy in exchange:
        copy.wait_recv()
    edge[0, pl.ds(0, seqs), :] = dq_got_lo[...]
    edge[0, pl.ds(seqs, seqs), :] = dq_got_hi[...]

    def settle(s):
        for i, (src, dst) in enumerate(((dke, dkl), (dve, dvl))):
            cols = pl.ds(i * feats, feats)
            low = pl.ds(HALO - 1, HALO)
            high = pl.ds(HALO + frames - HALO + 1, HALO)
            src[s, low, :] = src[s, low, :] + got_lo[s, :, cols].astype(F32)
            src[s, high, :] = src[s, high, :] + got_hi[s, :, cols].astype(F32)
            dst[s] = src[s, pl.ds(HALO, frames), :].astype(BF16)
            edge[i + 1, pl.ds(s, 1), :] = src[s, pl.ds(HALO - 1, 1), :]
            edge[i + 1, pl.ds(seqs + s, 1), :] = src[s, pl.ds(HALO + frames, 1), :]

    loop(seqs, settle)
    slot("w")
    place(2 * ff_blocks + 2, tn(whole(act_k), whole(dkl)))
    begin(2 * ff_blocks + 2)
    slot("k")
    place(2 * ff_blocks + 3, tn(whole(act_v), whole(dvl)))
    begin(2 * ff_blocks + 3)
    slot("v")
    for n in range(3):
        edge_mix[n] = nt(edge[n].astype(BF16), wqkv[n])

    def input_grads(t):
        two = pl.ds(2 * t, 2)
        for n, src in enumerate((dq, dkl, dvl)):
            value = nt(src[two].reshape(tall, feats), wqkv[n])
            dmx[n, :, pl.ds(PAD, frames), :] = value.reshape(2, frames, feats)
        for i in range(2):
            s = 2 * t + i
            for n in range(3):
                dmx[n, i, pl.ds(PAD - 1, 1), :] = edge_mix[n, pl.ds(s, 1), :]
                dmx[n, i, pl.ds(PAD + frames, 1), :] = edge_mix[n, pl.ds(seqs + s, 1), :]
            here = link[s, pl.ds(own, frames), :]
            after = link[s, pl.ds(own + 1, frames), :]
            e_parts, taps = [], []
            for lane in lanes:
                left = nf[s, pl.ds(own - 1, frames), lane] * here
                mid = nf[s, pl.ds(own, frames), lane]
                right = nf[s, pl.ds(own + 1, frames), lane] * after
                from_left, from_mid, from_right = 0.0, 0.0, 0.0
                for n in range(3):
                    k0, k1, k2 = (params[pl.ds(3 * n + c, 1), lane] for c in range(3))
                    g = dmx[n, i, pl.ds(PAD, frames), lane]
                    taps.append([fold(g * left), fold(g * mid), fold(g * right)])
                    from_mid = from_mid + k1 * g
                    from_right = from_right + k0 * dmx[n, i, pl.ds(PAD + 1, frames), lane]
                    from_left = from_left + k2 * dmx[n, i, pl.ds(PAD - 1, frames), lane]
                e_parts.append(from_mid + from_right * after + from_left * here)
            e = jnp.concatenate(e_parts, axis=1)
            centered, r = moments(x[s].astype(F32))
            xhat = centered * r
            eg = e * gain_one
            d_in = res[s] + r * (
                eg - jnp.mean(eg, axis=-1, keepdims=True) - xhat * jnp.mean(eg * xhat, axis=-1, keepdims=True)
            )
            for n in range(3):
                for c in range(3):
                    tap = jnp.concatenate([taps[3 * l + n][c] for l in range(len(lanes))], axis=1)
                    sums[3 * n + c] = sums[3 * n + c] + tap
            sums[9] = sums[9] + fold(e * xhat)
            res[s] = d_in
            for k in range(i, seqs, 2):
                if placed[("i", k)]:
                    pl.when(s == k)(lambda k=k: [advance(u, step) for u, step in placed[("i", k)]] and None)

    loop(pairs, input_grads)
    small_cur[0] = jnp.sum(sums[...], axis=1)

    def small_copy(level):
        peer = peer_of(small_steps[level], 1)
        return pltpu.make_async_remote_copy(
            src_ref=small_cur.at[level], dst_ref=small_recv.at[level],
            send_sem=sm_send.at[level], recv_sem=sm_recv.at[level],
            device_id=peer, device_id_type=MESH,
        )

    small_copy(0).start()
    for u, small_at in tail:
        if u >= 0:
            advance(u, small_at)
            continue
        small_copy(small_at - 1).wait_recv()
        total = small_cur[small_at - 1] + small_recv[small_at - 1]
        if small_at < levels:
            small_cur[small_at] = total
            small_copy(small_at).start()
        else:
            small_out[...] = total
    to_next.wait_send()
    to_prev.wait_send()
    for copy in exchange:
        copy.wait_send()
    for level in range(levels):
        small_copy(level).wait_send()
    for u in range(units):
        red.wait_sends(u)


def widen_kernel(
    places, outs, res, hid, du, small,
    output, d_inputs, d_gain_one, d_kernel, d_qkv, d_out, d_gain_two, d_up, d_down, d_scale, broad, sem,
):
    count, feats, _ = broad.shape
    ff_blocks = (count - 4) // 2
    passes = [pltpu.make_async_copy(src, dst, sem.at[count + i]) for i, (src, dst) in enumerate(((outs, output), (res, d_inputs)))]
    for put in passes:
        put.start()
    targets = [d_down.at[pl.ds(j * feats, feats)] for j in range(ff_blocks)]
    targets += [d_up.at[:, pl.ds(j * feats, feats)] for j in range(ff_blocks)]
    targets += [d_out] + [d_qkv.at[n] for n in range(3)]
    stores = []
    for i, (which, start) in enumerate(places):
        src = (hid, du)[which]

        def widen(r, src=src, start=start, i=i):
            here = pl.ds(pl.multiple_of(r * 64, 64), 64)
            broad[i, here, :] = src[pl.ds(pl.multiple_of(start + r * 64, 64), 64), :].astype(F32)

        loop(feats // 64, widen)
        stores.append(pltpu.make_async_copy(broad.at[i], targets[i], sem.at[i]))
        stores[-1].start()
    for n in range(3):
        d_kernel[n] = small[pl.ds(3 * n, 3), :]
    for i, dst in enumerate((d_gain_one, d_gain_two, d_scale)):
        dst[...] = small[pl.ds(9 + i, 1), :].reshape(feats)
    for store in passes + stores:
        store.wait()


def shards(
    inputs, lengths, norm_gain, conv_kernel, qkv_weight, out_weight, mlp_gain, up_weight,
    down_weight, layer_scale, cotangent,
):
    seqs, frames, feats = inputs.shape
    ff = up_weight.shape[1]
    seq_size, tm_size = lax.axis_size("seq"), lax.axis_size("tm")
    rows = max(feats, 16 * seq_size * tm_size)
    units = (2 * ff + 4 * feats) // rows
    kinds, orders = step_orders(seq_size, tm_size)
    orders, small_steps = orders[:units], kinds[6]
    levels = len(small_steps)
    copies = max(sum((1 << len(bits)) - 1 for bits in order) for order in orders)
    ext = frames + 2 * HALO
    dma = pltpu.SemaphoreType.DMA
    any_spec = pl.BlockSpec(memory_space=pl.ANY)
    vmem_spec = pl.BlockSpec(memory_space=pltpu.VMEM)
    low = lambda *shape: pltpu.VMEM(shape, BF16)
    wide = lambda *shape: pltpu.VMEM(shape, F32)
    acts = lambda: low(seqs, frames, feats)
    acts_ext = lambda: low(seqs, ext, feats)
    scratch = [
        wide(16, feats), acts(), acts(), low(3, feats, feats), low(feats, feats), low(feats, ff), low(ff, feats),
        low(seqs, HALO, feats), low(seqs, HALO, feats),
        wide(seqs, ext + 2 * PAD, feats), wide(seqs, ext + 2 * PAD, 128),
        acts(), acts(), acts(), acts(), acts_ext(), acts_ext(),
        wide(seqs, HEADS, ext, frames), acts(), acts(), acts(),
        acts(), acts(),
        wide(seqs, ext, feats), wide(seqs, ext, feats), wide(3, 2, frames + 2 * PAD, feats),
        low(seqs, HALO, 2 * feats), low(seqs, HALO, 2 * feats), low(seqs, HALO, 2 * feats), low(seqs, HALO, 2 * feats),
        wide(seqs, feats), wide(seqs, feats), wide(seqs, feats), wide(seqs, feats),
        wide(3, 2 * seqs, feats), wide(3, 2 * seqs, feats), wide(16, 8, feats),
        wide(levels, 16, feats), wide(levels, 16, feats),
        low(units, rows, feats), low(units, rows, feats),
        dma((6,)), dma((4 + seqs,)), dma((4 + seqs,)),
        dma((units, copies)), dma((units, copies)), dma((units, copies)), dma((units, copies)),
        dma((levels,)), dma((levels,)),
    ]
    cfg = (orders, small_steps, rows, seqs, frames, feats, ff, tm_size)
    out_type = jax.ShapeDtypeStruct
    stay = lambda v: pltpu.with_memory_space_constraint(v, pltpu.HBM)
    held = out_type((seqs * frames * ff // feats, feats), BF16)
    outs, res, hid, du, small = pl.pallas_call(
        functools.partial(layer_kernel, cfg),
        out_shape=(
            pltpu.VMEM(inputs.shape, BF16), pltpu.VMEM(inputs.shape, F32), pltpu.VMEM(held.shape, BF16),
            pltpu.VMEM(held.shape, BF16), pltpu.VMEM((16, feats), F32),
        ),
        in_specs=[pl.BlockSpec(memory_space=pltpu.SMEM), any_spec] + [vmem_spec] * 4 + [any_spec] * 5,
        out_specs=(vmem_spec,) * 5,
        scratch_shapes=scratch,
        compiler_params=pltpu.CompilerParams(
            collective_id=0, has_side_effects=True, vmem_limit_bytes=50 << 20
        ),
    )(
        lengths, stay(inputs), norm_gain, conv_kernel, mlp_gain, layer_scale, stay(qkv_weight), stay(out_weight),
        stay(up_weight), stay(down_weight), stay(cotangent),
    )
    count = (2 * ff + 4 * feats) // feats
    per_unit = rows // feats
    places = []
    for block in range(count):
        which, start = gathered_at(block // per_unit, rows, *held.shape)
        places.append((which, start + block % per_unit * feats))
    hbm_spec = pl.BlockSpec(memory_space=pltpu.HBM)
    return pl.pallas_call(
        functools.partial(widen_kernel, places),
        out_shape=(
            out_type(inputs.shape, BF16), out_type(inputs.shape, F32),
            out_type((feats,), F32), out_type((3, 3, feats), F32), out_type((3, feats, feats), F32),
            out_type((feats, feats), F32), out_type((feats,), F32), out_type((feats, ff), F32),
            out_type((ff, feats), F32), out_type((feats,), F32),
        ),
        in_specs=[vmem_spec] * 5,
        out_specs=(hbm_spec,) * 2 + (vmem_spec, vmem_spec, hbm_spec, hbm_spec, vmem_spec, hbm_spec, hbm_spec, vmem_spec),
        scratch_shapes=[wide(count, feats, feats), dma((count + 2,))],
        compiler_params=pltpu.CompilerParams(vmem_limit_bytes=16 << 20),
    )(outs, res, hid, du, small)


def solution(mesh):
    split = P("seq", "tm", None)
    return jax.shard_map(
        shards,
        mesh=mesh,
        in_specs=(split, P("seq", None)) + (P(),) * 8 + (split,),
        out_specs=(split, split) + (P(),) * 8,
        check_vma=False,
    )
```

```python
import functools

import jax
import jax.numpy as jnp
from jax import lax
from jax.experimental import pallas as pl
from jax.experimental.pallas import tpu as pltpu
from jax.sharding import PartitionSpec as P

HEADS = 4
HD = 128
HALF = 9
HALO = 16
PAD = 8
EPS = 1e-05
MESH = pl.DeviceIdType.MESH
F32 = jnp.float32
BF16 = jnp.bfloat16


LEAD = (5, 0, 2, 2, 0, 0, 5, 0, -3, 2, 10, 10)
CHOICE = (4, 3, 6, 1, 0, 1, 2, 4, 0, 1, 0, 1)


def step_orders(seq_size, tm_size):
    seq_bits = [("seq", b) for b in range(seq_size.bit_length() - 1)]
    tm_bits = [("tm", b) for b in range(tm_size.bit_length() - 1)]
    one = lambda bits: [(bit,) for bit in bits]
    two = lambda bits: [tuple(bits[i : i + 2]) for i in range(0, len(bits), 2)]
    core, rest = one(tm_bits[:1]), tm_bits[1:]
    swapped = seq_bits[::-1]
    kinds = [
        core + one(seq_bits) + two(rest),
        core + one(swapped) + two(rest),
        core + one(rest[:1]) + one(seq_bits) + one(rest[1:]),
        core + one(rest[:1]) + one(swapped) + one(rest[1:]),
        core + two(seq_bits) + two(rest),
        core + two(rest) + two(seq_bits),
        core + one(seq_bits) + one(rest),
        core + one(swapped) + one(rest),
        core + two(rest) + one(seq_bits),
        core + two(rest) + one(swapped),
        core + two(seq_bits) + one(rest),
        core + one(seq_bits[:1]) + two(rest) + one(seq_bits[1:]),
        core + one(swapped[:1]) + two(rest) + one(swapped[1:]),
        core + one(seq_bits[:1]) + one(rest[:1]) + one(seq_bits[1:]) + one(rest[1:]),
        core + one(swapped[:1]) + one(rest[:1]) + one(swapped[1:]) + one(rest[1:]),
    ]
    return kinds, [kinds[c] for c in CHOICE]


def bit_of(axis, bit):
    return lax.rem(lax.axis_index(axis) // (1 << bit), 2)


def peer_of(bits, flips):
    at = {"seq": lax.axis_index("seq"), "tm": lax.axis_index("tm")}
    for i, (axis, bit) in enumerate(bits):
        if flips >> i & 1:
            at[axis] = at[axis] + (1 - 2 * bit_of(axis, bit)) * (1 << bit)
    return at["seq"], at["tm"]


def digit_of(bits, flips=0):
    total = 0
    for i, (axis, bit) in enumerate(bits):
        mine = bit_of(axis, bit)
        total = total + (1 - mine if flips >> i & 1 else mine) * (1 << i)
    return total


def gathered_at(unit, rows, held_rows, feats):
    held = held_rows // rows
    index = unit % held
    if unit < held and rows == feats:
        half = held // 2
        index = 2 * (unit % half) + unit // half
    return unit // held, index * rows


class Reducer:
    def __init__(self, orders, rows, part, recv, fulls, sems):
        self.orders, self.rows = orders, rows
        self.part, self.recv, self.fulls = part, recv, fulls
        self.rs_send, self.rs_recv, self.ag_send, self.ag_recv = sems

    def levels(self, unit):
        return len(self.orders[unit])

    def size(self, unit, level):
        return self.rows >> sum(len(bits) for bits in self.orders[unit][:level])

    def owned(self, unit, level):
        off = 0
        for i in range(level):
            off = off + digit_of(self.orders[unit][i]) * self.size(unit, i + 1)
        return off

    def peers(self, unit, level):
        return range(1, 1 << len(self.orders[unit][level]))

    def slot(self, unit, level, flips):
        return sum((1 << len(bits)) - 1 for bits in self.orders[unit][:level]) + flips - 1

    def landing(self, unit, level, flips):
        return self.rows - self.size(unit, level) + (flips - 1) * self.size(unit, level + 1)

    def scatter_copies(self, unit, level):
        bits, found = self.orders[unit][level], []
        size = self.size(unit, level + 1)
        for flips in self.peers(unit, level):
            off = pl.multiple_of(self.owned(unit, level) + digit_of(bits, flips) * size, 16)
            at = self.slot(unit, level, flips)
            found.append(pltpu.make_async_remote_copy(
                src_ref=self.part.at[unit, pl.ds(off, size)],
                dst_ref=self.recv.at[unit, pl.ds(self.landing(unit, level, flips), size)],
                send_sem=self.rs_send.at[unit, at],
                recv_sem=self.rs_recv.at[unit, at],
                device_id=peer_of(bits, flips),
                device_id_type=MESH,
            ))
        return found

    def full(self, unit):
        which, start = gathered_at(unit, self.rows, *self.fulls[0].shape)
        return self.fulls[which], start

    def gather_copies(self, unit, level):
        bits, found = self.orders[unit][level], []
        ref, start = self.full(unit)
        off = pl.multiple_of(start + self.owned(unit, level + 1), 16)
        region = ref.at[pl.ds(off, self.size(unit, level + 1))]
        for flips in self.peers(unit, level):
            at = self.slot(unit, level, flips)
            found.append(pltpu.make_async_remote_copy(
                src_ref=region,
                dst_ref=region,
                send_sem=self.ag_send.at[unit, at],
                recv_sem=self.ag_recv.at[unit, at],
                device_id=peer_of(bits, flips),
                device_id_type=MESH,
            ))
        return found

    def combine(self, unit, level):
        for copy in self.scatter_copies(unit, level):
            copy.wait_recv()
        off, size = self.owned(unit, level + 1), self.size(unit, level + 1)
        step = min(size, 32)

        def body(i, carry):
            here = pl.ds(pl.multiple_of(off + i * step, 16), step)
            total = self.part[unit, here, :].astype(F32)
            for flips in self.peers(unit, level):
                there = pl.ds(pl.multiple_of(self.landing(unit, level, flips) + i * step, 16), step)
                total = total + self.recv[unit, there, :].astype(F32)
            if level == self.levels(unit) - 1:
                ref, start = self.full(unit)
                ref[pl.ds(pl.multiple_of(start + off + i * step, 16), step), :] = total.astype(BF16)
            else:
                self.part[unit, here, :] = total.astype(BF16)
            return carry

        lax.fori_loop(0, size // step, body, 0)

    def tick(self, unit, i):
        levels = self.levels(unit)
        if 0 < i <= levels:
            self.combine(unit, i - 1)
        elif i > levels:
            for copy in self.gather_copies(unit, 2 * levels - i):
                copy.wait_recv()
        if i < levels:
            out = self.scatter_copies(unit, i)
        elif i < 2 * levels:
            out = self.gather_copies(unit, 2 * levels - 1 - i)
        else:
            out = []
        for copy in out:
            copy.start()

    def wait_sends(self, unit):
        for level in range(self.levels(unit)):
            for copy in self.scatter_copies(unit, level) + self.gather_copies(unit, level):
                copy.wait_send()


def plan_steps(orders, small_steps, rows, feats, pieces, lead):
    core_rate, link_rate = 600e3, 104e3
    free, reached, arrival = {}, {}, {}
    levels = {u: len(order) for u, order in enumerate(orders)}
    levels[-1] = len(small_steps)

    def size_of(unit, level):
        return (rows >> sum(len(bits) for bits in orders[unit][: level + 1])) * feats * 2

    def send(unit, now, level):
        bits = (orders[unit] if unit >= 0 else small_steps)[level]
        size = size_of(unit, level) if unit >= 0 else 16 * feats * 4
        wire = 2 * size / link_rate
        near, far = ("tm", 1), ("tm", 2)
        if bits[0] == ("tm", 0):
            uses, lag = [("core", size / core_rate)], 1.1
        elif len(bits) == 2:
            if bits[0][0] == "seq":
                uses, lag = [(bit, 2 * wire) for bit in bits], 3.3
            else:
                uses, lag = [(near, 3 * wire), (far, 4 * wire)], 4.0
        elif bits[0][0] == "seq" or bits[0] == near:
            uses, lag = [(bits[0], wire)], 2.6
        else:
            uses, lag = [(near, wire), (far, 2 * wire)], 3.3
        start = max([now] + [free.get(name, 0.0) for name, _ in uses])
        for name, busy in uses:
            free[name] = start + busy
        return start + max(busy for _, busy in uses) + lag

    def step(unit, now):
        i = reached[unit]
        reached[unit] = i + 1
        cost = 0.05
        if unit >= 0:
            cost = 0.02 + (size_of(unit, i - 1) / 2.4e6 if 0 < i <= levels[unit] else 0.0)
        if i < levels[unit]:
            arrival[unit] = send(unit, now + cost, i)
        elif i < last(unit):
            arrival[unit] = send(unit, now + cost, 2 * levels[unit] - 1 - i)
        return cost

    def last(unit):
        return levels[unit] if unit < 0 else 2 * levels[unit]

    now, crossed, placed = 0.0, 0.0, {}
    for slot, us, begins in pieces:
        now = (max(now, crossed) if slot == "w" else now) + us
        if slot[0] == "b" and slot[1] % 2:
            free[("tm", 1)] = max(now, free.get(("tm", 1), 0.0)) + 0.65
            free[("tm", 2)] = max(now, free.get(("tm", 2), 0.0)) + 0.65
            crossed = max(free[("tm", 1)], free[("tm", 2)]) + 2.6
        todo = []
        if begins is not None:
            reached[begins] = 0
            now += step(begins, now)
        while True:
            ready = [u for u in reached if reached[u] <= last(u) and arrival[u] <= now]
            if not ready:
                break
            unit = min(ready, key=lambda u: (arrival[u] - lead[u], u))
            todo.append((unit, reached[unit]))
            now += step(unit, now)
        placed[slot] = todo
    work_end = now
    reached[-1] = 0
    now += step(-1, now)
    tail = []
    while True:
        left = [u for u in reached if reached[u] <= last(u)]
        if not left:
            break
        unit = min(left, key=lambda u: (arrival[u], u))
        now = max(now, arrival[unit])
        tail.append((unit, reached[unit]))
        now += step(unit, now)
    return placed, tail, (work_end, now)


def make_pieces(seqs, ff_blocks, per_unit):
    pairs = seqs // 2
    begun = lambda block: block // per_unit if block % per_unit == per_unit - 1 else None
    pieces = []
    for j in range(ff_blocks):
        pieces += [(("f", j, t), 1.53, None) for t in range(seqs // 4)]
        pieces += [(("d", j), 0.73, begun(j)), (("u", j), 0.73, begun(ff_blocks + j))]
    pieces += [(("x", t), 0.63, None) for t in range(pairs)]
    pieces += [(("b", s), 0.64, None) for s in range(seqs)]
    pieces += [
        ("q", 0.73, begun(2 * ff_blocks + 1)), ("o", 0.73, begun(2 * ff_blocks)), ("w", 0.5, None),
        ("k", 0.73, begun(2 * ff_blocks + 2)), ("v", 0.73, begun(2 * ff_blocks + 3)),
    ]
    pieces += [(("i", s), 0.91, None) for s in range(seqs)]
    return pieces


def beside(tm_size):
    at = lax.axis_index("tm")
    seq = lax.axis_index("seq")
    return [(at < tm_size - 1, (seq, at + 1)), (at > 0, (seq, at - 1))]


def greet(bits, tm_size):
    barrier = pltpu.get_barrier_semaphore()
    for step, flips in bits:
        pl.semaphore_signal(barrier, inc=1, device_id=peer_of(step, flips), device_id_type=MESH)
    for there, peer in beside(tm_size):
        @pl.when(there)
        def _():
            pl.semaphore_signal(barrier, inc=1, device_id=peer, device_id_type=MESH)


def enter(bits, tm_size):
    count = len(bits)
    for there, _ in beside(tm_size):
        count = count + there.astype(jnp.int32)
    pl.semaphore_wait(pltpu.get_barrier_semaphore(), count)


def nn(a, b):
    return lax.dot_general(a, b, (((1,), (0,)), ((), ())), preferred_element_type=F32)


def nt(a, b):
    return lax.dot_general(a, b, (((1,), (1,)), ((), ())), preferred_element_type=F32)


def tn(a, b):
    return lax.dot_general(a, b, (((0,), (0,)), ((), ())), preferred_element_type=F32)


def moments(v):
    mean = jnp.mean(v, axis=-1, keepdims=True)
    centered = v - mean
    var = jnp.mean(centered * centered, axis=-1, keepdims=True)
    return centered, lax.rsqrt(var + EPS)


def fold(v):
    rows, cols = v.shape
    return jnp.sum(v.reshape(rows // 8, 8, cols), axis=0)


def gelu_pair(v):
    c = 0.7978845608028654
    square = v * v
    inner = v * (c + (c * 0.044715) * square)
    t = jnp.tanh(inner)
    half = 0.5 * (1.0 + t)
    slope = half + (0.5 * v) * (1.0 - t * t) * (c + (3.0 * 0.044715 * c) * square)
    return v * half, slope


def loop(count, body):
    def step(i, carry):
        body(i)
        return carry

    lax.fori_loop(0, count, step, 0)


def layer_kernel(cfg, *refs):
    (
        lengths, x_hbm, norm_gain, conv_kernel, mlp_gain, layer_scale, wqkv_hbm, wout_hbm, wup_hbm, wdown_hbm, cot_hbm,
        outs, res, hid, du, small_out,
        params, x, cot, wqkv, wout, wup, wdown, halo_lo, halo_hi, nf, link,
        act_q, act_k, act_v, qs, ks, vs, prob, att, n2, dm, dbr, da,
        dke, dve, dmx, msg_hi, msg_lo, got_lo, got_hi, dq_hi, dq_lo, dq_got_lo, dq_got_hi,
        edge, edge_mix, sums, small_cur, small_recv,
        part, recv,
        in_sem, halo_send, halo_recv, rs_send, rs_recv, ag_send, ag_recv, sm_send, sm_recv,
    ) = refs
    orders, small_steps, rows, seqs, frames, feats, ff, tm_size = cfg
    units = len(orders)
    levels = len(small_steps)
    greeted = sorted({(bits, flips) for order in orders + [small_steps] for bits in order for flips in range(1, 1 << len(bits))})
    known = {}
    for bits, flips in greeted:
        known.setdefault(tuple(bit for i, bit in enumerate(bits) if flips >> i & 1), (bits, flips))
    greeted = list(known.values())
    ext = frames + 2 * HALO
    own = PAD + HALO
    seq_length = frames * tm_size
    vids = lengths.shape[1]
    temper = HD ** (-0.5)
    lanes = [pl.ds(c * 128, 128) for c in range(feats // 128)]
    pairs = seqs // 2
    per_unit = rows // feats
    base = lax.axis_index("tm") * frames
    red = Reducer(orders, rows, part, recv, (hid, du), (rs_send, rs_recv, ag_send, ag_recv))

    loads = [
        pltpu.make_async_copy(src, dst, in_sem.at[i])
        for i, (src, dst) in enumerate(
            [(x_hbm, x), (wqkv_hbm, wqkv), (wout_hbm, wout), (wup_hbm, wup), (wdown_hbm, wdown), (cot_hbm, cot)]
        )
    ]
    loads[0].start()

    class Across:
        def __init__(self, src, dst, i, side):
            (self.sends, peer), (self.gets, _) = beside(tm_size)[side], beside(tm_size)[1 - side]
            self.copy = pltpu.make_async_remote_copy(
                src_ref=src, dst_ref=dst, send_sem=halo_send.at[i], recv_sem=halo_recv.at[i],
                device_id=peer, device_id_type=MESH,
            )

        def start(self):
            pl.when(self.sends)(lambda: self.copy.start())

        def wait_recv(self):
            pl.when(self.gets)(lambda: self.copy.wait_recv())

        def wait_send(self):
            pl.when(self.sends)(lambda: self.copy.wait_send())

    greet(greeted, tm_size)
    for n in range(3):
        params[pl.ds(3 * n, 3), :] = conv_kernel[n].astype(F32)
    for i, src in enumerate((norm_gain, mlp_gain, layer_scale)):
        params[pl.ds(9 + i, 1), :] = src[...].astype(F32).reshape(1, feats)

    def clear_missing(side, refs_in):
        there = beside(tm_size)[side][0]

        @pl.when(jnp.logical_not(there))
        def _():
            for ref in refs_in:
                ref[...] = jnp.zeros_like(ref)

    clear_missing(1, (halo_lo, got_lo, dq_got_lo))
    clear_missing(0, (halo_hi, got_hi, dq_got_hi))
    to_next = Across(x.at[:, pl.ds(frames - HALO, HALO)], halo_lo, 0, 0)
    to_prev = Across(x.at[:, pl.ds(0, HALO)], halo_hi, 1, 1)
    sums[...] = jnp.zeros_like(sums)

    def bounds_of(s):
        total, found = 0, []
        for j in range(vids):
            total = total + lengths[s, j]
            found.append(total)
        return found

    gain_one = params[pl.ds(9, 1), :]
    gain_two = params[pl.ds(10, 1), :]
    scale = params[pl.ds(11, 1), :]

    def normed_rows(rows_in):
        centered, r = moments(rows_in.astype(F32))
        return (centered * r * gain_one).astype(BF16).astype(F32)

    loads[0].wait()
    for load in loads[1:]:
        load.start()

    def norm_own(t):
        two = pl.ds(2 * t, 2)
        value = normed_rows(x[two].reshape(2 * frames, feats))
        pos = base - own + lax.broadcasted_iota(jnp.int32, (ext + 2 * PAD, 128), 0)
        links = []
        for i in range(2):
            cut = pos == 0
            for bound in bounds_of(2 * t + i):
                cut = cut | (pos == bound)
            links.append(jnp.where(cut, 0.0, 1.0))
        zero = jnp.zeros((2, PAD, feats), F32)
        nf[two, pl.ds(own, frames), :] = value.reshape(2, frames, feats)
        nf[two, pl.ds(0, PAD), :] = zero
        nf[two, pl.ds(PAD + ext, PAD), :] = zero
        for i in range(2):
            link[2 * t + i] = links[i]

    loop(pairs, norm_own)
    enter(greeted, tm_size)
    to_next.start()
    to_prev.start()
    loads[1].wait()
    streams = ((act_q, qs, 0), (act_k, ks, HALO), (act_v, vs, HALO))

    def mixed_rows(s, start, count, lane):
        before = nf[s, pl.ds(PAD + start - 1, count), lane] * link[s, pl.ds(PAD + start, count), :]
        centre = nf[s, pl.ds(PAD + start, count), lane]
        after = nf[s, pl.ds(PAD + start + 1, count), lane] * link[s, pl.ds(PAD + start + 1, count), :]
        found = []
        for n in range(3):
            k0, k1, k2 = (params[pl.ds(3 * n + c, 1), lane] for c in range(3))
            found.append((k0 * before + k1 * centre + k2 * after).astype(BF16))
        return found

    def mix_project(t):
        two = pl.ds(2 * t, 2)
        rows_of = lambda i: [mixed_rows(2 * t + i, HALO, frames, lane) for lane in lanes]
        found = [rows_of(0), rows_of(1)]
        acts = [
            jnp.concatenate([jnp.concatenate([m[n] for m in half], axis=1) for half in found], axis=0)
            for n in range(3)
        ]
        values = [nn(act, wqkv[n]).astype(BF16) for n, act in enumerate(acts)]
        for (kept, dst, skip), act, value in zip(streams, acts, values):
            kept[two] = act.reshape(2, frames, feats)
            dst[two, pl.ds(skip, frames), :] = value.reshape(2, frames, feats)

    loop(pairs, mix_project)
    to_next.wait_recv()
    to_prev.wait_recv()
    ends = 2 * HALO

    def norm_halo(i):
        four = pl.ds(pl.multiple_of(4 * i, 4), 4)
        for src, at in ((halo_lo, PAD), (halo_hi, own + frames)):
            value = normed_rows(src[four].reshape(4 * HALO, feats))
            nf[four, pl.ds(at, HALO), :] = value.reshape(4, HALO, feats)

    loop(seqs // 4, norm_halo)

    def mix_ends(t):
        sides = ((0, 0, HALO, 0), (ends, frames, 0, frames - HALO))
        found = []
        for s in (2 * t, 2 * t + 1):
            for at, start, keep, row in sides:
                half = [mixed_rows(s, start, ends, lane) for lane in lanes]
                found.append((s, at, keep, row, [jnp.concatenate([m[n] for m in half], axis=1) for n in range(3)]))
        for s, at, keep, row, streams_here in found:
            for n, mixed in enumerate(streams_here):
                tile = pl.ds(pl.multiple_of((n * seqs + s) * 2 * ends + at, ends), ends)
                hid[tile, :] = mixed
                streams[n][0][s, pl.ds(row, HALO), :] = mixed[keep : keep + HALO]

    loop(pairs, mix_ends)
    for n, (_, dst, skip) in enumerate(streams):
        count = seqs * 2 * ends
        value = nn(hid[pl.ds(n * count, count), :], wqkv[n]).astype(BF16).reshape(seqs, 2 * ends, feats)
        piece = lambda first, last: lax.slice_in_dim(value, first, last, axis=1)
        if skip:
            dst[:, pl.ds(0, ends), :] = piece(0, ends)
            dst[:, pl.ds(frames, ends), :] = piece(ends, 2 * ends)
        else:
            dst[:, pl.ds(0, HALO), :] = piece(HALO, ends)
            dst[:, pl.ds(frames - HALO, HALO), :] = piece(ends, ends + HALO)

    def attend(t):
        key = lax.broadcasted_iota(jnp.int32, (ext, frames), 0) - HALO
        query = lax.broadcasted_iota(jnp.int32, (ext, frames), 1)
        pos_k = key + base
        pos_q = lax.broadcasted_iota(jnp.int32, (8, frames), 1) + base
        near = (key - query <= HALF) & (key - query >= -HALF) & (pos_k >= 0) & (pos_k < seq_length)
        results = []
        for s in (2 * t, 2 * t + 1):
            seg_k = jnp.zeros((ext, frames), jnp.int32)
            seg_q = jnp.zeros((8, frames), jnp.int32)
            for bound in bounds_of(s):
                seg_k = seg_k + (pos_k >= bound).astype(jnp.int32)
                seg_q = seg_q + (pos_q >= bound).astype(jnp.int32)
            bias = jnp.where(near & (seg_k == seg_q[0:1]), 0.0, -1e30)
            heads = [pl.ds(h * HD, HD) for h in range(HEADS)]
            scores = [nt(ks[s, :, head], qs[s, :, head]) * temper + bias for head in heads]
            raised = [jnp.exp(value - jnp.max(value, axis=0, keepdims=True)) for value in scores]
            probs = [value * (1.0 / jnp.sum(value, axis=0, keepdims=True)) for value in raised]
            found = [tn(probs[h].astype(BF16), vs[s, :, head]).astype(BF16) for h, head in enumerate(heads)]
            results.append((s, probs, found))
        for s, probs, found in results:
            for h in range(HEADS):
                prob[s, h] = probs[h]
            att[s] = jnp.concatenate(found, axis=1)

    loop(pairs, attend)
    for load in loads[2:]:
        load.wait()
    tall = 2 * frames
    chunk = feats
    tokens = seqs * frames
    def flat(ref, t):
        return ref[pl.ds(2 * t, 2)].reshape(tall, ref.shape[2])

    def back(value):
        return value.reshape(2, frames, feats)

    def residual_norm(t):
        four = pl.ds(4 * t, 4)
        tall_rows = lambda ref: ref[four].reshape(4 * frames, feats)
        residual = tall_rows(x).astype(F32) + nn(tall_rows(att), wout[...])
        d_mlp = (tall_rows(cot).astype(F32) * scale).astype(BF16)
        centered, r = moments(residual)
        normed_two = (centered * r * gain_two).astype(BF16)
        for ref, value in ((res, residual), (n2, normed_two), (dm, d_mlp)):
            ref[four] = value.reshape(4, frames, feats)

    loop(seqs // 4, residual_norm)
    whole = lambda ref: ref[...].reshape(seqs * frames, ref.shape[2])
    early = pl.ds(0, frames)

    def place(block, value):
        part[block // per_unit, pl.ds((block % per_unit) * feats, feats), :] = value.astype(BF16)

    ff_blocks = ff // feats

    def unit_begun(block):
        return block // per_unit if block % per_unit == per_unit - 1 else None

    placed, tail, _ = plan_steps(orders, small_steps, rows, feats, make_pieces(seqs, ff_blocks, per_unit), LEAD)

    def advance(u, i):
        red.tick(u, i)

    def slot(name, index=None, count=0):
        if index is None:
            for u, i in placed[name]:
                advance(u, i)
            return
        for k in range(count):
            if placed[name + (k,)]:
                pl.when(index == k)(lambda k=k: [advance(u, i) for u, i in placed[name + (k,)]] and None)

    def begin(block):
        u = unit_begun(block)
        if u is not None:
            advance(u, 0)

    mlp_sum, e_sum = dke, dve

    for j in range(ff_blocks):
        cols = pl.ds(j * chunk, chunk)

        def hidden_chunk(t, j=j, cols=cols):
            four = pl.ds(4 * t, 4)
            high = 4 * frames
            upper = nn(n2[four].reshape(high, feats), wup[:, cols])
            d_hidden = nt(dm[four].reshape(high, feats), wdown[cols, :])
            value, slope = gelu_pair(upper)
            value, slope = value.astype(BF16), (slope * d_hidden).astype(BF16)
            tile = pl.ds(pl.multiple_of(j * tokens + t * high, high), high)
            mlp_part, e_part = nn(value, wdown[cols, :]), nt(slope, wup[:, cols])
            if j:
                mlp_part = mlp_part + mlp_sum[four, early, :].reshape(high, feats)
                e_part = e_part + e_sum[four, early, :].reshape(high, feats)
            hid[tile, :] = value
            du[tile, :] = slope
            mlp_sum[four, early, :] = mlp_part.reshape(4, frames, feats)
            e_sum[four, early, :] = e_part.reshape(4, frames, feats)
            slot(("f", j), t, seqs // 4)

        loop(seqs // 4, hidden_chunk)
        rows_j = pl.ds(j * tokens, tokens)
        place(j, tn(hid[rows_j, :], whole(dm)))
        begin(j)
        slot(("d", j))
        place(ff_blocks + j, tn(whole(n2), du[rows_j, :]))
        begin(ff_blocks + j)
        slot(("u", j))

    def feed_back(t):
        two = pl.ds(2 * t, 2)
        mlp_out = mlp_sum[two, early, :].reshape(tall, feats)
        e = e_sum[two, early, :].reshape(tall, feats)
        residual = flat(res, t)
        cotan = flat(cot, t).astype(F32)
        output = (residual + scale * mlp_out).astype(BF16)
        centered, r = moments(residual)
        xhat = centered * r
        eg = e * gain_two
        d_res = cotan + r * (
            eg - jnp.mean(eg, axis=-1, keepdims=True) - xhat * jnp.mean(eg * xhat, axis=-1, keepdims=True)
        )
        d_branch = d_res.astype(BF16)
        d_att = nt(d_branch, wout[...]).astype(BF16)
        scale_sum = sums[11] + fold(cotan * mlp_out)
        gain_sum = sums[10] + fold(e * xhat)
        outs[two] = back(output)
        res[two] = back(d_res)
        dbr[two] = back(d_branch)
        da[two] = back(d_att)
        sums[11] = scale_sum
        sums[10] = gain_sum
        slot(("x",), t, pairs)

    loop(pairs, feed_back)


    dq = dm
    dkl, dvl = n2, att

    exchange = []
    for t in range(pairs):
        two = pl.ds(2 * t, 2)
        exchange += [
            Across(msg_hi.at[two], got_lo.at[two], 4 + 2 * t, 0),
            Across(msg_lo.at[two], got_hi.at[two], 5 + 2 * t, 1),
        ]
    exchange += [Across(dq_hi, dq_got_lo, 2, 0), Across(dq_lo, dq_got_hi, 3, 1)]

    def attend_back(s):
        heads = [pl.ds(h * HD, HD) for h in range(HEADS)]
        d_atts = [da[s, :, head] for head in heads]
        probs = [prob[s, h] for h in range(HEADS)]
        d_weights = [nt(vs[s, :, head], d_att) for head, d_att in zip(heads, d_atts)]
        d_scores = [
            (p * (d_w - jnp.sum(p * d_w, axis=0, keepdims=True))).astype(BF16) for p, d_w in zip(probs, d_weights)
        ]
        found = [
            (tn(d_s, ks[s, :, head]), nn(d_s, qs[s, :, head]), nn(p.astype(BF16), d_att))
            for head, d_s, p, d_att in zip(heads, d_scores, probs, d_atts)
        ]
        for head, (d_q, d_k, d_v) in zip(heads, found):
            dq[s, :, head] = (d_q * temper).astype(BF16)
            dke[s, :, head] = d_k * temper
            dve[s, :, head] = d_v
        for i, src in enumerate((dke, dve)):
            cols = pl.ds(i * feats, feats)
            msg_hi[s, :, cols] = src[s, pl.ds(HALO + frames - 1, HALO), :].astype(BF16)
            msg_lo[s, :, cols] = src[s, pl.ds(1, HALO), :].astype(BF16)
        dq_hi[pl.ds(s, 1), :] = dq[s, pl.ds(frames - 16, 16), :].astype(F32)[15:16]
        dq_lo[pl.ds(s, 1), :] = dq[s, pl.ds(0, 16), :].astype(F32)[0:1]
        for t in range(pairs):
            pl.when(s == 2 * t + 1)(lambda t=t: [copy.start() for copy in exchange[2 * t : 2 * t + 2]] and None)
        slot(("b",), s, seqs)

    loop(seqs, attend_back)
    for copy in exchange[2 * pairs :]:
        copy.start()
    place(2 * ff_blocks + 1, tn(whole(act_q), whole(dq)))
    begin(2 * ff_blocks + 1)
    slot("q")
    place(2 * ff_blocks, tn(whole(att), whole(dbr)))
    begin(2 * ff_blocks)
    slot("o")
    for copy in exchange:
        copy.wait_recv()
    edge[0, pl.ds(0, seqs), :] = dq_got_lo[...]
    edge[0, pl.ds(seqs, seqs), :] = dq_got_hi[...]

    def settle(s):
        for i, (src, dst) in enumerate(((dke, dkl), (dve, dvl))):
            cols = pl.ds(i * feats, feats)
            low = pl.ds(HALO - 1, HALO)
            high = pl.ds(HALO + frames - HALO + 1, HALO)
            src[s, low, :] = src[s, low, :] + got_lo[s, :, cols].astype(F32)
            src[s, high, :] = src[s, high, :] + got_hi[s, :, cols].astype(F32)
            dst[s] = src[s, pl.ds(HALO, frames), :].astype(BF16)
            edge[i + 1, pl.ds(s, 1), :] = src[s, pl.ds(HALO - 1, 1), :]
            edge[i + 1, pl.ds(seqs + s, 1), :] = src[s, pl.ds(HALO + frames, 1), :]

    loop(seqs, settle)
    slot("w")
    place(2 * ff_blocks + 2, tn(whole(act_k), whole(dkl)))
    begin(2 * ff_blocks + 2)
    slot("k")
    place(2 * ff_blocks + 3, tn(whole(act_v), whole(dvl)))
    begin(2 * ff_blocks + 3)
    slot("v")
    for n in range(3):
        edge_mix[n] = nt(edge[n].astype(BF16), wqkv[n])

    def input_grads(t):
        two = pl.ds(2 * t, 2)
        for n, src in enumerate((dq, dkl, dvl)):
            value = nt(src[two].reshape(tall, feats), wqkv[n])
            dmx[n, :, pl.ds(PAD, frames), :] = value.reshape(2, frames, feats)
        for i in range(2):
            s = 2 * t + i
            for n in range(3):
                dmx[n, i, pl.ds(PAD - 1, 1), :] = edge_mix[n, pl.ds(s, 1), :]
                dmx[n, i, pl.ds(PAD + frames, 1), :] = edge_mix[n, pl.ds(seqs + s, 1), :]
            here = link[s, pl.ds(own, frames), :]
            after = link[s, pl.ds(own + 1, frames), :]
            e_parts, taps = [], []
            for lane in lanes:
                left = nf[s, pl.ds(own - 1, frames), lane] * here
                mid = nf[s, pl.ds(own, frames), lane]
                right = nf[s, pl.ds(own + 1, frames), lane] * after
                from_left, from_mid, from_right = 0.0, 0.0, 0.0
                for n in range(3):
                    k0, k1, k2 = (params[pl.ds(3 * n + c, 1), lane] for c in range(3))
                    g = dmx[n, i, pl.ds(PAD, frames), lane]
                    taps.append([fold(g * left), fold(g * mid), fold(g * right)])
                    from_mid = from_mid + k1 * g
                    from_right = from_right + k0 * dmx[n, i, pl.ds(PAD + 1, frames), lane]
                    from_left = from_left + k2 * dmx[n, i, pl.ds(PAD - 1, frames), lane]
                e_parts.append(from_mid + from_right * after + from_left * here)
            e = jnp.concatenate(e_parts, axis=1)
            centered, r = moments(x[s].astype(F32))
            xhat = centered * r
            eg = e * gain_one
            d_in = res[s] + r * (
                eg - jnp.mean(eg, axis=-1, keepdims=True) - xhat * jnp.mean(eg * xhat, axis=-1, keepdims=True)
            )
            for n in range(3):
                for c in range(3):
                    tap = jnp.concatenate([taps[3 * l + n][c] for l in range(len(lanes))], axis=1)
                    sums[3 * n + c] = sums[3 * n + c] + tap
            sums[9] = sums[9] + fold(e * xhat)
            res[s] = d_in
            for k in range(i, seqs, 2):
                if placed[("i", k)]:
                    pl.when(s == k)(lambda k=k: [advance(u, step) for u, step in placed[("i", k)]] and None)

    loop(pairs, input_grads)
    small_cur[0] = jnp.sum(sums[...], axis=1)

    def small_copy(level):
        peer = peer_of(small_steps[level], 1)
        return pltpu.make_async_remote_copy(
            src_ref=small_cur.at[level], dst_ref=small_recv.at[level],
            send_sem=sm_send.at[level], recv_sem=sm_recv.at[level],
            device_id=peer, device_id_type=MESH,
        )

    small_copy(0).start()
    for u, small_at in tail:
        if u >= 0:
            advance(u, small_at)
            continue
        small_copy(small_at - 1).wait_recv()
        total = small_cur[small_at - 1] + small_recv[small_at - 1]
        if small_at < levels:
            small_cur[small_at] = total
            small_copy(small_at).start()
        else:
            small_out[...] = total
    to_next.wait_send()
    to_prev.wait_send()
    for copy in exchange:
        copy.wait_send()
    for level in range(levels):
        small_copy(level).wait_send()
    for u in range(units):
        red.wait_sends(u)


def widen_kernel(
    places, outs, res, hid, du, small,
    output, d_inputs, d_gain_one, d_kernel, d_qkv, d_out, d_gain_two, d_up, d_down, d_scale, broad, sem,
):
    count, feats, _ = broad.shape
    ff_blocks = (count - 4) // 2
    passes = [pltpu.make_async_copy(src, dst, sem.at[count + i]) for i, (src, dst) in enumerate(((outs, output), (res, d_inputs)))]
    for put in passes:
        put.start()
    targets = [d_down.at[pl.ds(j * feats, feats)] for j in range(ff_blocks)]
    targets += [d_up.at[:, pl.ds(j * feats, feats)] for j in range(ff_blocks)]
    targets += [d_out] + [d_qkv.at[n] for n in range(3)]
    stores = []
    for i, (which, start) in enumerate(places):
        src = (hid, du)[which]

        def widen(r, src=src, start=start, i=i):
            here = pl.ds(pl.multiple_of(r * 64, 64), 64)
            broad[i, here, :] = src[pl.ds(pl.multiple_of(start + r * 64, 64), 64), :].astype(F32)

        loop(feats // 64, widen)
        stores.append(pltpu.make_async_copy(broad.at[i], targets[i], sem.at[i]))
        stores[-1].start()
    for n in range(3):
        d_kernel[n] = small[pl.ds(3 * n, 3), :]
    for i, dst in enumerate((d_gain_one, d_gain_two, d_scale)):
        dst[...] = small[pl.ds(9 + i, 1), :].reshape(feats)
    for store in passes + stores:
        store.wait()


def shards(
    inputs, lengths, norm_gain, conv_kernel, qkv_weight, out_weight, mlp_gain, up_weight,
    down_weight, layer_scale, cotangent,
):
    seqs, frames, feats = inputs.shape
    ff = up_weight.shape[1]
    seq_size, tm_size = lax.axis_size("seq"), lax.axis_size("tm")
    rows = max(feats, 16 * seq_size * tm_size)
    units = (2 * ff + 4 * feats) // rows
    kinds, orders = step_orders(seq_size, tm_size)
    orders, small_steps = orders[:units], kinds[6]
    levels = len(small_steps)
    copies = max(sum((1 << len(bits)) - 1 for bits in order) for order in orders)
    ext = frames + 2 * HALO
    dma = pltpu.SemaphoreType.DMA
    any_spec = pl.BlockSpec(memory_space=pl.ANY)
    vmem_spec = pl.BlockSpec(memory_space=pltpu.VMEM)
    low = lambda *shape: pltpu.VMEM(shape, BF16)
    wide = lambda *shape: pltpu.VMEM(shape, F32)
    acts = lambda: low(seqs, frames, feats)
    acts_ext = lambda: low(seqs, ext, feats)
    scratch = [
        wide(16, feats), acts(), acts(), low(3, feats, feats), low(feats, feats), low(feats, ff), low(ff, feats),
        low(seqs, HALO, feats), low(seqs, HALO, feats),
        wide(seqs, ext + 2 * PAD, feats), wide(seqs, ext + 2 * PAD, 128),
        acts(), acts(), acts(), acts(), acts_ext(), acts_ext(),
        wide(seqs, HEADS, ext, frames), acts(), acts(), acts(),
        acts(), acts(),
        wide(seqs, ext, feats), wide(seqs, ext, feats), wide(3, 2, frames + 2 * PAD, feats),
        low(seqs, HALO, 2 * feats), low(seqs, HALO, 2 * feats), low(seqs, HALO, 2 * feats), low(seqs, HALO, 2 * feats),
        wide(seqs, feats), wide(seqs, feats), wide(seqs, feats), wide(seqs, feats),
        wide(3, 2 * seqs, feats), wide(3, 2 * seqs, feats), wide(16, 8, feats),
        wide(levels, 16, feats), wide(levels, 16, feats),
        low(units, rows, feats), low(units, rows, feats),
        dma((6,)), dma((4 + seqs,)), dma((4 + seqs,)),
        dma((units, copies)), dma((units, copies)), dma((units, copies)), dma((units, copies)),
        dma((levels,)), dma((levels,)),
    ]
    cfg = (orders, small_steps, rows, seqs, frames, feats, ff, tm_size)
    out_type = jax.ShapeDtypeStruct
    stay = lambda v: pltpu.with_memory_space_constraint(v, pltpu.HBM)
    held = out_type((seqs * frames * ff // feats, feats), BF16)
    outs, res, hid, du, small = pl.pallas_call(
        functools.partial(layer_kernel, cfg),
        out_shape=(
            pltpu.VMEM(inputs.shape, BF16), pltpu.VMEM(inputs.shape, F32), pltpu.VMEM(held.shape, BF16),
            pltpu.VMEM(held.shape, BF16), pltpu.VMEM((16, feats), F32),
        ),
        in_specs=[pl.BlockSpec(memory_space=pltpu.SMEM), any_spec] + [vmem_spec] * 4 + [any_spec] * 5,
        out_specs=(vmem_spec,) * 5,
        scratch_shapes=scratch,
        compiler_params=pltpu.CompilerParams(
            collective_id=0, has_side_effects=True, vmem_limit_bytes=50 << 20
        ),
    )(
        lengths, stay(inputs), norm_gain, conv_kernel, mlp_gain, layer_scale, stay(qkv_weight), stay(out_weight),
        stay(up_weight), stay(down_weight), stay(cotangent),
    )
    count = (2 * ff + 4 * feats) // feats
    per_unit = rows // feats
    places = []
    for block in range(count):
        which, start = gathered_at(block // per_unit, rows, *held.shape)
        places.append((which, start + block % per_unit * feats))
    hbm_spec = pl.BlockSpec(memory_space=pltpu.HBM)
    return pl.pallas_call(
        functools.partial(widen_kernel, places),
        out_shape=(
            out_type(inputs.shape, BF16), out_type(inputs.shape, F32),
            out_type((feats,), F32), out_type((3, 3, feats), F32), out_type((3, feats, feats), F32),
            out_type((feats, feats), F32), out_type((feats,), F32), out_type((feats, ff), F32),
            out_type((ff, feats), F32), out_type((feats,), F32),
        ),
        in_specs=[vmem_spec] * 5,
        out_specs=(hbm_spec,) * 2 + (vmem_spec, vmem_spec, hbm_spec, hbm_spec, vmem_spec, hbm_spec, hbm_spec, vmem_spec),
        scratch_shapes=[wide(count, feats, feats), dma((count + 2,))],
        compiler_params=pltpu.CompilerParams(vmem_limit_bytes=16 << 20),
    )(outs, res, hid, du, small)


def solution(mesh):
    split = P("seq", "tm", None)
    return jax.shard_map(
        shards,
        mesh=mesh,
        in_specs=(split, P("seq", None)) + (P(),) * 8 + (split,),
        out_specs=(split, split) + (P(),) * 8,
        check_vma=False,
    )
```
